128 devices in a mesh: dp: 16 (over z, x_lo, core), tensor: 8 (over x_hi, y).
Axes of the slice: x: 4 (x_hi: 2, x_lo: 2; x = x_hi * 2 + x_lo), y: 4, z: 4, core: 2. Of those that a mesh axis runs over, the one named last changes fastest.
Arguments:
- prompt_ids: int32 [16384], P(('dp', 'tensor')), may hold values from 0 to 128255
- prompt_lengths: int32 [32], replicated, may hold values from 1 to 512, as said below
- embed_table: bfloat16 [4096, 128256], P(('dp', 'tensor')), may hold values from -4 to 4
- norm_gain: float32 [4096], replicated, may hold values from 0.5 to 1.5
- w_query: bfloat16 [4096, 4096], P('dp', 'tensor'), may hold values from -3 to 3
- w_key: bfloat16 [4096, 1024], P('dp', 'tensor'), may hold values from -1 to 1
- w_value: bfloat16 [4096, 1024], P('dp', 'tensor'), may hold values from -0.09375 to 0.09375
- w_out: bfloat16 [4096, 4096], P('tensor', 'dp'), may hold values from -0.09375 to 0.09375
Outputs:
- hidden: bfloat16 [16384, 4096], P(('dp', 'tensor'))
- kv_cache: bfloat16 [128, 2, 512, 256], P(('dp', 'tensor'))
The draws below stay inside these ranges and needn't reach their ends.
Inputs may be any that keep to these rules, and one draw needn't show every extreme that they name: `prompt_lengths`: each group's prompt has 1 to 512 live tokens, and some group's has 512.
All inputs are finite; a program needn't handle non-finite values.
Results may differ from the reference program's by a relative error of at most 0.0095.
Values may be sent and summed in bfloat16 or wider, within the bound.
A program may use at most 192 MiB of HBM per device.

```python
import math
import jax
import jax.numpy as jnp
import numpy as np
from jax import lax

D = 4096
HEADS = 32
KVH = 8
HD = 128
VOCAB = 128256
TPG = 4
PROMPT = 512
GROUPS = 32
TOKENS = 16384
N_TENSOR = 8


def draw_prompt_lengths(key, part):
    base = jax.random.randint(jax.random.fold_in(key, 11), (GROUPS,), 1, PROMPT + 1)
    chosen = jax.random.randint(jax.random.fold_in(key, 12), (), 0, GROUPS)
    return jnp.where(jnp.arange(GROUPS) == chosen, PROMPT, base).astype(jnp.int32)


def draw_embed_table(key, part):
    base = jnp.clip(jax.random.normal(jax.random.fold_in(key, 21), (D, VOCAB), jnp.float32), -6.0, 6.0)
    return jnp.clip(0.2 * base, -4.0, 4.0).astype(jnp.bfloat16)


def shared_keys(key):
    base = jax.random.normal(jax.random.fold_in(key, 31), (D, KVH * HD), jnp.float32)
    return jnp.clip(base, -6.0, 6.0) * D ** (-0.5)


def draw_w_key(key, part):
    return jnp.clip(shared_keys(key), -1.0, 1.0).astype(jnp.bfloat16)


def draw_w_query(key, part):
    own = jnp.clip(jax.random.normal(jax.random.fold_in(key, 32), (D, D), jnp.float32), -6.0, 6.0) * D ** (-0.5)
    return jnp.clip(own, -3.0, 3.0).astype(jnp.bfloat16)


def set_ends(values, own_key, smallest, top_value):
    longest = values.shape.index(max(values.shape))
    spots = []
    for shift in (0, 1):
        where = [jax.random.randint(jax.random.fold_in(own_key, axis), (), 0, length) for axis, length in enumerate(values.shape)]
        where[longest] = (where[longest] + shift) % values.shape[longest]
        spots.append(tuple(where))
    return values.at[spots[0]].set(smallest).at[spots[1]].set(top_value)


def level_of(stream_key, shape, pieces, least, top_value):
    gain, own = 1.0, jax.random.fold_in(stream_key, 6)
    for dim, blocks in pieces:
        heights = jnp.exp(jax.random.uniform(jax.random.fold_in(own, dim), (blocks,), jnp.float32, least / len(pieces), top_value / len(pieces)))
        gain = gain * jnp.repeat(heights, shape[dim] // blocks).reshape([-1 if axis == dim else 1 for axis in range(len(shape))])
    return gain


def skewed_wide(stream_key, extent, number_of, slope):
    portions = [min(1 << octave, number_of + 1 - (1 << octave)) * (1 << 20) // math.isqrt((1 << octave) ** slope) + 1 for octave in range((number_of + 1).bit_length()) if 1 << octave <= number_of]
    width = 1 + sum(portions) // (1 << 30)
    grid = np.cumsum(np.array([max(1, weight // width) for weight in portions]))
    lot = jax.random.randint(jax.random.fold_in(stream_key, 1), extent, 0, int(grid[len(portions) - 1]))
    start = jnp.left_shift(1, jnp.searchsorted(jnp.asarray(grid, jnp.int32), lot, side="right").astype(jnp.int32))
    rank = start - 1 + jax.random.randint(jax.random.fold_in(stream_key, 4), extent, 0, 1 << 30) % jnp.minimum(start, number_of + 1 - start)
    return jax.random.permutation(jax.random.fold_in(stream_key, 2), number_of)[rank].astype(jnp.int32)


def scatter_about(stream_key, shape, deviation, bound, split=(), kind=jnp.bfloat16):
    entries = jax.random.normal(stream_key, shape, jnp.float32) * deviation
    if len(split) > 0:
        entries = level_of(stream_key, shape, split, -0.22, 0.18) * entries
    return jnp.clip(entries, min=-bound, max=bound).astype(kind)


def setup_inputs(seed: int = 0) -> dict:
    arg_keys = jax.random.split(jax.random.key(seed), 9)
    return {
        "prompt_ids": set_ends(skewed_wide(arg_keys[0], (TOKENS,), VOCAB, 2), jax.random.fold_in(arg_keys[0], 3), 0, VOCAB - 1).astype(jnp.int32),
        "prompt_lengths": draw_prompt_lengths(jax.random.fold_in(arg_keys[8], 71), 0),
        "embed_table": draw_embed_table(jax.random.fold_in(arg_keys[8], 71), 0),
        "norm_gain": jnp.clip(1.0 + 0.1 * jax.random.normal(arg_keys[3], (D,), jnp.float32), 0.5, 1.5),
        "w_query": draw_w_query(jax.random.fold_in(arg_keys[8], 71), 0),
        "w_key": draw_w_key(jax.random.fold_in(arg_keys[8], 71), 0),
        "w_value": scatter_about(arg_keys[6], (D, KVH * HD), D ** -0.5, 0.09375, ((0, 16), (1, 8))),
        "w_out": scatter_about(arg_keys[7], (D, D), D ** -0.5, 0.09375, ((0, 8), (1, 16))),
    }


norm_eps = 1e-05
rope_theta = 500000.0

def rotate(heads_in, positions):
    half = heads_in.shape[-1] // 2
    freq = rope_theta ** (-2.0 * jnp.arange(half, dtype=jnp.float32) / heads_in.shape[-1])
    angle = positions.astype(jnp.float32)[:, None] * freq[None, :]
    cosine = jnp.cos(angle)[:, None, :]
    sine = jnp.sin(angle)[:, None, :]
    first = heads_in[..., :half]
    second = heads_in[..., half:]
    return jnp.concatenate([first * cosine - second * sine, second * cosine + first * sine], axis=-1)

def attend(query_rot, key_rot, value_rows, length):
    row_count = query_rot.shape[0]
    block = min(512, row_count)
    positions = jnp.arange(row_count, dtype=jnp.int32)
    keys_wide = key_rot.astype(jnp.float32)
    values_wide = value_rows.astype(jnp.float32)

    def one_block(offset):
        queries = lax.dynamic_slice_in_dim(query_rot, offset, block, 0).astype(jnp.float32)
        scores = jnp.einsum('qhgd,khd->hgqk', queries, keys_wide) / jnp.sqrt(jnp.float32(HD))
        query_pos = offset + jnp.arange(block, dtype=jnp.int32)
        allowed = (positions[None, :] <= query_pos[:, None]) & (positions[None, :] < length)
        scores = jnp.where(allowed, scores, -1e+30)
        biggest = lax.optimization_barrier(jnp.max(scores, axis=-1, keepdims=True))
        expd = jnp.exp(scores - biggest)
        weights = (expd / lax.optimization_barrier(jnp.sum(expd, axis=-1, keepdims=True))).astype(jnp.bfloat16)
        result = jnp.einsum('hgqk,khd->qhgd', weights.astype(jnp.float32), values_wide)
        return result.astype(jnp.bfloat16)
    starts = jnp.arange(0, row_count, block, dtype=jnp.int32)
    outs = lax.map(one_block, starts)
    return outs.reshape(row_count, -1)

def layer_group(token_ids, length, embed_table, norm_gain, w_query, w_key, w_value, w_out):
    row_count = token_ids.shape[0]
    tokens_in = jnp.take(embed_table, token_ids, axis=1).T
    wide_in = tokens_in.astype(jnp.float32)
    scale = lax.rsqrt(lax.optimization_barrier(jnp.mean(wide_in * wide_in, axis=1, keepdims=True)) + norm_eps)
    normed = (wide_in * scale * norm_gain.astype(jnp.float32)[None, :]).astype(jnp.bfloat16)
    query = jnp.dot(normed, w_query, preferred_element_type=jnp.float32)
    key_raw = jnp.dot(normed, w_key, preferred_element_type=jnp.float32)
    value_raw = jnp.dot(normed, w_value, preferred_element_type=jnp.float32)
    positions = jnp.arange(row_count, dtype=jnp.int32)
    query_rot = rotate(query.reshape(row_count, HEADS, HD), positions).astype(jnp.bfloat16)
    key_rot = rotate(key_raw.reshape(row_count, KVH, HD), positions).astype(jnp.bfloat16)
    value_rows = value_raw.reshape(row_count, KVH, HD).astype(jnp.bfloat16)
    attended = attend(query_rot.reshape(row_count, KVH, HEADS // KVH, HD), key_rot, value_rows, length)
    blocks = N_TENSOR // TPG
    block_width = D // N_TENSOR
    attended_four = attended.reshape(row_count, blocks, TPG, block_width).astype(jnp.float32)
    out_four = w_out.reshape(blocks, TPG, block_width, D).astype(jnp.float32)
    parts = jnp.einsum('rkmw,kmwd->mrd', attended_four, out_four)
    parts = lax.optimization_barrier(parts.astype(jnp.bfloat16)).astype(jnp.float32)
    hidden = (wide_in + lax.optimization_barrier(jnp.sum(parts, axis=0))).astype(jnp.bfloat16)
    kv_width = KVH * HD // N_TENSOR

    def member_major(table_rows):
        shaped = table_rows.reshape(row_count, blocks, TPG, kv_width)
        return shaped.transpose(2, 0, 1, 3).reshape(TPG, row_count, blocks * kv_width)
    cache = jnp.stack([member_major(key_rot.reshape(row_count, KVH * HD)), member_major(value_rows.reshape(row_count, KVH * HD))], axis=1)
    return (hidden, cache)

def reference(prompt_ids, prompt_lengths, embed_table, norm_gain, w_query, w_key, w_value, w_out):
    grouped_ids = prompt_ids.reshape(GROUPS, PROMPT)

    def one_group(pair):
        return layer_group(pair[0], pair[1], embed_table, norm_gain, w_query, w_key, w_value, w_out)
    hidden, cache = lax.map(one_group, (grouped_ids, prompt_lengths))
    return (hidden.reshape(GROUPS * PROMPT, D), cache.reshape(GROUPS * TPG, 2, PROMPT, KVH * HD // TPG))
```

```python
import jax
import jax.numpy as jnp
from jax import lax
from jax.experimental import pallas as pl
from jax.experimental.pallas import tpu as pltpu
from jax.sharding import Mesh
from jax.sharding import PartitionSpec as P

HEADS = 32
KVH = 8
HD = 128
TPG = 4
AXES = ("z", "xlo", "core", "xhi", "y")
DP = ("z", "xlo", "core")
TENSOR = ("xhi", "y")

norm_eps = 1e-05
rope_theta = 500000.0

BLOCKS = 252
STRIP = BLOCKS * 128


def lookup_kernel(row_ref, strip_ref, table_ref, out_ref, raw, major, rows, sems):
    feats, vocab = table_ref.shape
    tiles = vocab // 128
    count = sems.shape[0]
    ends = [tiles * k // count for k in range(count + 1)]
    copies = []
    for k in range(count):
        part = pl.ds(ends[k] * 128, (ends[k + 1] - ends[k]) * 128)
        copies.append(pltpu.make_async_copy(table_ref.at[:, part], raw.at[:, part], sems.at[k]))
    for copy in copies:
        copy.start()
    for copy in copies:
        copy.wait()

    def turn(b, _):
        parts = []
        for strip in range(4):
            first = jnp.minimum(b * 128 + strip * STRIP, vocab - 128)
            parts.append(raw[:, pl.ds(pl.multiple_of(first, 128), 128)])
        block = jnp.concatenate(parts, axis=0)
        major[pl.ds(pl.multiple_of(b * 128, 128), 128), :] = block.T.astype(jnp.float32)
        return 0

    lax.fori_loop(0, BLOCKS, turn, 0, unroll=12)
    eye = (
        lax.broadcasted_iota(jnp.int32, (128, 128), 0)
        == lax.broadcasted_iota(jnp.int32, (128, 128), 1)
    ).astype(jnp.bfloat16)
    prompt = rows.shape[0]

    def group(g, _):
        def some(s, _):
            for i in range(128):
                rows[pl.ds(s * 128 + i, 1), :] = major[pl.ds(row_ref[g * prompt + s * 128 + i], 1), :]
            return 0

        lax.fori_loop(0, prompt // 128, some, 0)
        found = lax.dot_general(
            eye,
            rows[...].astype(jnp.bfloat16),
            (((1,), (1,)), ((), ())),
            preferred_element_type=jnp.float32,
        )
        strip = strip_ref[pl.ds(g, 1), :]
        chosen = found[:feats]
        for k in range(1, 4):
            chosen = jnp.where(strip == k, found[k * feats : (k + 1) * feats], chosen)
        out_ref[pl.ds(g, 1)] = chosen.astype(jnp.bfloat16)[None]
        return 0

    lax.fori_loop(0, out_ref.shape[0], group, 0)


def lookup(table, ids, prompt):
    feats, vocab = table.shape
    groups = ids.shape[0] // prompt
    strip = ids // STRIP
    row = ids - strip * STRIP
    return pl.pallas_call(
        lookup_kernel,
        out_shape=jax.ShapeDtypeStruct((groups, feats, prompt), jnp.bfloat16),
        in_specs=[
            pl.BlockSpec(memory_space=pltpu.SMEM),
            pl.BlockSpec(memory_space=pltpu.VMEM),
            pl.BlockSpec(memory_space=pl.ANY),
        ],
        out_specs=pl.BlockSpec(memory_space=pltpu.VMEM),
        scratch_shapes=[
            pltpu.VMEM((feats, vocab), jnp.bfloat16),
            pltpu.VMEM((STRIP, 128), jnp.float32),
            pltpu.VMEM((prompt, 128), jnp.float32),
            pltpu.SemaphoreType.DMA((6,)),
        ],
        compiler_params=pltpu.CompilerParams(vmem_limit_bytes=50 * 2**20),
        cost_estimate=pl.CostEstimate(flops=30_000_000_000, bytes_accessed=8_000_000, transcendentals=0),
    )(row, strip.reshape(groups, prompt), table)


def rotate(heads_in, positions):
    half = heads_in.shape[-1] // 2
    freq = rope_theta ** (-2.0 * jnp.arange(half, dtype=jnp.float32) / heads_in.shape[-1])
    angle = positions.astype(jnp.float32)[:, None] * freq[None, :]
    cosine = jnp.cos(angle)[:, None, :]
    sine = jnp.sin(angle)[:, None, :]
    first = heads_in[..., :half]
    second = heads_in[..., half:]
    return jnp.concatenate(
        [first * cosine - second * sine, second * cosine + first * sine], axis=-1
    )


def attend(query_rot, key_rot, value_rows, length):
    row_count = query_rot.shape[0]
    positions = jnp.arange(row_count, dtype=jnp.int32)
    scores = jnp.einsum(
        "qhgd,khd->hgqk", query_rot, key_rot, preferred_element_type=jnp.float32
    ) / jnp.sqrt(jnp.float32(HD))
    allowed = (positions[None, :] <= positions[:, None]) & (positions[None, :] < length)
    scores = jnp.where(allowed, scores, -1e30)
    biggest = jnp.max(scores, axis=-1, keepdims=True)
    expd = jnp.exp(scores - biggest)
    weights = (expd / jnp.sum(expd, axis=-1, keepdims=True)).astype(jnp.bfloat16)
    result = jnp.einsum("hgqk,khd->qhgd", weights, value_rows, preferred_element_type=jnp.float32)
    return result.astype(jnp.bfloat16).reshape(row_count, -1)


def swapped(block, apart):
    return lax.ppermute(block, "y", [(k, k ^ 1 << apart) for k in range(TPG)])


def shards(prompt_ids, prompt_lengths, embed_table, norm_gain, w_query, w_key, w_value, w_out):
    quarter = prompt_ids.shape[0]
    row_count = quarter * TPG
    devices = lax.axis_size(AXES)
    features = embed_table.shape[0]
    model_width = features * devices
    member = lax.axis_index("y")
    group_index = lax.axis_index(("z", "xlo", "core", "xhi"))
    length = lax.dynamic_slice_in_dim(prompt_lengths, group_index, 1, 0)[0]
    all_ids = lax.all_gather(prompt_ids, AXES, axis=0, tiled=True)

    query_width = w_query.shape[1]
    key_width = w_key.shape[1]
    packed = jnp.concatenate([w_query, w_key, w_value], axis=1)
    wide = lax.all_gather(packed, ("xhi", "z", "xlo", "core"), axis=0, tiled=True)
    wide = wide.reshape(2, model_width, packed.shape[1])
    out_parts = lax.all_gather(w_out, ("xhi", "z", "xlo", "core"), axis=0, tiled=False)

    picked = lookup(embed_table, all_ids, row_count)
    group_count = devices // TPG
    outgoing = jnp.broadcast_to(
        picked[:, None], (group_count, TPG, features, row_count)
    ).reshape(devices, features, row_count)
    arrived = lax.all_to_all(outgoing, AXES, split_axis=0, concat_axis=0, tiled=True)
    tokens = arrived.reshape(model_width, row_count)
    wide_in = tokens.astype(jnp.float32)
    scale = lax.rsqrt(jnp.mean(wide_in * wide_in, axis=0, keepdims=True) + norm_eps)
    normed = (wide_in * scale * norm_gain[:, None]).astype(jnp.bfloat16)
    own_rows = lax.dynamic_slice_in_dim(tokens, member * quarter, quarter, 1).T

    projected = jnp.einsum("dr,kdc->rkc", normed, wide, preferred_element_type=jnp.float32)
    blocks = projected.shape[1]
    local_heads = blocks * query_width // HD
    local_kv = blocks * key_width // HD
    positions = jnp.arange(row_count, dtype=jnp.int32)
    query = projected[:, :, :query_width].reshape(row_count, local_heads, HD)
    key_raw = projected[:, :, query_width : query_width + key_width]
    value_rows = projected[:, :, query_width + key_width :].astype(jnp.bfloat16)
    query_rot = rotate(query, positions).astype(jnp.bfloat16)
    key_rot = rotate(key_raw, positions).astype(jnp.bfloat16)
    cache = jnp.stack(
        [key_rot.reshape(row_count, local_kv * HD), value_rows.reshape(row_count, local_kv * HD)],
        axis=0,
    )[None]
    attended = attend(
        query_rot.reshape(row_count, local_kv, HEADS // KVH, HD), key_rot, value_rows, length
    )
    attended = attended.reshape(row_count, blocks, query_width)
    out_wide = out_parts.reshape(blocks, -1, query_width, out_parts.shape[-1])
    partial_sum = jnp.einsum(
        "rkw,kdwc->rdc", attended, out_wide, preferred_element_type=jnp.float32
    ).reshape(row_count, model_width)
    running = partial_sum
    for bit_index in reversed(range(2)):
        half_rows = running.shape[0] // 2
        upper_half = member >> bit_index & 1 == 1
        kept = jnp.where(upper_half, running[half_rows:], running[:half_rows]).astype(jnp.bfloat16)
        given = jnp.where(upper_half, running[:half_rows], running[half_rows:]).astype(jnp.bfloat16)
        arrived_sum = swapped(given, bit_index)
        running = kept.astype(jnp.float32) + arrived_sum.astype(jnp.float32)
    hidden = (own_rows.astype(jnp.float32) + running).astype(jnp.bfloat16)
    return (hidden, cache)


def solution(mesh):
    split = Mesh(mesh.devices.reshape(4, 2, 2, 2, 4), AXES)
    placed = (
        P(AXES),
        P(),
        P(AXES, None),
        P(),
        P(DP, TENSOR),
        P(DP, TENSOR),
        P(DP, TENSOR),
        P(TENSOR, DP),
    )
    return jax.shard_map(
        shards,
        mesh=split,
        in_specs=placed,
        out_specs=(P(AXES, None), P(AXES, None, None, None)),
        check_vma=False,
    )
```

```python
import jax
import jax.numpy as jnp
from jax import lax
from jax.experimental import pallas as pl
from jax.experimental.pallas import tpu as pltpu
from jax.sharding import Mesh
from jax.sharding import PartitionSpec as P

HEADS = 32
KVH = 8
HD = 128
TPG = 4
AXES = ("z", "xlo", "core", "xhi", "y")
DP = ("z", "xlo", "core")
TENSOR = ("xhi", "y")

norm_eps = 1e-05
rope_theta = 500000.0

MESH = pl.DeviceIdType.MESH
BLOCKS = 252
STRIP = BLOCKS * 128

def place(g, y):
    return (g // 8, g // 4 % 2, g // 2 % 2, g % 2, y)

def front_kernel(ids_ref, table_ref, out_ref, raw, major, rows, ids, spots, spots_s, stage,
                 table_sems, spot_sem, id_send, id_recv, far_send, far_recv, side_send, side_recv):
    feats, vocab = table_ref.shape
    z = lax.axis_index("z"); xlo = lax.axis_index("xlo"); core = lax.axis_index("core")
    xhi = lax.axis_index("xhi"); y = lax.axis_index("y")
    me = ((z * 2 + xlo) * 2 + core) * 2 + xhi
    groups = out_ref.shape[0]
    up = (y + 1) % 4
    down = (y + 3) % 4
    tiles = vocab // 128
    count = table_sems.shape[0]
    ends = [tiles * k // count for k in range(count + 1)]
    copies = []
    for k in range(count):
        part = pl.ds(ends[k] * 128, (ends[k + 1] - ends[k]) * 128)
        copies.append(pltpu.make_async_copy(table_ref.at[:, part], raw.at[:, part], table_sems.at[k]))
    for copy in copies:
        copy.start()
    barrier = pltpu.get_barrier_semaphore()
    for k in range(1, 4):
        pl.semaphore_signal(barrier, inc=1, device_id=place(me, (y + k) % 4), device_id_type=MESH)
    def greet(k, _):
        pl.semaphore_signal(barrier, inc=1, device_id=place((me + k) % groups, y), device_id_type=MESH)
        return 0
    lax.fori_loop(1, groups, greet, 0)
    pl.semaphore_wait(barrier, 3 + groups - 1)
    ids[pl.ds(me, 1), pl.ds(y, 1), :] = ids_ref[...][None]
    line = []
    for k in range(1, 4):
        c = pltpu.make_async_remote_copy(ids_ref, ids.at[me, pl.ds(y, 1)], id_send.at[k - 1], id_recv.at[k - 1],
            device_id=place(me, (y + k) % 4), device_id_type=MESH)
        c.start(); line.append(c)

    for copy in copies:
        copy.wait()

    def turn(b, _):
        parts = []
        for strip in range(4):
            first = jnp.minimum(b * 128 + strip * STRIP, vocab - 128)
            parts.append(raw[:, pl.ds(pl.multiple_of(first, 128), 128)])
        block = jnp.concatenate(parts, axis=0)
        major[pl.ds(pl.multiple_of(b * 128, 128), 128), :] = block.T.astype(jnp.float32)
        return 0

    half = BLOCKS // 4
    lax.fori_loop(0, half, turn, 0, unroll=9)
    for c in line:
        c.wait()
    def spread(k, _):
        to = (me + k) % groups
        pltpu.make_async_remote_copy(ids.at[me], ids.at[me], id_send.at[3], id_recv.at[3],
            device_id=place(to, y), device_id_type=MESH).start()
        return 0
    lax.fori_loop(1, groups, spread, 0)
    lax.fori_loop(half, BLOCKS, turn, 0, unroll=9)
    others = pltpu.make_async_remote_copy(ids.at[pl.ds(0, groups - 1)], ids.at[pl.ds(0, groups - 1)], id_send.at[3], id_recv.at[3],
        device_id=place(me, up), device_id_type=MESH)
    others.wait_recv()
    all_ids = ids[...]
    strip_of = jnp.zeros_like(all_ids)
    for k in range(1, 4):
        strip_of = strip_of + jnp.where(all_ids >= k * STRIP, 1, 0)
    spots[...] = all_ids - strip_of * STRIP
    to_smem = pltpu.make_async_copy(spots, spots_s, spot_sem)
    to_smem.start()
    to_smem.wait()
    eye = (lax.broadcasted_iota(jnp.int32, (128, 128), 0) == lax.broadcasted_iota(jnp.int32, (128, 128), 1)).astype(jnp.bfloat16)

    def find(g, put):
        def some(s, _):
            for i in range(128):
                rows[pl.ds(s * 128 + i, 1), :] = major[pl.ds(spots_s[g, s, i], 1), :]
            return 0
        lax.fori_loop(0, 4, some, 0)
        found = lax.dot_general(eye, rows[...].astype(jnp.bfloat16), (((1,), (1,)), ((), ())), preferred_element_type=jnp.float32)
        for s in range(4):
            word = ids[pl.ds(g, 1), pl.ds(s, 1), :].reshape(1, 128)
            part = found[:, s * 128:(s + 1) * 128]
            chosen = part[:feats]
            for k in range(1, 4):
                chosen = jnp.where(word >= k * STRIP, part[k * feats:(k + 1) * feats], chosen)
            put(s, chosen.astype(jnp.bfloat16))

    def chunk(p, lo, n):
        zs = (z + 4 - p) % 4
        return pl.ds(zs * 8 + lo, n)

    def side(p, way, lo, n, of, to, slot):
        part = out_ref.at[chunk(p, lo, n), of]
        return pltpu.make_async_remote_copy(part, part, side_send.at[slot, p], side_recv.at[slot, p],
            device_id=place(me, to), device_id_type=MESH)

    def relay(p):
        side(p, 0, 0, 8, down, up, 0).wait_recv()
        side(p, 0, 0, 4, down, up, 2).start()
        side(p, 0, 0, 8, up, down, 1).wait_recv()
        side(p, 0, 4, 4, up, down, 3).start()

    for p in range(4):
        if p == 0:
            def put_own(s, val):
                out_ref[pl.ds(me, 1), pl.ds(y, 1), :, s * 128:(s + 1) * 128] = val[None, None]
            find(me, put_own)
        def one(e, _):
            to_z = (z + p) % 4
            to = ((to_z * 2 + (xlo + e // 4) % 2) * 2 + (core + e // 2) % 2) * 2 + (xhi + e) % 2
            def put(s, val):
                stage[p, pl.ds(e, 1), :, s * 128:(s + 1) * 128] = val[None]
            find(to, put)
            pltpu.make_async_remote_copy(stage.at[p, e], out_ref.at[me, y], far_send.at[p], far_recv.at[p],
                device_id=place(to, y), device_id_type=MESH).start()
            return 0
        lax.fori_loop(1 if p == 0 else 0, 8, one, 0)
        n = 7 if p == 0 else 8
        pltpu.make_async_remote_copy(stage.at[p, pl.ds(0, n)], out_ref.at[pl.ds(0, n), y], far_send.at[p], far_recv.at[p],
            device_id=place(me, up), device_id_type=MESH).wait_recv()
        side(p, 0, 0, 8, y, up, 0).start()
        side(p, 0, 0, 8, y, down, 1).start()
        if p:
            relay(p - 1)
    relay(3)
    others.wait_send()
    for p in range(4):
        n = 7 if p == 0 else 8
        pltpu.make_async_remote_copy(stage.at[p, pl.ds(0, n)], out_ref.at[pl.ds(0, n), y], far_send.at[p], far_recv.at[p],
            device_id=place(me, up), device_id_type=MESH).wait_send()
        side(p, 0, 0, 4, down, up, 2).wait_recv()
        side(p, 0, 4, 4, up, down, 3).wait_recv()
        side(p, 0, 0, 8, y, up, 0).wait_send()
        side(p, 0, 0, 8, y, down, 1).wait_send()
        side(p, 0, 0, 4, down, up, 2).wait_send()
        side(p, 0, 4, 4, up, down, 3).wait_send()


def front(table, ids):
    feats, vocab = table.shape
    return pl.pallas_call(
        front_kernel,
        out_shape=jax.ShapeDtypeStruct((32, 4, feats, 512), jnp.bfloat16),
        in_specs=[pl.BlockSpec(memory_space=pltpu.VMEM), pl.BlockSpec(memory_space=pl.ANY)],
        out_specs=pl.BlockSpec(memory_space=pltpu.VMEM),
        scratch_shapes=[
            pltpu.VMEM((feats, vocab), jnp.bfloat16),
            pltpu.VMEM((STRIP, 128), jnp.float32),
            pltpu.VMEM((512, 128), jnp.float32),
            pltpu.VMEM((32, 4, 128), jnp.int32),
            pltpu.VMEM((32, 4, 128), jnp.int32),
            pltpu.SMEM((32, 4, 128), jnp.int32),
            pltpu.VMEM((4, 8, feats, 512), jnp.bfloat16),
            pltpu.SemaphoreType.DMA((6,)),
            pltpu.SemaphoreType.DMA,
            pltpu.SemaphoreType.DMA((4,)),
            pltpu.SemaphoreType.DMA((4,)),
            pltpu.SemaphoreType.DMA((4,)),
            pltpu.SemaphoreType.DMA((4,)),
            pltpu.SemaphoreType.DMA((4, 4)),
            pltpu.SemaphoreType.DMA((4, 4)),
        ],
        compiler_params=pltpu.CompilerParams(vmem_limit_bytes=50 * 2**20, collective_id=0, has_side_effects=True),
        cost_estimate=pl.CostEstimate(flops=60_000_000_000, bytes_accessed=8_000_000, transcendentals=0),
    )(ids.reshape(1, 128), table)


def rotate(heads_in, positions):
    half = heads_in.shape[-1] // 2
    freq = rope_theta ** (-2.0 * jnp.arange(half, dtype=jnp.float32) / heads_in.shape[-1])
    angle = positions.astype(jnp.float32)[:, None] * freq[None, :]
    cosine = jnp.cos(angle)[:, None, :]
    sine = jnp.sin(angle)[:, None, :]
    first = heads_in[..., :half]
    second = heads_in[..., half:]
    return jnp.concatenate(
        [first * cosine - second * sine, second * cosine + first * sine], axis=-1
    )


def attend(query_rot, key_rot, value_rows, length):
    row_count = query_rot.shape[0]
    positions = jnp.arange(row_count, dtype=jnp.int32)
    scores = jnp.einsum(
        "qhgd,khd->hgqk", query_rot, key_rot, preferred_element_type=jnp.float32
    ) / jnp.sqrt(jnp.float32(HD))
    allowed = (positions[None, :] <= positions[:, None]) & (positions[None, :] < length)
    scores = jnp.where(allowed, scores, -1e30)
    biggest = jnp.max(scores, axis=-1, keepdims=True)
    expd = jnp.exp(scores - biggest)
    weights = (expd / jnp.sum(expd, axis=-1, keepdims=True)).astype(jnp.bfloat16)
    result = jnp.einsum("hgqk,khd->qhgd", weights, value_rows, preferred_element_type=jnp.float32)
    return result.astype(jnp.bfloat16).reshape(row_count, -1)


def swapped(block, apart):
    return lax.ppermute(block, "y", [(k, k ^ 1 << apart) for k in range(TPG)])


def shards(prompt_ids, prompt_lengths, embed_table, norm_gain, w_query, w_key, w_value, w_out):
    quarter = prompt_ids.shape[0]
    row_count = quarter * TPG
    devices = lax.axis_size(AXES)
    features = embed_table.shape[0]
    model_width = features * devices
    member = lax.axis_index("y")
    group_index = lax.axis_index(("z", "xlo", "core", "xhi"))
    length = lax.dynamic_slice_in_dim(prompt_lengths, group_index, 1, 0)[0]
    query_width = w_query.shape[1]
    key_width = w_key.shape[1]
    packed = jnp.concatenate([w_query, w_key, w_value], axis=1)
    wide = lax.all_gather(packed, ("xhi", "z", "xlo", "core"), axis=0, tiled=True)
    wide = wide.reshape(2, model_width, packed.shape[1])
    out_parts = lax.all_gather(w_out, ("xhi", "z", "xlo", "core"), axis=0, tiled=False)

    tokens = front(embed_table, prompt_ids).reshape(model_width, row_count)
    wide_in = tokens.astype(jnp.float32)
    scale = lax.rsqrt(jnp.mean(wide_in * wide_in, axis=0, keepdims=True) + norm_eps)
    normed = (wide_in * scale * norm_gain[:, None]).astype(jnp.bfloat16)
    own_rows = lax.dynamic_slice_in_dim(tokens, member * quarter, quarter, 1).T

    projected = jnp.einsum("dr,kdc->rkc", normed, wide, preferred_element_type=jnp.float32)
    blocks = projected.shape[1]
    local_heads = blocks * query_width // HD
    local_kv = blocks * key_width // HD
    positions = jnp.arange(row_count, dtype=jnp.int32)
    query = projected[:, :, :query_width].reshape(row_count, local_heads, HD)
    key_raw = projected[:, :, query_width : query_width + key_width]
    value_rows = projected[:, :, query_width + key_width :].astype(jnp.bfloat16)
    query_rot = rotate(query, positions).astype(jnp.bfloat16)
    key_rot = rotate(key_raw, positions).astype(jnp.bfloat16)
    cache = jnp.stack(
        [key_rot.reshape(row_count, local_kv * HD), value_rows.reshape(row_count, local_kv * HD)],
        axis=0,
    )[None]
    attended = attend(
        query_rot.reshape(row_count, local_kv, HEADS // KVH, HD), key_rot, value_rows, length
    )
    attended = attended.reshape(row_count, blocks, query_width)
    out_wide = out_parts.reshape(blocks, -1, query_width, out_parts.shape[-1])
    partial_sum = jnp.einsum(
        "rkw,kdwc->rdc", attended, out_wide, preferred_element_type=jnp.float32
    ).reshape(row_count, model_width)
    running = partial_sum
    for bit_index in reversed(range(2)):
        half_rows = running.shape[0] // 2
        upper_half = member >> bit_index & 1 == 1
        kept = jnp.where(upper_half, running[half_rows:], running[:half_rows]).astype(jnp.bfloat16)
        given = jnp.where(upper_half, running[:half_rows], running[half_rows:]).astype(jnp.bfloat16)
        arrived_sum = swapped(given, bit_index)
        running = kept.astype(jnp.float32) + arrived_sum.astype(jnp.float32)
    hidden = (own_rows.astype(jnp.float32) + running).astype(jnp.bfloat16)
    return (hidden, cache)


def solution(mesh):
    split = Mesh(mesh.devices.reshape(4, 2, 2, 2, 4), AXES)
    placed = (
        P(AXES),
        P(),
        P(AXES, None),
        P(),
        P(DP, TENSOR),
        P(DP, TENSOR),
        P(DP, TENSOR),
        P(TENSOR, DP),
    )
    return jax.shard_map(
        shards,
        mesh=split,
        in_specs=placed,
        out_specs=(P(AXES, None), P(AXES, None, None, None)),
        check_vma=False,
    )
```

```python
import jax
import jax.numpy as jnp
import numpy as np
from jax import lax
from jax.experimental import pallas as pl
from jax.experimental.pallas import tpu as pltpu
from jax.sharding import Mesh
from jax.sharding import PartitionSpec as P

HD = 128
TPG = 4
AXES = ("z", "xlo", "core", "xhi", "y")
DP = ("z", "xlo", "core")
TENSOR = ("xhi", "y")

norm_eps = 1e-05
rope_theta = 500000.0

MESH = pl.DeviceIdType.MESH
BLOCKS = 252
STRIP = BLOCKS * 128

def place(g, y):
    return (g // 8, g // 4 % 2, g // 2 % 2, g % 2, y)

def front_kernel(ids_ref, table_ref, out_ref, raw, major, rows, ids, spots, spots_s, stage,
                 table_sems, spot_sem, id_send, id_recv, far_send, far_recv, side_send, side_recv):
    feats, vocab = table_ref.shape
    z = lax.axis_index("z"); xlo = lax.axis_index("xlo"); core = lax.axis_index("core")
    xhi = lax.axis_index("xhi"); y = lax.axis_index("y")
    me = ((z * 2 + xlo) * 2 + core) * 2 + xhi
    groups = out_ref.shape[0]
    up = (y + 1) % 4
    down = (y + 3) % 4
    tiles = vocab // 128
    count = table_sems.shape[0]
    ends = [tiles * k // count for k in range(count + 1)]
    copies = []
    for k in range(count):
        part = pl.ds(ends[k] * 128, (ends[k + 1] - ends[k]) * 128)
        copies.append(pltpu.make_async_copy(table_ref.at[:, part], raw.at[:, part], table_sems.at[k]))
    for copy in copies:
        copy.start()
    barrier = pltpu.get_barrier_semaphore()
    for k in range(1, 4):
        pl.semaphore_signal(barrier, inc=1, device_id=place(me, (y + k) % 4), device_id_type=MESH)
    def greet(k, _):
        pl.semaphore_signal(barrier, inc=1, device_id=place((me + k) % groups, y), device_id_type=MESH)
        return 0
    lax.fori_loop(1, groups, greet, 0)
    pl.semaphore_wait(barrier, 3 + groups - 1)
    ids[pl.ds(me, 1), pl.ds(y, 1), :] = ids_ref[...][None]
    line = []
    for k in range(1, 4):
        c = pltpu.make_async_remote_copy(ids_ref, ids.at[me, pl.ds(y, 1)], id_send.at[k - 1], id_recv.at[k - 1],
            device_id=place(me, (y + k) % 4), device_id_type=MESH)
        c.start(); line.append(c)

    for copy in copies:
        copy.wait()

    def turn(b, _):
        parts = []
        for strip in range(4):
            first = jnp.minimum(b * 128 + strip * STRIP, vocab - 128)
            parts.append(raw[:, pl.ds(pl.multiple_of(first, 128), 128)])
        block = jnp.concatenate(parts, axis=0)
        major[pl.ds(pl.multiple_of(b * 128, 128), 128), :] = block.T.astype(jnp.float32)
        return 0

    half = BLOCKS // 4
    lax.fori_loop(0, half, turn, 0, unroll=9)
    for c in line:
        c.wait()
    def spread(k, _):
        to = (me + k) % groups
        pltpu.make_async_remote_copy(ids.at[me], ids.at[me], id_send.at[3], id_recv.at[3],
            device_id=place(to, y), device_id_type=MESH).start()
        return 0
    lax.fori_loop(1, groups, spread, 0)
    lax.fori_loop(half, BLOCKS, turn, 0, unroll=9)
    others = pltpu.make_async_remote_copy(ids.at[pl.ds(0, groups - 1)], ids.at[pl.ds(0, groups - 1)], id_send.at[3], id_recv.at[3],
        device_id=place(me, up), device_id_type=MESH)
    others.wait_recv()
    all_ids = ids[...]
    strip_of = jnp.zeros_like(all_ids)
    for k in range(1, 4):
        strip_of = strip_of + jnp.where(all_ids >= k * STRIP, 1, 0)
    spots[...] = all_ids - strip_of * STRIP
    to_smem = pltpu.make_async_copy(spots, spots_s, spot_sem)
    to_smem.start()
    to_smem.wait()
    eye = (lax.broadcasted_iota(jnp.int32, (128, 128), 0) == lax.broadcasted_iota(jnp.int32, (128, 128), 1)).astype(jnp.bfloat16)

    def find(g, put):
        def some(s, _):
            for i in range(128):
                rows[pl.ds(s * 128 + i, 1), :] = major[pl.ds(spots_s[g, s, i], 1), :]
            return 0
        lax.fori_loop(0, 4, some, 0)
        found = lax.dot_general(eye, rows[...].astype(jnp.bfloat16), (((1,), (1,)), ((), ())), preferred_element_type=jnp.float32)
        for s in range(4):
            word = ids[pl.ds(g, 1), pl.ds(s, 1), :].reshape(1, 128)
            part = found[:, s * 128:(s + 1) * 128]
            chosen = part[:feats]
            for k in range(1, 4):
                chosen = jnp.where(word >= k * STRIP, part[k * feats:(k + 1) * feats], chosen)
            put(s, chosen.astype(jnp.bfloat16))

    def chunk(p, lo, n):
        zs = (z + 4 - p) % 4
        return pl.ds(zs * 8 + lo, n)

    def side(p, way, lo, n, of, to, slot):
        part = out_ref.at[chunk(p, lo, n), of]
        return pltpu.make_async_remote_copy(part, part, side_send.at[slot, p], side_recv.at[slot, p],
            device_id=place(me, to), device_id_type=MESH)

    def relay(p):
        side(p, 0, 0, 8, down, up, 0).wait_recv()
        side(p, 0, 0, 4, down, up, 2).start()
        side(p, 0, 0, 8, up, down, 1).wait_recv()
        side(p, 0, 4, 4, up, down, 3).start()

    for p in range(4):
        if p == 0:
            def put_own(s, val):
                out_ref[pl.ds(me, 1), pl.ds(y, 1), :, s * 128:(s + 1) * 128] = val[None, None]
            find(me, put_own)
        def one(e, _):
            to_z = (z + p) % 4
            to = ((to_z * 2 + (xlo + e // 4) % 2) * 2 + (core + e // 2) % 2) * 2 + (xhi + e) % 2
            def put(s, val):
                stage[p, pl.ds(e, 1), :, s * 128:(s + 1) * 128] = val[None]
            find(to, put)
            pltpu.make_async_remote_copy(stage.at[p, e], out_ref.at[me, y], far_send.at[p], far_recv.at[p],
                device_id=place(to, y), device_id_type=MESH).start()
            return 0
        lax.fori_loop(1 if p == 0 else 0, 8, one, 0)
        n = 7 if p == 0 else 8
        pltpu.make_async_remote_copy(stage.at[p, pl.ds(0, n)], out_ref.at[pl.ds(0, n), y], far_send.at[p], far_recv.at[p],
            device_id=place(me, up), device_id_type=MESH).wait_recv()
        side(p, 0, 0, 8, y, up, 0).start()
        side(p, 0, 0, 8, y, down, 1).start()
        if p:
            relay(p - 1)
    relay(3)
    others.wait_send()
    for p in range(4):
        n = 7 if p == 0 else 8
        pltpu.make_async_remote_copy(stage.at[p, pl.ds(0, n)], out_ref.at[pl.ds(0, n), y], far_send.at[p], far_recv.at[p],
            device_id=place(me, up), device_id_type=MESH).wait_send()
        side(p, 0, 0, 4, down, up, 2).wait_recv()
        side(p, 0, 4, 4, up, down, 3).wait_recv()
        side(p, 0, 0, 8, y, up, 0).wait_send()
        side(p, 0, 0, 8, y, down, 1).wait_send()
        side(p, 0, 0, 4, down, up, 2).wait_send()
        side(p, 0, 4, 4, up, down, 3).wait_send()


def front(table, ids):
    feats, vocab = table.shape
    return pl.pallas_call(
        front_kernel,
        out_shape=jax.ShapeDtypeStruct((32, 4, feats, 512), jnp.bfloat16),
        in_specs=[pl.BlockSpec(memory_space=pltpu.VMEM), pl.BlockSpec(memory_space=pl.ANY)],
        out_specs=pl.BlockSpec(memory_space=pltpu.VMEM),
        scratch_shapes=[
            pltpu.VMEM((feats, vocab), jnp.bfloat16),
            pltpu.VMEM((STRIP, 128), jnp.float32),
            pltpu.VMEM((512, 128), jnp.float32),
            pltpu.VMEM((32, 4, 128), jnp.int32),
            pltpu.VMEM((32, 4, 128), jnp.int32),
            pltpu.SMEM((32, 4, 128), jnp.int32),
            pltpu.VMEM((4, 8, feats, 512), jnp.bfloat16),
            pltpu.SemaphoreType.DMA((6,)),
            pltpu.SemaphoreType.DMA,
            pltpu.SemaphoreType.DMA((4,)),
            pltpu.SemaphoreType.DMA((4,)),
            pltpu.SemaphoreType.DMA((4,)),
            pltpu.SemaphoreType.DMA((4,)),
            pltpu.SemaphoreType.DMA((4, 4)),
            pltpu.SemaphoreType.DMA((4, 4)),
        ],
        compiler_params=pltpu.CompilerParams(vmem_limit_bytes=50 * 2**20, collective_id=0, has_side_effects=True),
        cost_estimate=pl.CostEstimate(flops=60_000_000_000, bytes_accessed=8_000_000, transcendentals=0),
    )(ids.reshape(1, 128), table)


def back_kernel(lens_ref, tokens_ref, gain_ref, cos_ref, sin_ref, w_ref, wo_ref, hidden_ref, cache_ref,
                turned, w, wo, x, normed, squares, q, k, v, attended, stage, mid, passed, final,
                load_sems, far_send, far_recv, near_send, near_recv, sum_send, sum_recv):
    z = lax.axis_index("z"); xlo = lax.axis_index("xlo"); core = lax.axis_index("core")
    xhi = lax.axis_index("xhi"); y = lax.axis_index("y")
    me = ((z * 2 + xlo) * 2 + core) * 2 + xhi
    width, prompt = turned.shape
    quarter = prompt // 4
    up = (y + 1) % 4
    down = (y + 3) % 4
    far = (y + 2) % 4

    def at(member):
        return (z, xlo, core, xhi, member)

    loads = [
        pltpu.make_async_copy(tokens_ref, turned, load_sems.at[0]),
        pltpu.make_async_copy(w_ref, w, load_sems.at[1]),
        pltpu.make_async_copy(wo_ref, wo, load_sems.at[2]),
    ]
    for load in loads:
        load.start()
    barrier = pltpu.get_barrier_semaphore()
    for member in (up, down):
        pl.semaphore_signal(barrier, inc=1, device_id=at(member), device_id_type=MESH)
    pl.semaphore_wait(barrier, 2)

    loads[0].wait()
    squares[...] = jnp.zeros_like(squares)

    def turn(c, _):
        cols = pl.ds(pl.multiple_of(c * 128, 128), 128)
        piece = turned[cols, :].T
        x[:, cols] = piece
        wide = piece.astype(jnp.float32)
        squares[...] += wide * wide
        return 0

    lax.fori_loop(0, width // 128, turn, 0, unroll=2)
    scale = lax.rsqrt(jnp.sum(squares[...], axis=1, keepdims=True) / width + norm_eps)
    squares[...] = jnp.broadcast_to(scale, squares.shape)

    def norm(c, _):
        cols = pl.ds(pl.multiple_of(c * 128, 128), 128)
        wide = x[:, cols].astype(jnp.float32) * squares[...] * gain_ref[:, cols]
        normed[:, cols] = wide.astype(jnp.bfloat16)
        return 0

    lax.fori_loop(0, width // 128, norm, 0, unroll=2)
    loads[1].wait()

    def rotated(part):
        return (part * cos_ref[...] + pltpu.roll(part, HD // 2, 1) * sin_ref[...]).astype(jnp.bfloat16)

    def query(i, _):
        b = i // 2
        cols = pl.ds(pl.multiple_of(i % 2 * 256, 256), 256)
        both = jnp.dot(normed[...], w[b, :, cols], preferred_element_type=jnp.float32)
        for h in range(2):
            q[pl.ds(i * 2 + h, 1)] = rotated(both[:, h * HD : (h + 1) * HD])[None]
        return 0

    lax.fori_loop(0, 4, query, 0)

    for b in range(2):
        both = jnp.dot(normed[...], w[b, :, 512:768], preferred_element_type=jnp.float32)
        key = rotated(both[:, :HD])
        value = both[:, HD:].astype(jnp.bfloat16)
        k[b] = key
        v[b] = value
        cache_ref[0, 0, :, b * HD : (b + 1) * HD] = key
        cache_ref[0, 1, :, b * HD : (b + 1) * HD] = value

    length = lens_ref[me]

    def head(h, _):
        b = h // 4
        for r in range(4):
            rows = slice(r * quarter, (r + 1) * quarter)
            keys = (r + 1) * quarter
            scores = lax.dot_general(q[h, rows, :], k[b, :keys, :], (((1,), (1,)), ((), ())), preferred_element_type=jnp.float32)
            scores = scores * np.float32(1 / np.sqrt(HD))
            p = lax.broadcasted_iota(jnp.int32, (quarter, keys), 0) + r * quarter
            j = lax.broadcasted_iota(jnp.int32, (quarter, keys), 1)
            scores = jnp.where((j <= p) & (j < length), scores, -1e30)
            expd = jnp.exp(scores - jnp.max(scores, axis=1, keepdims=True))
            weights = (expd / jnp.sum(expd, axis=1, keepdims=True)).astype(jnp.bfloat16)
            got = jnp.dot(weights, v[b, :keys, :], preferred_element_type=jnp.float32)
            attended[rows, pl.ds(pl.multiple_of(h * HD, HD), HD)] = got.astype(jnp.bfloat16)
        return 0

    lax.fori_loop(0, 8, head, 0)
    loads[2].wait()

    def send(src, dst, ssem, rsem, member):
        return pltpu.make_async_remote_copy(src, dst, ssem, rsem, device_id=at(member), device_id_type=MESH)

    def far_copy(c, way):
        return send(stage.at[c, far, way], mid.at[c, way], far_send.at[c, way], far_recv.at[c, way], down if way else up)

    def near_copy(c, way):
        return send(stage.at[c, down if way else up, 1 - way], final.at[c, way, 1 - way], near_send.at[c, way], near_recv.at[c, way], down if way else up)

    def sum_copy(c, way):
        return send(passed.at[c, way], final.at[c, way, way], sum_send.at[c, way], sum_recv.at[c, way], down if way else up)

    def pass_on(c):
        for way in range(2):
            far_copy(c, way).wait_recv()
            mine = stage[pl.ds(c, 1), pl.ds(down if way else up, 1), way].reshape(quarter, 256)
            passed[pl.ds(c, 1), way] = (mine.astype(jnp.float32) + mid[pl.ds(c, 1), way].reshape(quarter, 256).astype(jnp.float32)).astype(jnp.bfloat16)[None]
            sum_copy(c, way).start()

    def finish(c):
        for way in range(2):
            near_copy(c, way).wait_recv()
            sum_copy(c, way).wait_recv()
        own = pl.ds(pl.multiple_of(y * quarter, quarter), quarter)
        for half in range(2):
            cols = pl.ds(pl.multiple_of(c * 512 + half * 256, 256), 256)
            total = stage[pl.ds(c, 1), pl.ds(y, 1), half].reshape(quarter, 256).astype(jnp.float32)
            for way in range(2):
                total = total + final[pl.ds(c, 1), way, half].reshape(quarter, 256).astype(jnp.float32)
            hidden_ref[:, cols] = (x[own, cols].astype(jnp.float32) + total).astype(jnp.bfloat16)

    chunks = stage.shape[0]

    def project(c, _):
        for half in range(2):
            part = jnp.dot(attended[:, :512], wo[0, c * 2 + half], preferred_element_type=jnp.float32)
            part = part + jnp.dot(attended[:, 512:], wo[1, c * 2 + half], preferred_element_type=jnp.float32)
            part = part.astype(jnp.bfloat16)
            for member in range(4):
                stage[pl.ds(c, 1), member, half] = part[member * quarter : (member + 1) * quarter][None]
        for way in range(2):
            far_copy(c, way).start()
        for way in range(2):
            near_copy(c, way).start()

        @pl.when(c > 0)
        def _():
            pass_on(c - 1)

        return 0

    lax.fori_loop(0, chunks, project, 0)
    pass_on(chunks - 1)

    def last(c, _):
        finish(c)
        return 0

    lax.fori_loop(0, chunks, last, 0)

    def drain(c, _):
        for way in range(2):
            far_copy(c, way).wait_send()
            near_copy(c, way).wait_send()
            sum_copy(c, way).wait_send()
        return 0

    lax.fori_loop(0, chunks, drain, 0)


def back(lengths, tokens, gain, w, wo):
    width, prompt = tokens.shape
    quarter = prompt // 4
    angle = np.arange(prompt)[:, None] * rope_theta ** (-2.0 * np.arange(HD // 2) / HD)[None, :]
    cosine = np.concatenate([np.cos(angle), np.cos(angle)], axis=1).astype(np.float32)
    sine = np.concatenate([-np.sin(angle), np.sin(angle)], axis=1).astype(np.float32)
    chunks = width // 512
    bf = jnp.bfloat16
    vmem = pl.BlockSpec(memory_space=pltpu.VMEM)
    anyw = pl.BlockSpec(memory_space=pl.ANY)
    dma = pltpu.SemaphoreType.DMA
    return pl.pallas_call(
        back_kernel,
        out_shape=(
            jax.ShapeDtypeStruct((quarter, width), bf),
            jax.ShapeDtypeStruct((1, 2, prompt, 2 * HD), bf),
        ),
        in_specs=[pl.BlockSpec(memory_space=pltpu.SMEM), anyw, vmem, vmem, vmem, anyw, anyw],
        out_specs=(vmem, vmem),
        scratch_shapes=[
            pltpu.VMEM((width, prompt), bf),
            pltpu.VMEM(w.shape, bf),
            pltpu.VMEM(wo.shape, bf),
            pltpu.VMEM((prompt, width), bf),
            pltpu.VMEM((prompt, width), bf),
            pltpu.VMEM((prompt, 128), jnp.float32),
            pltpu.VMEM((8, prompt, HD), bf),
            pltpu.VMEM((2, prompt, HD), bf),
            pltpu.VMEM((2, prompt, HD), bf),
            pltpu.VMEM((prompt, 1024), bf),
            pltpu.VMEM((chunks, 4, 2, quarter, 256), bf),
            pltpu.VMEM((chunks, 2, quarter, 256), bf),
            pltpu.VMEM((chunks, 2, quarter, 256), bf),
            pltpu.VMEM((chunks, 2, 2, quarter, 256), bf),
            dma((3,)),
        ] + [dma((chunks, 2))] * 6,
        compiler_params=pltpu.CompilerParams(vmem_limit_bytes=58 * 2**20, collective_id=1, has_side_effects=True),
        cost_estimate=pl.CostEstimate(flops=60_000_000_000, bytes_accessed=30_000_000, transcendentals=0),
    )(lengths, tokens, gain.reshape(1, width), cosine, sine, w, wo)


def shards(prompt_ids, prompt_lengths, embed_table, norm_gain, w_query, w_key, w_value, w_out):
    row_count = prompt_ids.shape[0] * TPG
    model_width = embed_table.shape[0] * lax.axis_size(AXES)
    packed = jnp.concatenate([w_query, w_key, w_value], axis=1)
    plane = ("xhi", "z", "xlo", "core")
    wide = lax.all_gather(packed, plane, axis=0, tiled=True)
    wide = wide.reshape(2, model_width, packed.shape[1])
    out_wide = lax.all_gather(w_out, plane, axis=0, tiled=False)
    out_wide = out_wide.reshape(2, -1, *w_out.shape)
    tokens = front(embed_table, prompt_ids).reshape(model_width, row_count)
    return back(prompt_lengths, tokens, norm_gain, wide, out_wide)


def solution(mesh):
    split = Mesh(mesh.devices.reshape(4, 2, 2, 2, 4), AXES)
    placed = (
        P(AXES),
        P(),
        P(AXES, None),
        P(),
        P(DP, TENSOR),
        P(DP, TENSOR),
        P(DP, TENSOR),
        P(TENSOR, DP),
    )
    return jax.shard_map(
        shards,
        mesh=split,
        in_specs=placed,
        out_specs=(P(AXES, None), P(AXES, None, None, None)),
        check_vma=False,
    )
```

```python
import jax
import jax.numpy as jnp
import numpy as np
from jax import lax
from jax.experimental import pallas as pl
from jax.experimental.pallas import tpu as pltpu
from jax.sharding import Mesh
from jax.sharding import PartitionSpec as P

HD = 128
TPG = 4
AXES = ("z", "xlo", "core", "xhi", "y")
DP = ("z", "xlo", "core")
TENSOR = ("xhi", "y")

norm_eps = 1e-05
rope_theta = 500000.0

MESH = pl.DeviceIdType.MESH
BLOCKS = 252
STRIP = BLOCKS * 128

class Plane:
    def __init__(self, whole, own, sems):
        self.whole, self.own = whole, own
        self.send, self.recv, self.core_send, self.core_recv = sems
        self.z = lax.axis_index("z")
        self.xlo = lax.axis_index("xlo")
        self.core = lax.axis_index("core")
        self.xhi = lax.axis_index("xhi")
        self.y = lax.axis_index("y")
        self.x = self.xhi * 2 + self.xlo
        self.half = whole.shape[4] // 2

    def neighbours(self):
        found = []
        for cls in range(2):
            for way in range(2):
                found.append(self.device(cls, self.first(cls) + (3 if way else 1), self.second(cls)))
        found.append((self.z, self.xlo, 1 - self.core, self.xhi, self.y))
        return found

    def first(self, cls):
        return self.x if cls else self.z

    def second(self, cls):
        return self.z if cls else self.x

    def device(self, cls, f, s):
        f, s = f % 4, s % 4
        x, z = (f, s) if cls else (s, f)
        return (z, x % 2, self.core, x // 2, self.y)

    def rows(self, cls, part):
        if part is None:
            return pl.ds(cls * self.half, self.half)
        return pl.ds(cls * self.half + part * (self.half // 2), self.half // 2)

    def piece(self, cls, f, s, part=None):
        f, s = f % 4, s % 4
        x, z = (f, s) if cls else (s, f)
        return self.whole.at[x // 2, z, x % 2, self.core, self.rows(cls, part)]

    def copy(self, cls, stage, slot, f, s, part, own):
        step = 3 if slot % 2 else 1
        pf, ps = self.first(cls), self.second(cls)
        to = self.device(cls, pf + step, ps) if stage == 0 else self.device(cls, pf, ps + step)
        dst = self.piece(cls, f, s, part)
        src = self.own.at[self.rows(cls, part)] if own else dst
        return pltpu.make_async_remote_copy(
            src, dst, self.send.at[cls, stage, slot], self.recv.at[cls, stage, slot], device_id=to, device_id_type=MESH
        )

    def full(self, cls, stage, way):
        o = max(stage - 1, 0)
        return self.copy(cls, stage, way, self.first(cls) + o, self.second(cls), None, o == 0)

    def relay(self, cls, stage, way):
        step = 1 if way else 3
        f, s = self.first(cls), self.second(cls)
        if stage == 0:
            f = f + step
        else:
            f, s = f + stage - 1, s + step
        return self.copy(cls, stage, 2 + way, f, s, way, False)

    def cores(self, cls, o):
        s = (self.second(cls) + o) % 4
        if cls:
            ref = self.whole.at[:, s, :, self.core, self.rows(cls, None)]
        else:
            ref = self.whole.at[s // 2, :, s % 2, self.core, self.rows(cls, None)]
        return pltpu.make_async_remote_copy(
            ref,
            ref,
            self.core_send.at[cls, o],
            self.core_recv.at[cls, o],
            device_id=(self.z, self.xlo, 1 - self.core, self.xhi, self.y),
            device_id_type=MESH,
        )

    def each(self, act, *args):
        for cls in range(2):
            for way in range(2):
                act(cls, way, *args)

    def start_full(self, *stages):
        for stage in stages:
            self.each(lambda cls, way: self.full(cls, stage, way).start())

    def take_full(self, *stages):
        for stage in stages:
            self.each(lambda cls, way: self.full(cls, stage, way).wait_recv())
            self.each(lambda cls, way: self.relay(cls, stage, way).start())

    def take_relay(self, *stages):
        for stage in stages:
            self.each(lambda cls, way: self.relay(cls, stage, way).wait_recv())

    def step(self, n):
        if n == 0:
            self.start_full(0, 1)
        elif n == 1:
            self.take_full(0)
            self.start_full(2, 4)
        elif n == 2:
            self.take_relay(0)
            self.start_full(3)
            self.take_full(1)
        elif n == 3:
            for cls in range(2):
                self.cores(cls, 0).start()
            self.take_full(2, 4)
        elif n == 4:
            self.take_full(3)
            for o in (1, 3):
                for cls in range(2):
                    self.cores(cls, o).start()
        elif n == 5:
            self.take_relay(1, 2, 3, 4)
            for cls in range(2):
                self.cores(cls, 2).start()
        else:
            for cls in range(2):
                for o in range(4):
                    self.cores(cls, o).wait()
            for stage in range(5):
                self.each(lambda cls, way: self.full(cls, stage, way).wait_send())
                self.each(lambda cls, way: self.relay(cls, stage, way).wait_send())

    @staticmethod
    def sems():
        dma = pltpu.SemaphoreType.DMA
        return [dma((2, 5, 4)), dma((2, 5, 4)), dma((2, 4)), dma((2, 4))]


def place(g, y):
    return (g // 8, g // 4 % 2, g // 2 % 2, g % 2, y)

def front_kernel(ids_ref, table_ref, wq_ref, wk_ref, wv_ref, out_ref, whole_ref, raw, major, rows, ids, spots, spots_s, stage, own,
                 table_sems, spot_sem, own_sems, id_send, id_recv, far_send, far_recv, side_send, side_recv, *plane_sems):
    feats, vocab = table_ref.shape
    z = lax.axis_index("z"); xlo = lax.axis_index("xlo"); core = lax.axis_index("core")
    xhi = lax.axis_index("xhi"); y = lax.axis_index("y")
    me = ((z * 2 + xlo) * 2 + core) * 2 + xhi
    groups = out_ref.shape[0]
    up = (y + 1) % 4
    down = (y + 3) % 4
    plane = Plane(whole_ref, own, plane_sems)
    mine = [
        pltpu.make_async_copy(ref, own.at[:, pl.ds(first, ref.shape[1])], own_sems.at[k])
        for k, (ref, first) in enumerate(((wq_ref, 0), (wk_ref, 512), (wv_ref, 640)))
    ]
    for copy in mine:
        copy.start()
    tiles = vocab // 128
    count = table_sems.shape[0]
    ends = [tiles * k // count for k in range(count + 1)]
    copies = []
    for k in range(count):
        part = pl.ds(ends[k] * 128, (ends[k + 1] - ends[k]) * 128)
        copies.append(pltpu.make_async_copy(table_ref.at[:, part], raw.at[:, part], table_sems.at[k]))
    for copy in copies:
        copy.start()
    barrier = pltpu.get_barrier_semaphore()
    for k in range(1, 4):
        pl.semaphore_signal(barrier, inc=1, device_id=place(me, (y + k) % 4), device_id_type=MESH)
    def greet(k, _):
        pl.semaphore_signal(barrier, inc=1, device_id=place((me + k) % groups, y), device_id_type=MESH)
        return 0
    lax.fori_loop(1, groups, greet, 0)
    pl.semaphore_wait(barrier, 3 + groups - 1)
    ids[pl.ds(me, 1), pl.ds(y, 1), :] = ids_ref[...][None]
    line = []
    for k in range(1, 4):
        c = pltpu.make_async_remote_copy(ids_ref, ids.at[me, pl.ds(y, 1)], id_send.at[k - 1], id_recv.at[k - 1],
            device_id=place(me, (y + k) % 4), device_id_type=MESH)
        c.start()
        line.append(c)
    for copy in mine:
        copy.wait()
    keep = pltpu.make_async_copy(own, whole_ref.at[xhi, z, xlo, core], own_sems.at[3])
    keep.start()
    plane.step(0)
    for copy in copies:
        copy.wait()

    def turn(b, _):
        parts = []
        for strip in range(4):
            first = jnp.minimum(b * 128 + strip * STRIP, vocab - 128)
            parts.append(raw[:, pl.ds(pl.multiple_of(first, 128), 128)])
        block = jnp.concatenate(parts, axis=0)
        major[pl.ds(pl.multiple_of(b * 128, 128), 128), :] = block.T.astype(jnp.float32)
        return 0

    def spread(k, _):
        to = (me + k) % groups
        pltpu.make_async_remote_copy(ids.at[me], ids.at[me], id_send.at[3], id_recv.at[3],
            device_id=place(to, y), device_id_type=MESH).start()
        return 0

    for part in range(4):
        lax.fori_loop(BLOCKS // 4 * part, BLOCKS // 4 * (part + 1), turn, 0, unroll=9)
        if part == 0:
            for c in line:
                c.wait()
            lax.fori_loop(1, groups, spread, 0)
        elif part == 1:
            plane.step(1)
        elif part == 3:
            plane.step(2)
            keep.wait()
    others = pltpu.make_async_remote_copy(ids.at[pl.ds(0, groups - 1)], ids.at[pl.ds(0, groups - 1)], id_send.at[3], id_recv.at[3],
        device_id=place(me, up), device_id_type=MESH)
    others.wait_recv()
    all_ids = ids[...]
    strip_of = jnp.zeros_like(all_ids)
    for k in range(1, 4):
        strip_of = strip_of + jnp.where(all_ids >= k * STRIP, 1, 0)
    spots[...] = all_ids - strip_of * STRIP
    to_smem = pltpu.make_async_copy(spots, spots_s, spot_sem)
    to_smem.start()
    to_smem.wait()
    eye = (lax.broadcasted_iota(jnp.int32, (128, 128), 0) == lax.broadcasted_iota(jnp.int32, (128, 128), 1)).astype(jnp.bfloat16)

    def find(g, put):
        def some(s, _):
            for i in range(128):
                rows[pl.ds(s * 128 + i, 1), :] = major[pl.ds(spots_s[g, s, i], 1), :]
            return 0
        lax.fori_loop(0, 4, some, 0)
        found = lax.dot_general(eye, rows[...].astype(jnp.bfloat16), (((1,), (1,)), ((), ())), preferred_element_type=jnp.float32)
        for s in range(4):
            word = ids[pl.ds(g, 1), pl.ds(s, 1), :].reshape(1, 128)
            part = found[:, s * 128:(s + 1) * 128]
            chosen = part[:feats]
            for k in range(1, 4):
                chosen = jnp.where(word >= k * STRIP, part[k * feats:(k + 1) * feats], chosen)
            put(s, chosen.astype(jnp.bfloat16))

    def chunk(p, lo, n):
        zs = (z + 4 - p) % 4
        return pl.ds(zs * 8 + lo, n)

    def side(p, way, lo, n, of, to, slot):
        part = out_ref.at[chunk(p, lo, n), of]
        return pltpu.make_async_remote_copy(part, part, side_send.at[slot, p], side_recv.at[slot, p],
            device_id=place(me, to), device_id_type=MESH)

    def relay(p):
        side(p, 0, 0, 8, down, up, 0).wait_recv()
        side(p, 0, 0, 4, down, up, 2).start()
        side(p, 0, 0, 8, up, down, 1).wait_recv()
        side(p, 0, 4, 4, up, down, 3).start()

    for p in range(4):
        if p == 0:
            def put_own(s, val):
                out_ref[pl.ds(me, 1), pl.ds(y, 1), :, s * 128:(s + 1) * 128] = val[None, None]
            find(me, put_own)
        def one(e, _):
            to_z = (z + p) % 4
            to = ((to_z * 2 + (xlo + e // 4) % 2) * 2 + (core + e // 2) % 2) * 2 + (xhi + e) % 2
            def put(s, val):
                stage[p, pl.ds(e, 1), :, s * 128:(s + 1) * 128] = val[None]
            find(to, put)
            pltpu.make_async_remote_copy(stage.at[p, e], out_ref.at[me, y], far_send.at[p], far_recv.at[p],
                device_id=place(to, y), device_id_type=MESH).start()
            return 0
        lax.fori_loop(1 if p == 0 else 0, 8, one, 0)
        n = 7 if p == 0 else 8
        pltpu.make_async_remote_copy(stage.at[p, pl.ds(0, n)], out_ref.at[pl.ds(0, n), y], far_send.at[p], far_recv.at[p],
            device_id=place(me, up), device_id_type=MESH).wait_recv()
        side(p, 0, 0, 8, y, up, 0).start()
        side(p, 0, 0, 8, y, down, 1).start()
        if p:
            relay(p - 1)
        if p < 3:
            plane.step(3 + p)
    relay(3)
    others.wait_send()
    plane.step(6)
    for p in range(4):
        n = 7 if p == 0 else 8
        pltpu.make_async_remote_copy(stage.at[p, pl.ds(0, n)], out_ref.at[pl.ds(0, n), y], far_send.at[p], far_recv.at[p],
            device_id=place(me, up), device_id_type=MESH).wait_send()
        side(p, 0, 0, 4, down, up, 2).wait_recv()
        side(p, 0, 4, 4, up, down, 3).wait_recv()
        side(p, 0, 0, 8, y, up, 0).wait_send()
        side(p, 0, 0, 8, y, down, 1).wait_send()
        side(p, 0, 0, 4, down, up, 2).wait_send()
        side(p, 0, 4, 4, up, down, 3).wait_send()


def front(table, ids, wq, wk, wv):
    feats, vocab = table.shape
    depth, across = wq.shape[0], wq.shape[1] + wk.shape[1] + wv.shape[1]
    return pl.pallas_call(
        front_kernel,
        out_shape=(
            jax.ShapeDtypeStruct((32, 4, feats, 512), jnp.bfloat16),
            jax.ShapeDtypeStruct((2, 4, 2, 2, depth, across), jnp.bfloat16),
        ),
        in_specs=[pl.BlockSpec(memory_space=pltpu.VMEM)] + [pl.BlockSpec(memory_space=pl.ANY)] * 4,
        out_specs=(pl.BlockSpec(memory_space=pltpu.VMEM), pl.BlockSpec(memory_space=pl.ANY)),
        scratch_shapes=[
            pltpu.VMEM((feats, vocab), jnp.bfloat16),
            pltpu.VMEM((STRIP, 128), jnp.float32),
            pltpu.VMEM((512, 128), jnp.float32),
            pltpu.VMEM((32, 4, 128), jnp.int32),
            pltpu.VMEM((32, 4, 128), jnp.int32),
            pltpu.SMEM((32, 4, 128), jnp.int32),
            pltpu.VMEM((4, 8, feats, 512), jnp.bfloat16),
            pltpu.VMEM((depth, across), jnp.bfloat16),
            pltpu.SemaphoreType.DMA((6,)),
            pltpu.SemaphoreType.DMA,
            pltpu.SemaphoreType.DMA((4,)),
            pltpu.SemaphoreType.DMA((4,)),
            pltpu.SemaphoreType.DMA((4,)),
            pltpu.SemaphoreType.DMA((4,)),
            pltpu.SemaphoreType.DMA((4,)),
            pltpu.SemaphoreType.DMA((4, 4)),
            pltpu.SemaphoreType.DMA((4, 4)),
        ] + Plane.sems(),
        compiler_params=pltpu.CompilerParams(vmem_limit_bytes=50 * 2**20, collective_id=0, has_side_effects=True),
        cost_estimate=pl.CostEstimate(flops=60_000_000_000, bytes_accessed=8_000_000, transcendentals=0),
    )(ids.reshape(1, 128), table, wq, wk, wv)


def back_kernel(lens_ref, tokens_ref, gain_ref, cos_ref, sin_ref, w_ref, wo_ref, hidden_ref, cache_ref,
                turned, w, wo, x, normed, squares, q, k, v, attended, stage, mid, passed, final,
                load_sems, far_send, far_recv, near_send, near_recv, sum_send, sum_recv, *plane_sems):
    z = lax.axis_index("z"); xlo = lax.axis_index("xlo"); core = lax.axis_index("core")
    xhi = lax.axis_index("xhi"); y = lax.axis_index("y")
    me = ((z * 2 + xlo) * 2 + core) * 2 + xhi
    width, prompt = turned.shape
    quarter = prompt // 4
    up = (y + 1) % 4
    down = (y + 3) % 4
    far = (y + 2) % 4

    def at(member):
        return (z, xlo, core, xhi, member)

    loads = [
        pltpu.make_async_copy(tokens_ref, turned, load_sems.at[0]),
        pltpu.make_async_copy(w_ref, w, load_sems.at[1]),
        pltpu.make_async_copy(wo_ref, wo.at[xhi, z, xlo, core], load_sems.at[2]),
    ]
    plane = Plane(wo, wo.at[xhi, z, xlo, core], plane_sems)
    for load in loads:
        load.start()
    barrier = pltpu.get_barrier_semaphore()
    greeted = [at(up), at(down)] + plane.neighbours()
    for device in greeted:
        pl.semaphore_signal(barrier, inc=1, device_id=device, device_id_type=MESH)
    pl.semaphore_wait(barrier, len(greeted))
    loads[2].wait()
    plane.step(0)

    loads[0].wait()
    squares[...] = jnp.zeros_like(squares)

    def turn(c, _):
        cols = pl.ds(pl.multiple_of(c * 128, 128), 128)
        piece = turned[cols, :].T
        x[:, cols] = piece
        wide = piece.astype(jnp.float32)
        squares[...] += wide * wide
        return 0

    lax.fori_loop(0, width // 128, turn, 0, unroll=2)
    plane.step(1)
    scale = lax.rsqrt(jnp.sum(squares[...], axis=1, keepdims=True) / width + norm_eps)
    squares[...] = jnp.broadcast_to(scale, squares.shape)

    def norm(c, _):
        cols = pl.ds(pl.multiple_of(c * 128, 128), 128)
        wide = x[:, cols].astype(jnp.float32) * squares[...] * gain_ref[:, cols]
        normed[:, cols] = wide.astype(jnp.bfloat16)
        return 0

    lax.fori_loop(0, width // 128, norm, 0, unroll=2)
    loads[1].wait()
    plane.step(2)

    def rotated(part):
        return (part * cos_ref[...] + pltpu.roll(part, HD // 2, 1) * sin_ref[...]).astype(jnp.bfloat16)

    def query(i, _):
        b = i // 2
        cols = pl.ds(pl.multiple_of(i % 2 * 256, 256), 256)
        both = jnp.dot(normed[...], w[b, :, cols], preferred_element_type=jnp.float32)
        for h in range(2):
            q[pl.ds(i * 2 + h, 1)] = rotated(both[:, h * HD : (h + 1) * HD])[None]
        return 0

    lax.fori_loop(0, 2, query, 0)
    plane.step(3)
    lax.fori_loop(2, 4, query, 0)
    plane.step(4)

    for b in range(2):
        both = jnp.dot(normed[...], w[b, :, 512:768], preferred_element_type=jnp.float32)
        key = rotated(both[:, :HD])
        value = both[:, HD:].astype(jnp.bfloat16)
        k[b] = key
        v[b] = value
        cache_ref[0, 0, :, b * HD : (b + 1) * HD] = key
        cache_ref[0, 1, :, b * HD : (b + 1) * HD] = value

    plane.step(5)
    length = lens_ref[me]

    def head(h, _):
        b = h // 4
        for r in range(4):
            rows = slice(r * quarter, (r + 1) * quarter)
            keys = (r + 1) * quarter
            scores = lax.dot_general(q[h, rows, :], k[b, :keys, :], (((1,), (1,)), ((), ())), preferred_element_type=jnp.float32)
            scores = scores * np.float32(1 / np.sqrt(HD))
            p = lax.broadcasted_iota(jnp.int32, (quarter, keys), 0) + r * quarter
            j = lax.broadcasted_iota(jnp.int32, (quarter, keys), 1)
            scores = jnp.where((j <= p) & (j < length), scores, -1e30)
            expd = jnp.exp(scores - jnp.max(scores, axis=1, keepdims=True))
            weights = (expd / jnp.sum(expd, axis=1, keepdims=True)).astype(jnp.bfloat16)
            got = jnp.dot(weights, v[b, :keys, :], preferred_element_type=jnp.float32)
            attended[rows, pl.ds(pl.multiple_of(h * HD, HD), HD)] = got.astype(jnp.bfloat16)
        return 0

    lax.fori_loop(0, 8, head, 0)
    plane.step(6)

    def send(src, dst, ssem, rsem, member):
        return pltpu.make_async_remote_copy(src, dst, ssem, rsem, device_id=at(member), device_id_type=MESH)

    def far_copy(c, way):
        return send(stage.at[c, far, way], mid.at[c, way], far_send.at[c, way], far_recv.at[c, way], down if way else up)

    def near_copy(c, way):
        return send(stage.at[c, down if way else up, 1 - way], final.at[c, way, 1 - way], near_send.at[c, way], near_recv.at[c, way], down if way else up)

    def sum_copy(c, way):
        return send(passed.at[c, way], final.at[c, way, way], sum_send.at[c, way], sum_recv.at[c, way], down if way else up)

    def pass_on(c):
        for way in range(2):
            far_copy(c, way).wait_recv()
            mine = stage[pl.ds(c, 1), pl.ds(down if way else up, 1), way].reshape(quarter, 256)
            passed[pl.ds(c, 1), way] = (mine.astype(jnp.float32) + mid[pl.ds(c, 1), way].reshape(quarter, 256).astype(jnp.float32)).astype(jnp.bfloat16)[None]
            sum_copy(c, way).start()

    def finish(c):
        for way in range(2):
            near_copy(c, way).wait_recv()
            sum_copy(c, way).wait_recv()
        own = pl.ds(pl.multiple_of(y * quarter, quarter), quarter)
        for half in range(2):
            cols = pl.ds(pl.multiple_of(c * 512 + half * 256, 256), 256)
            total = stage[pl.ds(c, 1), pl.ds(y, 1), half].reshape(quarter, 256).astype(jnp.float32)
            for way in range(2):
                total = total + final[pl.ds(c, 1), way, half].reshape(quarter, 256).astype(jnp.float32)
            hidden_ref[:, cols] = (x[own, cols].astype(jnp.float32) + total).astype(jnp.bfloat16)

    chunks = stage.shape[0]

    def project(c, _):
        for half in range(2):
            part = jnp.dot(attended[:, :512], wo[0, c // 2, c % 2, half], preferred_element_type=jnp.float32)
            part = part + jnp.dot(attended[:, 512:], wo[1, c // 2, c % 2, half], preferred_element_type=jnp.float32)
            part = part.astype(jnp.bfloat16)
            for member in range(4):
                stage[pl.ds(c, 1), member, half] = part[member * quarter : (member + 1) * quarter][None]
        for way in range(2):
            far_copy(c, way).start()
        for way in range(2):
            near_copy(c, way).start()

        @pl.when(c > 0)
        def _():
            pass_on(c - 1)

        return 0

    lax.fori_loop(0, chunks, project, 0)
    pass_on(chunks - 1)

    def last(c, _):
        finish(c)
        return 0

    lax.fori_loop(0, chunks, last, 0)

    def drain(c, _):
        for way in range(2):
            far_copy(c, way).wait_send()
            near_copy(c, way).wait_send()
            sum_copy(c, way).wait_send()
        return 0

    lax.fori_loop(0, chunks, drain, 0)


def back(lengths, tokens, gain, w, wo):
    width, prompt = tokens.shape
    quarter = prompt // 4
    angle = np.arange(prompt)[:, None] * rope_theta ** (-2.0 * np.arange(HD // 2) / HD)[None, :]
    cosine = np.concatenate([np.cos(angle), np.cos(angle)], axis=1).astype(np.float32)
    sine = np.concatenate([-np.sin(angle), np.sin(angle)], axis=1).astype(np.float32)
    chunks = width // 512
    bf = jnp.bfloat16
    vmem = pl.BlockSpec(memory_space=pltpu.VMEM)
    anyw = pl.BlockSpec(memory_space=pl.ANY)
    dma = pltpu.SemaphoreType.DMA
    return pl.pallas_call(
        back_kernel,
        out_shape=(
            jax.ShapeDtypeStruct((quarter, width), bf),
            jax.ShapeDtypeStruct((1, 2, prompt, 2 * HD), bf),
        ),
        in_specs=[pl.BlockSpec(memory_space=pltpu.SMEM), anyw, vmem, vmem, vmem, anyw, anyw],
        out_specs=(vmem, vmem),
        scratch_shapes=[
            pltpu.VMEM((width, prompt), bf),
            pltpu.VMEM(w.shape, bf),
            pltpu.VMEM((2, 4, 2, 2, *wo.shape), bf),
            pltpu.VMEM((prompt, width), bf),
            pltpu.VMEM((prompt, width), bf),
            pltpu.VMEM((prompt, 128), jnp.float32),
            pltpu.VMEM((8, prompt, HD), bf),
            pltpu.VMEM((2, prompt, HD), bf),
            pltpu.VMEM((2, prompt, HD), bf),
            pltpu.VMEM((prompt, 1024), bf),
            pltpu.VMEM((chunks, 4, 2, quarter, 256), bf),
            pltpu.VMEM((chunks, 2, quarter, 256), bf),
            pltpu.VMEM((chunks, 2, quarter, 256), bf),
            pltpu.VMEM((chunks, 2, 2, quarter, 256), bf),
            dma((3,)),
        ] + [dma((chunks, 2))] * 6 + Plane.sems(),
        compiler_params=pltpu.CompilerParams(vmem_limit_bytes=58 * 2**20, collective_id=1, has_side_effects=True),
        cost_estimate=pl.CostEstimate(flops=60_000_000_000, bytes_accessed=30_000_000, transcendentals=0),
    )(lengths, tokens, gain.reshape(1, width), cosine, sine, w, wo)


def shards(prompt_ids, prompt_lengths, embed_table, norm_gain, w_query, w_key, w_value, w_out):
    row_count = prompt_ids.shape[0] * TPG
    model_width = embed_table.shape[0] * lax.axis_size(AXES)
    tokens, wide = front(embed_table, prompt_ids, w_query, w_key, w_value)
    tokens = tokens.reshape(model_width, row_count)
    wide = wide.reshape(2, model_width, wide.shape[-1])
    return back(prompt_lengths, tokens, norm_gain, wide, w_out)


def solution(mesh):
    split = Mesh(mesh.devices.reshape(4, 2, 2, 2, 4), AXES)
    placed = (
        P(AXES),
        P(),
        P(AXES, None),
        P(),
        P(DP, TENSOR),
        P(DP, TENSOR),
        P(DP, TENSOR),
        P(TENSOR, DP),
    )
    return jax.shard_map(
        shards,
        mesh=split,
        in_specs=placed,
        out_specs=(P(AXES, None), P(AXES, None, None, None)),
        check_vma=False,
    )
```

```python
import jax
import jax.numpy as jnp
import numpy as np
from jax import lax
from jax.experimental import pallas as pl
from jax.experimental.pallas import tpu as pltpu
from jax.sharding import Mesh
from jax.sharding import PartitionSpec as P

HD = 128
AXES = ("z", "xlo", "core", "xhi", "y")
DP = ("z", "xlo", "core")
TENSOR = ("xhi", "y")
MESH = pl.DeviceIdType.MESH

norm_eps = 1e-05
rope_theta = 500000.0

BLOCKS = 252
STRIP = BLOCKS * 128
TILES = 21
LOADS = BLOCKS // TILES


class Plane:
    def __init__(self, whole, own, sems):
        self.whole, self.own = whole, own
        self.send, self.recv, self.core_send, self.core_recv = sems
        self.z = lax.axis_index("z")
        self.xlo = lax.axis_index("xlo")
        self.core = lax.axis_index("core")
        self.xhi = lax.axis_index("xhi")
        self.y = lax.axis_index("y")
        self.x = self.xhi * 2 + self.xlo
        self.half = whole.shape[4] // 2

    def neighbours(self):
        found = []
        for cls in range(2):
            for way in range(2):
                found.append(self.device(cls, self.first(cls) + (3 if way else 1), self.second(cls)))
        found.append((self.z, self.xlo, 1 - self.core, self.xhi, self.y))
        return found

    def first(self, cls):
        return self.x if cls else self.z

    def second(self, cls):
        return self.z if cls else self.x

    def device(self, cls, f, s):
        f, s = f % 4, s % 4
        x, z = (f, s) if cls else (s, f)
        return (z, x % 2, self.core, x // 2, self.y)

    def rows(self, cls, part):
        if part is None:
            return pl.ds(cls * self.half, self.half)
        return pl.ds(cls * self.half + part * (self.half // 2), self.half // 2)

    def piece(self, cls, f, s, part=None):
        f, s = f % 4, s % 4
        x, z = (f, s) if cls else (s, f)
        return self.whole.at[x // 2, z, x % 2, self.core, self.rows(cls, part)]

    def copy(self, cls, stage, slot, f, s, part, own):
        step = 3 if slot % 2 else 1
        pf, ps = self.first(cls), self.second(cls)
        to = self.device(cls, pf + step, ps) if stage == 0 else self.device(cls, pf, ps + step)
        dst = self.piece(cls, f, s, part)
        src = self.own.at[self.rows(cls, part)] if own else dst
        return pltpu.make_async_remote_copy(
            src, dst, self.send.at[cls, stage, slot], self.recv.at[cls, stage, slot], device_id=to, device_id_type=MESH
        )

    def full(self, cls, stage, way):
        o = max(stage - 1, 0)
        return self.copy(cls, stage, way, self.first(cls) + o, self.second(cls), None, o == 0)

    def relay(self, cls, stage, way):
        step = 1 if way else 3
        f, s = self.first(cls), self.second(cls)
        if stage == 0:
            f = f + step
        else:
            f, s = f + stage - 1, s + step
        return self.copy(cls, stage, 2 + way, f, s, way, False)

    def cores(self, cls, o):
        s = (self.second(cls) + o) % 4
        if cls:
            ref = self.whole.at[:, s, :, self.core, self.rows(cls, None)]
        else:
            ref = self.whole.at[s // 2, :, s % 2, self.core, self.rows(cls, None)]
        return pltpu.make_async_remote_copy(
            ref,
            ref,
            self.core_send.at[cls, o],
            self.core_recv.at[cls, o],
            device_id=(self.z, self.xlo, 1 - self.core, self.xhi, self.y),
            device_id_type=MESH,
        )

    def each(self, act, *args):
        for cls in range(2):
            for way in range(2):
                act(cls, way, *args)

    def start_full(self, *stages):
        for stage in stages:
            self.each(lambda cls, way: self.full(cls, stage, way).start())

    def take_full(self, *stages):
        for stage in stages:
            self.each(lambda cls, way: self.full(cls, stage, way).wait_recv())
            self.each(lambda cls, way: self.relay(cls, stage, way).start())

    def take_relay(self, *stages):
        for stage in stages:
            self.each(lambda cls, way: self.relay(cls, stage, way).wait_recv())

    def step(self, n):
        if n == 0:
            self.start_full(0, 1)
        elif n == 1:
            self.take_full(0)
            self.start_full(2, 4)
        elif n == 2:
            self.take_relay(0)
            self.start_full(3)
            self.take_full(1)
        elif n == 3:
            for cls in range(2):
                self.cores(cls, 0).start()
            self.take_full(2, 4)
        elif n == 4:
            self.take_full(3)
            for o in (1, 3):
                for cls in range(2):
                    self.cores(cls, o).start()
        elif n == 5:
            self.take_relay(1, 2, 3, 4)
            for cls in range(2):
                self.cores(cls, 2).start()
        else:
            for cls in range(2):
                for o in range(4):
                    self.cores(cls, o).wait()
            for stage in range(5):
                self.each(lambda cls, way: self.full(cls, stage, way).wait_send())
                self.each(lambda cls, way: self.relay(cls, stage, way).wait_send())

    @staticmethod
    def sems():
        dma = pltpu.SemaphoreType.DMA
        return [dma((2, 5, 4)), dma((2, 5, 4)), dma((2, 4)), dma((2, 4))]


def place(g, y):
    return (g // 8, g // 4 % 2, g // 2 % 2, g % 2, y)


def kernel(lens_ref, ids_ref, gain_ref, cos_ref, sin_ref, table_ref, wq_ref, wk_ref, wv_ref, wo_ref, hidden_ref, cache_ref,
           raw, major, rows, ids, spots, spots_s, staged, xt, w, wo, own_x, xb, normed, squares, q, k, v, attended,
           stage, mid, passed, final, table_sems, spot_sem, own_sems, id_send, id_recv, look_send, look_recv,
           side_send, side_recv, far_send, far_recv, near_send, near_recv, sum_send, sum_recv, *plane_sems):
    feats, vocab = table_ref.shape
    z = lax.axis_index("z")
    xlo = lax.axis_index("xlo")
    core = lax.axis_index("core")
    xhi = lax.axis_index("xhi")
    y = lax.axis_index("y")
    me = ((z * 2 + xlo) * 2 + core) * 2 + xhi
    groups = ids.shape[0]
    quarter, width = hidden_ref.shape
    up = (y + 1) % 4
    down = (y + 3) % 4
    far = (y + 2) % 4
    tiles = vocab // 128

    def at(member):
        return place(me, member)

    def send(src, dst, ssem, rsem, device):
        return pltpu.make_async_remote_copy(src, dst, ssem, rsem, device_id=device, device_id_type=MESH)


    def table_base(n, strip):
        return jnp.minimum(strip * BLOCKS + n * TILES, tiles - TILES)

    def table_copy(n, strip):
        first = pl.multiple_of(table_base(n, strip) * 128, 128)
        return pltpu.make_async_copy(
            table_ref.at[:, pl.ds(first, TILES * 128)], raw.at[n % 2, strip], table_sems.at[n % 2, strip]
        )

    for n in range(2):
        for strip in range(4):
            table_copy(n, strip).start()
    own_w = w.at[xhi, z, xlo, core]
    own_wo = wo.at[xhi, z, xlo, core]
    mine = [
        pltpu.make_async_copy(ref, own_w.at[:, pl.ds(first, ref.shape[1])], own_sems.at[n])
        for n, (ref, first) in enumerate(((wq_ref, 0), (wk_ref, 512), (wv_ref, 640)))
    ] + [pltpu.make_async_copy(wo_ref, own_wo, own_sems.at[3])]
    for copy in mine:
        copy.start()
    plane_w = Plane(w, own_w, plane_sems[:4])
    plane_o = Plane(wo, own_wo, plane_sems[4:])

    barrier = pltpu.get_barrier_semaphore()
    for n in range(1, 4):
        pl.semaphore_signal(barrier, inc=1, device_id=at((y + n) % 4), device_id_type=MESH)

    def greet(n, _):
        pl.semaphore_signal(barrier, inc=1, device_id=place((me + n) % groups, y), device_id_type=MESH)
        return 0

    lax.fori_loop(1, groups, greet, 0)

    def turn(n, _):
        for strip in range(4):
            table_copy(n, strip).wait()

        def tile(t, _):
            parts = []
            for strip in range(4):
                first = jnp.minimum(strip * BLOCKS + n * TILES + t, tiles - 1) - table_base(n, strip)
                parts.append(raw[n % 2, strip, :, pl.ds(pl.multiple_of(first * 128, 128), 128)])
            block = jnp.concatenate(parts, axis=0)
            major[pl.ds(pl.multiple_of((n * TILES + t) * 128, 128), 128), :] = block.T.astype(jnp.float32)
            return 0

        lax.fori_loop(0, TILES, tile, 0, unroll=7)

        @pl.when(n + 2 < LOADS)
        def _():
            for strip in range(4):
                table_copy(n + 2, strip).start()

        return 0

    lax.fori_loop(0, 3, turn, 0)
    pl.semaphore_wait(barrier, 3 + groups - 1)
    ids[pl.ds(me, 1), pl.ds(y, 1), :] = ids_ref[...][None]
    line = [
        send(ids_ref, ids.at[me, pl.ds(y, 1)], id_send.at[n - 1], id_recv.at[n - 1], at((y + n) % 4)) for n in range(1, 4)
    ]
    for copy in line:
        copy.start()
    for copy in mine:
        copy.wait()
    plane_w.step(0)
    lax.fori_loop(3, 6, turn, 0)
    for copy in line:
        copy.wait()

    def spread(n, _):
        send(ids.at[me], ids.at[me], id_send.at[3], id_recv.at[3], place((me + n) % groups, y)).start()
        return 0

    lax.fori_loop(1, groups, spread, 0)
    lax.fori_loop(6, 9, turn, 0)
    plane_w.step(1)
    lax.fori_loop(9, LOADS, turn, 0)
    most = pl.ds(0, groups - 1)
    others = send(ids.at[most], ids.at[most], id_send.at[3], id_recv.at[3], at(up))
    others.wait_recv()
    all_ids = ids[...]
    strip_of = jnp.zeros_like(all_ids)
    for n in range(1, 4):
        strip_of = strip_of + jnp.where(all_ids >= n * STRIP, 1, 0)
    spots[...] = all_ids - strip_of * STRIP
    to_smem = pltpu.make_async_copy(spots, spots_s, spot_sem)
    to_smem.start()
    to_smem.wait()
    eye = (
        lax.broadcasted_iota(jnp.int32, (128, 128), 0) == lax.broadcasted_iota(jnp.int32, (128, 128), 1)
    ).astype(jnp.bfloat16)


    def look(s):
        def four(j, _):
            def some(i, _):
                g = (me + 4 * j + i) % groups
                for n in range(128):
                    rows[pl.ds(i * 128 + n, 1), :] = major[pl.ds(spots_s[g, s, n], 1), :]
                return 0

            lax.fori_loop(0, 4, some, 0)
            found = lax.dot_general(
                eye, rows[...].astype(jnp.bfloat16), (((1,), (1,)), ((), ())), preferred_element_type=jnp.float32
            )
            for i in range(4):
                g = (me + 4 * j + i) % groups
                word = ids[pl.ds(g, 1), pl.ds(s, 1), :].reshape(1, 128)
                part = found[:, i * 128 : (i + 1) * 128]
                chosen = part[:feats]
                for n in range(1, 4):
                    chosen = jnp.where(word >= n * STRIP, part[n * feats : (n + 1) * feats], chosen)
                chosen = chosen.astype(jnp.bfloat16)
                staged[s, pl.ds(4 * j + i, 1)] = chosen[None]

                def give():
                    send(staged.at[s, 4 * j + i], xt.at[s, me, y], look_send.at[s], look_recv.at[s], place(g, y)).start()

                if i:
                    give()
                else:
                    pl.when(j > 0)(give)

                    @pl.when(j == 0)
                    def _():
                        xt[s, pl.ds(me, 1), pl.ds(y, 1)] = chosen[None, None]

            return 0

        lax.fori_loop(0, 8, four, 0)

    def looked(s):
        return send(staged.at[s, most], xt.at[s, most, y], look_send.at[s], look_recv.at[s], at(up))

    def side(s, slot):
        first, count, of = ((0, groups, y), (0, groups, y), (0, groups // 2, down), (groups // 2, groups // 2, up))[slot]
        part = xt.at[s, pl.ds(first, count), of]
        return send(part, part, side_send.at[s, slot], side_recv.at[s, slot], at(down if slot % 2 else up))

    def gather(s):
        looked(s).wait_recv()
        side(s, 0).start()
        side(s, 1).start()

    def relay(s):
        for way in range(2):
            side(s, way).wait_recv()
            side(s, 2 + way).start()


    length = lens_ref[me]

    def block(s):
        for way in range(2):
            side(s, 2 + way).wait_recv()
        squares[...] = jnp.zeros_like(squares)

        def over(c, _):
            cols = pl.ds(pl.multiple_of(c * 128, 128), 128)
            piece = xt[s, pl.ds(c, 1)].reshape(128, 128).T
            xb[:, cols] = piece
            wide = piece.astype(jnp.float32)
            squares[...] += wide * wide
            return 0

        lax.fori_loop(0, width // 128, over, 0, unroll=4)
        scale = lax.rsqrt(jnp.sum(squares[...], axis=1, keepdims=True) / width + norm_eps)
        squares[...] = jnp.broadcast_to(scale, squares.shape)

        @pl.when(y == s)
        def _():
            own_x[...] = xb[...]

        def norm(c, _):
            cols = pl.ds(pl.multiple_of(c * 128, 128), 128)
            wide = xb[:, cols].astype(jnp.float32) * squares[...] * gain_ref[:, cols]
            normed[:, cols] = wide.astype(jnp.bfloat16)
            return 0

        lax.fori_loop(0, width // 128, norm, 0, unroll=4)
        here = slice(s * quarter, (s + 1) * quarter)

        def project(b, first):
            return jnp.dot(
                normed[...],
                w[b, :, :, :, :, first : first + 256].reshape(width, 256),
                preferred_element_type=jnp.float32,
            )

        def rotated(part):
            return (part * cos_ref[here, :] + pltpu.roll(part, HD // 2, 1) * sin_ref[here, :]).astype(jnp.bfloat16)

        def heads(b, _):
            for n in range(2):
                both = project(b, n * 256)
                for h in range(2):
                    q[pl.ds(b * 4 + n * 2 + h, 1)] = rotated(both[:, h * HD : (h + 1) * HD])[None]
            both = project(b, 512)
            k[pl.ds(b, 1), here] = rotated(both[:, :HD])[None]
            v[pl.ds(b, 1), here] = both[:, HD:].astype(jnp.bfloat16)[None]
            return 0

        lax.fori_loop(0, 2, heads, 0)
        for b in range(2):
            cache_ref[0, 0, here, b * HD : (b + 1) * HD] = k[b, here]
            cache_ref[0, 1, here, b * HD : (b + 1) * HD] = v[b, here]
        keys = (s + 1) * quarter
        p = lax.broadcasted_iota(jnp.int32, (quarter, keys), 0) + s * quarter
        j = lax.broadcasted_iota(jnp.int32, (quarter, keys), 1)
        allowed = (j <= p) & (j < length)

        def head(h, _):
            b = h // 4
            scores = lax.dot_general(
                q[h], k[b, :keys], (((1,), (1,)), ((), ())), preferred_element_type=jnp.float32
            )
            scores = jnp.where(allowed, scores * np.float32(1 / np.sqrt(HD)), -1e30)
            expd = jnp.exp(scores - jnp.max(scores, axis=1, keepdims=True))
            weights = (expd / jnp.sum(expd, axis=1, keepdims=True)).astype(jnp.bfloat16)
            got = jnp.dot(weights, v[b, :keys], preferred_element_type=jnp.float32)
            attended[here, pl.ds(pl.multiple_of(h * HD, HD), HD)] = got.astype(jnp.bfloat16)
            return 0

        lax.fori_loop(0, 8, head, 0, unroll=2)

    look(0)
    plane_w.step(2)
    look(1)
    gather(0)
    look(2)
    gather(1)
    relay(0)
    plane_w.step(3)
    look(3)
    gather(2)
    relay(1)
    plane_w.step(4)
    gather(3)
    plane_o.step(0)
    plane_w.step(5)
    plane_w.step(6)
    relay(2)
    block(0)
    relay(3)
    plane_o.step(1)
    block(1)
    plane_o.step(2)
    block(2)
    plane_o.step(3)
    plane_o.step(4)
    block(3)
    plane_o.step(5)
    others.wait_send()
    for s in range(4):
        looked(s).wait_send()
        for slot in range(4):
            side(s, slot).wait_send()
    plane_o.step(6)


    def far_copy(c, way):
        return send(stage.at[c, far, way], mid.at[c, way], far_send.at[c, way], far_recv.at[c, way], at(down if way else up))

    def near_copy(c, way):
        part = stage.at[c, down if way else up, 1 - way]
        return send(part, final.at[c, way, 1 - way], near_send.at[c, way], near_recv.at[c, way], at(down if way else up))

    def sum_copy(c, way):
        return send(passed.at[c, way], final.at[c, way, way], sum_send.at[c, way], sum_recv.at[c, way], at(down if way else up))

    def wide(ref):
        return ref.reshape(quarter, 256).astype(jnp.float32)

    def pass_on(c):
        for way in range(2):
            far_copy(c, way).wait_recv()
            total = wide(stage[pl.ds(c, 1), pl.ds(down if way else up, 1), way]) + wide(mid[pl.ds(c, 1), way])
            passed[pl.ds(c, 1), way] = total.astype(jnp.bfloat16)[None]
            sum_copy(c, way).start()

    def finish(c, _):
        for way in range(2):
            near_copy(c, way).wait_recv()
            sum_copy(c, way).wait_recv()
        for half in range(2):
            cols = pl.ds(pl.multiple_of(c * 512 + half * 256, 256), 256)
            total = wide(stage[pl.ds(c, 1), pl.ds(y, 1), half])
            for way in range(2):
                total = total + wide(final[pl.ds(c, 1), way, half])
            hidden_ref[:, cols] = (own_x[:, cols].astype(jnp.float32) + total).astype(jnp.bfloat16)
        return 0

    chunks = stage.shape[0]

    def output(c, _):
        for half in range(2):
            part = jnp.dot(attended[:, :512], wo[0, c // 2, c % 2, half], preferred_element_type=jnp.float32)
            part = part + jnp.dot(attended[:, 512:], wo[1, c // 2, c % 2, half], preferred_element_type=jnp.float32)
            part = part.astype(jnp.bfloat16)
            for member in range(4):
                stage[pl.ds(c, 1), member, half] = part[member * quarter : (member + 1) * quarter][None]
        for way in range(2):
            far_copy(c, way).start()
        for way in range(2):
            near_copy(c, way).start()

        @pl.when(c > 0)
        def _():
            pass_on(c - 1)

        return 0

    lax.fori_loop(0, chunks, output, 0)
    pass_on(chunks - 1)
    lax.fori_loop(0, chunks, finish, 0)

    def drain(c, _):
        for way in range(2):
            far_copy(c, way).wait_send()
            near_copy(c, way).wait_send()
            sum_copy(c, way).wait_send()
        return 0

    lax.fori_loop(0, chunks, drain, 0)


def shards(prompt_ids, prompt_lengths, embed_table, norm_gain, w_query, w_key, w_value, w_out):
    quarter = prompt_ids.shape[0]
    prompt = quarter * 4
    feats, vocab = embed_table.shape
    width = feats * lax.axis_size(AXES)
    depth, across = w_query.shape[0], w_query.shape[1] + w_key.shape[1] + w_value.shape[1]
    groups = prompt_lengths.shape[0]
    angle = np.arange(prompt)[:, None] * rope_theta ** (-2.0 * np.arange(HD // 2) / HD)[None, :]
    cosine = np.concatenate([np.cos(angle), np.cos(angle)], axis=1).astype(np.float32)
    sine = np.concatenate([-np.sin(angle), np.sin(angle)], axis=1).astype(np.float32)
    chunks = width // 512
    bf, f32 = jnp.bfloat16, jnp.float32
    vmem = pl.BlockSpec(memory_space=pltpu.VMEM)
    anyw = pl.BlockSpec(memory_space=pl.ANY)
    dma = pltpu.SemaphoreType.DMA
    return pl.pallas_call(
        kernel,
        out_shape=(
            jax.ShapeDtypeStruct((quarter, width), bf),
            jax.ShapeDtypeStruct((1, 2, prompt, 2 * HD), bf),
        ),
        in_specs=[pl.BlockSpec(memory_space=pltpu.SMEM)] + [vmem] * 4 + [anyw] * 5,
        out_specs=(vmem, vmem),
        scratch_shapes=[
            pltpu.VMEM((2, 4, feats, TILES * 128), bf),
            pltpu.VMEM((STRIP, 128), f32),
            pltpu.VMEM((512, 128), f32),
            pltpu.VMEM((groups, 4, 128), jnp.int32),
            pltpu.VMEM((groups, 4, 128), jnp.int32),
            pltpu.SMEM((groups, 4, 128), jnp.int32),
            pltpu.VMEM((4, groups, feats, 128), bf),
            pltpu.VMEM((4, groups, 4, feats, 128), bf),
            pltpu.VMEM((2, 4, 2, 2, depth, across), bf),
            pltpu.VMEM((2, 4, 2, 2, *w_out.shape), bf),
            pltpu.VMEM((quarter, width), bf),
            pltpu.VMEM((quarter, width), bf),
            pltpu.VMEM((quarter, width), bf),
            pltpu.VMEM((quarter, 128), f32),
            pltpu.VMEM((8, quarter, HD), bf),
            pltpu.VMEM((2, prompt, HD), bf),
            pltpu.VMEM((2, prompt, HD), bf),
            pltpu.VMEM((prompt, 1024), bf),
            pltpu.VMEM((chunks, 4, 2, quarter, 256), bf),
            pltpu.VMEM((chunks, 2, quarter, 256), bf),
            pltpu.VMEM((chunks, 2, quarter, 256), bf),
            pltpu.VMEM((chunks, 2, 2, quarter, 256), bf),
            dma((2, 4)),
            dma,
            dma((4,)),
            dma((4,)),
            dma((4,)),
            dma((4,)),
            dma((4,)),
            dma((4, 4)),
            dma((4, 4)),
        ]
        + [dma((chunks, 2))] * 6
        + Plane.sems()
        + Plane.sems(),
        compiler_params=pltpu.CompilerParams(vmem_limit_bytes=67043328, collective_id=0, has_side_effects=True),
    )(
        prompt_lengths,
        prompt_ids.reshape(1, quarter),
        norm_gain.reshape(1, width),
        cosine,
        sine,
        embed_table,
        w_query,
        w_key,
        w_value,
        w_out,
    )


def solution(mesh):
    split = Mesh(mesh.devices.reshape(4, 2, 2, 2, 4), AXES)
    placed = (
        P(AXES),
        P(),
        P(AXES, None),
        P(),
        P(DP, TENSOR),
        P(DP, TENSOR),
        P(DP, TENSOR),
        P(TENSOR, DP),
    )
    return jax.shard_map(
        shards,
        mesh=split,
        in_specs=placed,
        out_specs=(P(AXES, None), P(AXES, None, None, None)),
        check_vma=False,
    )
```

```python
import jax
import jax.numpy as jnp
import numpy as np
from jax import lax
from jax.experimental import pallas as pl
from jax.experimental.pallas import tpu as pltpu
from jax.sharding import Mesh
from jax.sharding import PartitionSpec as P

HD = 128
AXES = ("z", "xlo", "core", "xhi", "y")
DP = ("z", "xlo", "core")
TENSOR = ("xhi", "y")
MESH = pl.DeviceIdType.MESH

norm_eps = 1e-05
rope_theta = 500000.0

BLOCKS = 252
STRIP = BLOCKS * 128
TILES = 21
LOADS = BLOCKS // TILES


class Plane:
    def __init__(self, whole, own, sems, by_row=False):
        self.whole, self.own, self.by_row = whole, own, by_row
        self.send, self.recv, self.core_send, self.core_recv = sems
        self.z = lax.axis_index("z")
        self.xlo = lax.axis_index("xlo")
        self.core = lax.axis_index("core")
        self.xhi = lax.axis_index("xhi")
        self.y = lax.axis_index("y")
        self.x = self.xhi * 2 + self.xlo
        self.half = whole.shape[4] // 2

    def neighbours(self):
        found = []
        for cls in range(2):
            for way in range(2):
                found.append(self.device(cls, self.first(cls) + (3 if way else 1), self.second(cls)))
        found.append((self.z, self.xlo, 1 - self.core, self.xhi, self.y))
        return found

    def first(self, cls):
        return self.x if cls else self.z

    def second(self, cls):
        return self.z if cls else self.x

    def device(self, cls, f, s):
        f, s = f % 4, s % 4
        x, z = (f, s) if cls else (s, f)
        return (z, x % 2, self.core, x // 2, self.y)

    def rows(self, cls, part):
        if part is None:
            return pl.ds(cls * self.half, self.half)
        return pl.ds(cls * self.half + part * (self.half // 2), self.half // 2)

    def piece(self, cls, f, s, part=None):
        f, s = f % 4, s % 4
        x, z = (f, s) if cls else (s, f)
        return self.whole.at[x // 2, z, x % 2, self.core, self.rows(cls, part)]

    def copy(self, cls, stage, slot, f, s, part, own):
        step = 3 if slot % 2 else 1
        pf, ps = self.first(cls), self.second(cls)
        to = self.device(cls, pf + step, ps) if stage == 0 else self.device(cls, pf, ps + step)
        dst = self.piece(cls, f, s, part)
        src = self.own.at[self.rows(cls, part)] if own else dst
        return pltpu.make_async_remote_copy(
            src, dst, self.send.at[cls, stage, slot], self.recv.at[cls, stage, slot], device_id=to, device_id_type=MESH
        )

    def full(self, cls, stage, way):
        o = max(stage - 1, 0)
        return self.copy(cls, stage, way, self.first(cls) + o, self.second(cls), None, o == 0)

    def relay(self, cls, stage, way):
        step = 1 if way else 3
        f, s = self.first(cls), self.second(cls)
        if stage == 0:
            f = f + step
        else:
            f, s = f + stage - 1, s + step
        return self.copy(cls, stage, 2 + way, f, s, way, False)

    def cores(self, cls, o):
        s = ((self.z if self.by_row else self.second(cls)) + o) % 4
        if cls or self.by_row:
            ref = self.whole.at[:, s, :, self.core, self.rows(cls, None)]
        else:
            ref = self.whole.at[s // 2, :, s % 2, self.core, self.rows(cls, None)]
        return pltpu.make_async_remote_copy(
            ref,
            ref,
            self.core_send.at[cls, o],
            self.core_recv.at[cls, o],
            device_id=(self.z, self.xlo, 1 - self.core, self.xhi, self.y),
            device_id_type=MESH,
        )

    def each(self, act, *args):
        for cls in range(2):
            for way in range(2):
                act(cls, way, *args)

    def start_full(self, *stages):
        for stage in stages:
            self.each(lambda cls, way: self.full(cls, stage, way).start())

    def take_full(self, *stages):
        for stage in stages:
            self.each(lambda cls, way: self.full(cls, stage, way).wait_recv())
            self.each(lambda cls, way: self.relay(cls, stage, way).start())

    def take_relay(self, *stages):
        for stage in stages:
            self.each(lambda cls, way: self.relay(cls, stage, way).wait_recv())

    def start_cores(self, cls, *offsets):
        for o in offsets:
            self.cores(cls, o).start()

    def row_step(self, n):
        ways = range(2)
        if n == 0:
            self.start_full(0, 1)
        elif n == 1:
            self.take_full(0)
            self.start_full(2, 4)
        elif n == 2:
            self.take_relay(0)
            self.start_full(3)
            self.take_full(1)
            self.start_cores(1, 0)
        elif n == 3:
            for way in ways:
                self.relay(0, 1, way).wait_recv()
            self.start_cores(0, 0)
            self.take_full(2, 4)
        elif n == 4:
            self.take_full(3)
            self.start_cores(1, 1, 3)
            for stage in (2, 4):
                for way in ways:
                    self.relay(0, stage, way).wait_recv()
            self.start_cores(0, 1, 3)
        else:
            for way in ways:
                self.relay(0, 3, way).wait_recv()
                for stage in range(1, 5):
                    self.relay(1, stage, way).wait_recv()
            self.start_cores(0, 2)
            self.start_cores(1, 2)

    def row_ready(self, o):
        for cls in range(2):
            self.cores(cls, o).wait_recv()

    def drain(self):
        for cls in range(2):
            for o in range(4):
                self.cores(cls, o).wait_send()
        for stage in range(5):
            self.each(lambda cls, way: self.full(cls, stage, way).wait_send())
            self.each(lambda cls, way: self.relay(cls, stage, way).wait_send())

    def step(self, n):
        if n == 0:
            self.start_full(1)
        elif n == -1:
            self.start_full(0)
        elif n == 1:
            self.take_full(0)
            self.start_full(2, 4)
        elif n == 10:
            self.take_full(0)
        elif n == 11:
            self.start_full(2)
        elif n == 12:
            self.start_full(4)
        elif n == 13:
            self.take_relay(0)
            self.start_full(3)
        elif n == 14:
            self.take_full(1)
        elif n == 15:
            for cls in range(2):
                self.cores(cls, 0).start()
            self.take_full(2)
        elif n == 16:
            self.take_full(4)
        elif n == 2:
            self.take_relay(0)
            self.start_full(3)
            self.take_full(1)
        elif n == 3:
            for cls in range(2):
                self.cores(cls, 0).start()
            self.take_full(2, 4)
        elif n == 4:
            self.take_full(3)
            for o in (1, 3):
                for cls in range(2):
                    self.cores(cls, o).start()
        elif n == 5:
            self.take_relay(1, 2, 3, 4)
            for cls in range(2):
                self.cores(cls, 2).start()
        else:
            for cls in range(2):
                for o in range(4):
                    self.cores(cls, o).wait_recv()

    @staticmethod
    def sems():
        dma = pltpu.SemaphoreType.DMA
        return [dma((2, 5, 4)), dma((2, 5, 4)), dma((2, 4)), dma((2, 4))]


def place(g, y):
    return (g // 8, g // 4 % 2, g // 2 % 2, g % 2, y)


def kernel(lens_ref, ids_ref, gain_ref, cos_ref, sin_ref, table_ref, wq_ref, wk_ref, wv_ref, wo_ref, hidden_ref, cache_ref,
           raw, major, rows, ids, spots, spots_s, staged, xt, w, wo, own_x, xb, normed, squares, q, k, v, attended,
           stage, mid, passed, final, table_sems, spot_sem, own_sems, id_send, id_recv, look_send, look_recv,
           side_send, side_recv, far_send, far_recv, near_send, near_recv, sum_send, sum_recv, *plane_sems):
    feats, vocab = table_ref.shape
    z = lax.axis_index("z")
    xlo = lax.axis_index("xlo")
    core = lax.axis_index("core")
    xhi = lax.axis_index("xhi")
    y = lax.axis_index("y")
    me = ((z * 2 + xlo) * 2 + core) * 2 + xhi
    groups = ids.shape[0]
    quarter, width = hidden_ref.shape
    up = (y + 1) % 4
    down = (y + 3) % 4
    far = (y + 2) % 4
    tiles = vocab // 128

    def at(member):
        return place(me, member)

    def send(src, dst, ssem, rsem, device):
        return pltpu.make_async_remote_copy(src, dst, ssem, rsem, device_id=device, device_id_type=MESH)

    barrier = pltpu.get_barrier_semaphore()
    for n in range(1, 4):
        pl.semaphore_signal(barrier, inc=1, device_id=at((y + n) % 4), device_id_type=MESH)

    def greet(n, _):
        pl.semaphore_signal(barrier, inc=1, device_id=place((me + n) % groups, y), device_id_type=MESH)
        return 0

    lax.fori_loop(1, groups, greet, 0)


    def table_base(n, strip):
        return jnp.minimum(strip * BLOCKS + n * TILES, tiles - TILES)

    def table_copy(n, strip):
        first = pl.multiple_of(table_base(n, strip) * 128, 128)
        return pltpu.make_async_copy(
            table_ref.at[:, pl.ds(first, TILES * 128)], raw.at[n % 2, strip], table_sems.at[n % 2, strip]
        )

    for n in range(2):
        for strip in range(4):
            table_copy(n, strip).start()
    own_w = w.at[xhi, z, xlo, core]
    own_wo = wo.at[xhi, z, xlo, core]
    mine = [
        pltpu.make_async_copy(ref, own_w.at[:, pl.ds(first, ref.shape[1])], own_sems.at[n])
        for n, (ref, first) in enumerate(((wq_ref, 0), (wk_ref, 512), (wv_ref, 640)))
    ] + [pltpu.make_async_copy(wo_ref, own_wo, own_sems.at[3])]
    for copy in mine:
        copy.start()
    plane_w = Plane(w, own_w, plane_sems[:4])
    plane_o = Plane(wo, own_wo, plane_sems[4:], True)

    def turn(n, _):
        for strip in range(4):
            table_copy(n, strip).wait()

        def tile(t, _):
            parts = []
            for strip in range(4):
                first = jnp.minimum(strip * BLOCKS + n * TILES + t, tiles - 1) - table_base(n, strip)
                parts.append(raw[n % 2, strip, :, pl.ds(pl.multiple_of(first * 128, 128), 128)])
            block = jnp.concatenate(parts, axis=0)
            major[pl.ds(pl.multiple_of((n * TILES + t) * 128, 128), 128), :] = block.T.astype(jnp.float32)
            return 0

        lax.fori_loop(0, TILES, tile, 0, unroll=7)

        @pl.when(n + 2 < LOADS)
        def _():
            for strip in range(4):
                table_copy(n + 2, strip).start()

        return 0

    lax.fori_loop(0, 2, turn, 0)
    pl.semaphore_wait(barrier, 3 + groups - 1)
    ids[pl.ds(me, 1), pl.ds(y, 1), :] = ids_ref[...][None]
    line = [
        send(ids_ref, ids.at[me, pl.ds(y, 1)], id_send.at[n - 1], id_recv.at[n - 1], at((y + n) % 4)) for n in range(1, 4)
    ]
    for copy in line:
        copy.start()
    for copy in mine:
        copy.wait()
    plane_w.step(-1)
    lax.fori_loop(2, 5, turn, 0)
    for copy in line:
        copy.wait()

    def spread(n, _):
        send(ids.at[me], ids.at[me], id_send.at[3], id_recv.at[3], place((me + n) % groups, y)).start()
        return 0

    lax.fori_loop(1, groups, spread, 0)
    plane_w.step(0)
    lax.fori_loop(5, LOADS, turn, 0)
    most = pl.ds(0, groups - 1)
    others = send(ids.at[most], ids.at[most], id_send.at[3], id_recv.at[3], at(up))
    others.wait_recv()
    all_ids = ids[...]
    strip_of = jnp.zeros_like(all_ids)
    for n in range(1, 4):
        strip_of = strip_of + jnp.where(all_ids >= n * STRIP, 1, 0)
    spots_of = all_ids - strip_of * STRIP
    for s in range(4):
        spots[s] = spots_of[:, s]
    to_smem = [pltpu.make_async_copy(spots.at[s], spots_s.at[s], spot_sem.at[s]) for s in range(4)]
    for copy in to_smem:
        copy.start()
    eye = (
        lax.broadcasted_iota(jnp.int32, (128, 128), 0) == lax.broadcasted_iota(jnp.int32, (128, 128), 1)
    ).astype(jnp.bfloat16)


    def look(s):
        to_smem[s].wait()

        def four(j, _):
            def some(i, _):
                g = (me + 4 * j + i) % groups
                for n in range(128):
                    rows[pl.ds(i * 128 + n, 1), :] = major[pl.ds(spots_s[s, g, n], 1), :]
                return 0

            lax.fori_loop(0, 4, some, 0)
            found = lax.dot_general(
                eye, rows[...].astype(jnp.bfloat16), (((1,), (1,)), ((), ())), preferred_element_type=jnp.float32
            )
            for i in range(4):
                g = (me + 4 * j + i) % groups
                word = ids[pl.ds(g, 1), pl.ds(s, 1), :].reshape(1, 128)
                part = found[:, i * 128 : (i + 1) * 128]
                chosen = part[:feats]
                for n in range(1, 4):
                    chosen = jnp.where(word >= n * STRIP, part[n * feats : (n + 1) * feats], chosen)
                chosen = chosen.astype(jnp.bfloat16)
                staged[s, pl.ds(4 * j + i, 1)] = chosen[None]

                def give():
                    send(staged.at[s, 4 * j + i], xt.at[s, me, y], look_send.at[s], look_recv.at[s], place(g, y)).start()

                if i:
                    give()
                else:
                    pl.when(j > 0)(give)

                    @pl.when(j == 0)
                    def _():
                        xt[s, pl.ds(me, 1), pl.ds(y, 1)] = chosen[None, None]

            return 0

        lax.fori_loop(0, 8, four, 0)

    def looked(s):
        return send(staged.at[s, most], xt.at[s, most, y], look_send.at[s], look_recv.at[s], at(up))

    def side(s, slot):
        first, count, of = ((0, groups, y), (0, groups, y), (0, groups // 2, down), (groups // 2, groups // 2, up))[slot]
        part = xt.at[s, pl.ds(first, count), of]
        return send(part, part, side_send.at[s, slot], side_recv.at[s, slot], at(down if slot % 2 else up))

    def gather(s):
        looked(s).wait_recv()
        side(s, 0).start()
        side(s, 1).start()

    def relay(s):
        for way in range(2):
            side(s, way).wait_recv()
            side(s, 2 + way).start()


    length = lens_ref[me]

    def prepare(s):
        for way in range(2):
            side(s, 2 + way).wait_recv()
        squares[...] = jnp.zeros_like(squares)

        def over(c, _):
            cols = pl.ds(pl.multiple_of(c * 128, 128), 128)
            piece = xt[s, pl.ds(c, 1)].reshape(128, 128).T
            xb[:, cols] = piece
            wide = piece.astype(jnp.float32)
            squares[...] += wide * wide
            return 0

        lax.fori_loop(0, width // 128, over, 0, unroll=4)
        scale = lax.rsqrt(jnp.sum(squares[...], axis=1, keepdims=True) / width + norm_eps)
        squares[...] = jnp.broadcast_to(scale, squares.shape)

        @pl.when(y == s)
        def _():
            own_x[...] = xb[...]

        here = slice(s * quarter, (s + 1) * quarter)

        def norm(c, _):
            cols = pl.ds(pl.multiple_of(c * 128, 128), 128)
            wide = xb[:, cols].astype(jnp.float32) * squares[...] * gain_ref[:, cols]
            normed[here, cols] = wide.astype(jnp.bfloat16)
            return 0

        lax.fori_loop(0, width // 128, norm, 0, unroll=4)
    def project(lo, hi):
        here = slice(lo * quarter, hi * quarter)

        def product(b, first):
            return jnp.dot(
                normed[here, :],
                w[b, :, :, :, :, first : first + 256].reshape(width, 256),
                preferred_element_type=jnp.float32,
            )

        def rotated(part):
            return (part * cos_ref[here, :] + pltpu.roll(part, HD // 2, 1) * sin_ref[here, :]).astype(jnp.bfloat16)

        def heads(b, _):
            for n in range(2):
                both = product(b, n * 256)
                for h in range(2):
                    q[pl.ds(b * 4 + n * 2 + h, 1), here] = rotated(both[:, h * HD : (h + 1) * HD])[None]
            both = product(b, 512)
            k[pl.ds(b, 1), here] = rotated(both[:, :HD])[None]
            v[pl.ds(b, 1), here] = both[:, HD:].astype(jnp.bfloat16)[None]
            return 0

        lax.fori_loop(0, 2, heads, 0)
        for b in range(2):
            cache_ref[0, 0, here, b * HD : (b + 1) * HD] = k[b, here]
            cache_ref[0, 1, here, b * HD : (b + 1) * HD] = v[b, here]

    def attend(s):
        here = slice(s * quarter, (s + 1) * quarter)
        keys = (s + 1) * quarter
        p = lax.broadcasted_iota(jnp.int32, (quarter, keys), 0) + s * quarter
        j = lax.broadcasted_iota(jnp.int32, (quarter, keys), 1)
        allowed = ((j <= p) & (j < length))[None]
        for b in range(2):
            scores = lax.dot_general(
                q[b * 4 : b * 4 + 4, here].reshape(4 * quarter, HD),
                k[b, :keys],
                (((1,), (1,)), ((), ())),
                preferred_element_type=jnp.float32,
            ).reshape(4, quarter, keys)
            scores = jnp.where(allowed, scores * np.float32(1 / np.sqrt(HD)), -1e30)
            expd = jnp.exp(scores - jnp.max(scores, axis=2, keepdims=True))
            weights = (expd / jnp.sum(expd, axis=2, keepdims=True)).astype(jnp.bfloat16)
            got = jnp.dot(weights.reshape(4 * quarter, keys), v[b, :keys], preferred_element_type=jnp.float32)
            got = got.astype(jnp.bfloat16)
            for h in range(4):
                attended[here, (b * 4 + h) * HD : (b * 4 + h + 1) * HD] = got[h * quarter : (h + 1) * quarter]

    plane_w.step(10)
    plane_w.step(11)
    look(0)
    plane_w.step(12)
    look(1)
    gather(0)
    plane_w.step(13)
    plane_w.step(14)
    look(2)
    gather(1)
    relay(0)
    plane_w.step(15)
    plane_w.step(16)
    look(3)
    gather(2)
    plane_w.step(4)
    relay(1)
    prepare(0)
    gather(3)
    plane_w.step(5)
    relay(2)
    plane_o.row_step(0)
    plane_w.step(6)
    prepare(1)
    plane_o.row_step(1)
    project(0, 2)
    relay(3)
    prepare(2)
    plane_o.row_step(2)
    attend(0)
    attend(1)
    project(2, 3)
    attend(2)
    prepare(3)
    plane_o.row_step(3)
    project(3, 4)
    attend(3)


    def far_copy(c, way):
        return send(stage.at[c, far, way], mid.at[c, way], far_send.at[c, way], far_recv.at[c, way], at(down if way else up))

    def near_copy(c, way):
        part = stage.at[c, down if way else up, 1 - way]
        return send(part, final.at[c, way, 1 - way], near_send.at[c, way], near_recv.at[c, way], at(down if way else up))

    def sum_copy(c, way):
        return send(passed.at[c, way], final.at[c, way, way], sum_send.at[c, way], sum_recv.at[c, way], at(down if way else up))

    def wide(ref):
        return ref.reshape(quarter, 256).astype(jnp.float32)

    def pass_on(c):
        for way in range(2):
            far_copy(c, way).wait_recv()
            total = wide(stage[pl.ds(c, 1), pl.ds(down if way else up, 1), way]) + wide(mid[pl.ds(c, 1), way])
            passed[pl.ds(c, 1), way] = total.astype(jnp.bfloat16)[None]
            sum_copy(c, way).start()

    def row_of(c):
        g = c // 2
        return (z + g + g // 2 * (1 - 2 * (g % 2))) % 4

    def finish(c, _):
        for way in range(2):
            near_copy(c, way).wait_recv()
            sum_copy(c, way).wait_recv()
        for half in range(2):
            cols = pl.ds(pl.multiple_of(row_of(c) * 1024 + c % 2 * 512 + half * 256, 256), 256)
            total = wide(stage[pl.ds(c, 1), pl.ds(y, 1), half])
            for way in range(2):
                total = total + wide(final[pl.ds(c, 1), way, half])
            hidden_ref[:, cols] = (own_x[:, cols].astype(jnp.float32) + total).astype(jnp.bfloat16)
        return 0

    chunks = stage.shape[0]

    def output(c, _):
        for half in range(2):
            part = jnp.dot(attended[:, :512], wo[0, row_of(c), c % 2, half], preferred_element_type=jnp.float32)
            part = part + jnp.dot(attended[:, 512:], wo[1, row_of(c), c % 2, half], preferred_element_type=jnp.float32)
            part = part.astype(jnp.bfloat16)
            for member in range(4):
                stage[pl.ds(c, 1), member, half] = part[member * quarter : (member + 1) * quarter][None]
        for way in range(2):
            far_copy(c, way).start()
        for way in range(2):
            near_copy(c, way).start()

        @pl.when(c > 0)
        def _():
            pass_on(c - 1)

        @pl.when(c > 1)
        def _():
            finish(c - 2, 0)

        return 0

    plane_o.row_ready(0)
    lax.fori_loop(0, 1, output, 0)
    plane_o.row_step(4)
    lax.fori_loop(1, 2, output, 0)
    plane_o.row_ready(1)
    lax.fori_loop(2, 4, output, 0)
    plane_o.row_step(5)
    plane_o.row_ready(3)
    lax.fori_loop(4, 6, output, 0)
    plane_o.row_ready(2)
    lax.fori_loop(6, chunks, output, 0)
    pass_on(chunks - 1)
    lax.fori_loop(chunks - 2, chunks, finish, 0)
    others.wait_send()
    for s in range(4):
        looked(s).wait_send()
        for slot in range(4):
            side(s, slot).wait_send()
    plane_w.drain()
    plane_o.drain()

    def drain(c, _):
        for way in range(2):
            far_copy(c, way).wait_send()
            near_copy(c, way).wait_send()
            sum_copy(c, way).wait_send()
        return 0

    lax.fori_loop(0, chunks, drain, 0)


def shards(prompt_ids, prompt_lengths, embed_table, norm_gain, w_query, w_key, w_value, w_out):
    quarter = prompt_ids.shape[0]
    prompt = quarter * 4
    feats, vocab = embed_table.shape
    width = feats * lax.axis_size(AXES)
    depth, across = w_query.shape[0], w_query.shape[1] + w_key.shape[1] + w_value.shape[1]
    groups = prompt_lengths.shape[0]
    angle = np.arange(prompt)[:, None] * rope_theta ** (-2.0 * np.arange(HD // 2) / HD)[None, :]
    cosine = np.concatenate([np.cos(angle), np.cos(angle)], axis=1).astype(np.float32)
    sine = np.concatenate([-np.sin(angle), np.sin(angle)], axis=1).astype(np.float32)
    chunks = width // 512
    bf, f32 = jnp.bfloat16, jnp.float32
    vmem = pl.BlockSpec(memory_space=pltpu.VMEM)
    anyw = pl.BlockSpec(memory_space=pl.ANY)
    dma = pltpu.SemaphoreType.DMA
    return pl.pallas_call(
        kernel,
        out_shape=(
            jax.ShapeDtypeStruct((quarter, width), bf),
            jax.ShapeDtypeStruct((1, 2, prompt, 2 * HD), bf),
        ),
        in_specs=[pl.BlockSpec(memory_space=pltpu.SMEM)] + [vmem] * 4 + [anyw] * 5,
        out_specs=(vmem, vmem),
        scratch_shapes=[
            pltpu.VMEM((2, 4, feats, TILES * 128), bf),
            pltpu.VMEM((STRIP, 128), f32),
            pltpu.VMEM((512, 128), f32),
            pltpu.VMEM((groups, 4, 128), jnp.int32),
            pltpu.VMEM((4, groups, 128), jnp.int32),
            pltpu.SMEM((4, groups, 128), jnp.int32),
            pltpu.VMEM((4, groups, feats, 128), bf),
            pltpu.VMEM((4, groups, 4, feats, 128), bf),
            pltpu.VMEM((2, 4, 2, 2, depth, across), bf),
            pltpu.VMEM((2, 4, 2, 2, *w_out.shape), bf),
            pltpu.VMEM((quarter, width), bf),
            pltpu.VMEM((quarter, width), bf),
            pltpu.VMEM((prompt, width), bf),
            pltpu.VMEM((quarter, 128), f32),
            pltpu.VMEM((8, prompt, HD), bf),
            pltpu.VMEM((2, prompt, HD), bf),
            pltpu.VMEM((2, prompt, HD), bf),
            pltpu.VMEM((prompt, 1024), bf),
            pltpu.VMEM((chunks, 4, 2, quarter, 256), bf),
            pltpu.VMEM((chunks, 2, quarter, 256), bf),
            pltpu.VMEM((chunks, 2, quarter, 256), bf),
            pltpu.VMEM((chunks, 2, 2, quarter, 256), bf),
            dma((2, 4)),
            dma((4,)),
            dma((4,)),
            dma((4,)),
            dma((4,)),
            dma((4,)),
            dma((4,)),
            dma((4, 4)),
            dma((4, 4)),
        ]
        + [dma((chunks, 2))] * 6
        + Plane.sems()
        + Plane.sems(),
        compiler_params=pltpu.CompilerParams(vmem_limit_bytes=67043328, collective_id=0, has_side_effects=True),
    )(
        prompt_lengths,
        prompt_ids.reshape(1, quarter),
        norm_gain.reshape(1, width),
        cosine,
        sine,
        embed_table,
        w_query,
        w_key,
        w_value,
        w_out,
    )


def solution(mesh):
    split = Mesh(mesh.devices.reshape(4, 2, 2, 2, 4), AXES)
    placed = (
        P(AXES),
        P(),
        P(AXES, None),
        P(),
        P(DP, TENSOR),
        P(DP, TENSOR),
        P(DP, TENSOR),
        P(TENSOR, DP),
    )
    return jax.shard_map(
        shards,
        mesh=split,
        in_specs=placed,
        out_specs=(P(AXES, None), P(AXES, None, None, None)),
        check_vma=False,
    )
```

```python
import jax
import jax.numpy as jnp
import numpy as np
from jax import lax
from jax.experimental import pallas as pl
from jax.experimental.pallas import tpu as pltpu
from jax.sharding import Mesh
from jax.sharding import PartitionSpec as P

HD = 128
AXES = ("z", "xlo", "core", "xhi", "y")
DP = ("z", "xlo", "core")
TENSOR = ("xhi", "y")
MESH = pl.DeviceIdType.MESH

norm_eps = 1e-05
rope_theta = 500000.0

BLOCKS = 252
STRIP = BLOCKS * 128
TILES = 21
LOADS = BLOCKS // TILES


class Plane:
    def __init__(self, whole, own, sems, by_row=False):
        self.whole, self.own, self.by_row = whole, own, by_row
        self.send, self.recv, self.core_send, self.core_recv = sems
        self.z = lax.axis_index("z")
        self.xlo = lax.axis_index("xlo")
        self.core = lax.axis_index("core")
        self.xhi = lax.axis_index("xhi")
        self.y = lax.axis_index("y")
        self.x = self.xhi * 2 + self.xlo
        self.half = whole.shape[4] // 2

    def neighbours(self):
        found = []
        for cls in range(2):
            for way in range(2):
                found.append(self.device(cls, self.first(cls) + (3 if way else 1), self.second(cls)))
        found.append((self.z, self.xlo, 1 - self.core, self.xhi, self.y))
        return found

    def first(self, cls):
        return self.x if cls else self.z

    def second(self, cls):
        return self.z if cls else self.x

    def device(self, cls, f, s):
        f, s = f % 4, s % 4
        x, z = (f, s) if cls else (s, f)
        return (z, x % 2, self.core, x // 2, self.y)

    def rows(self, cls, part):
        if part is None:
            return pl.ds(cls * self.half, self.half)
        return pl.ds(cls * self.half + part * (self.half // 2), self.half // 2)

    def piece(self, cls, f, s, part=None):
        f, s = f % 4, s % 4
        x, z = (f, s) if cls else (s, f)
        return self.whole.at[x // 2, z, x % 2, self.core, self.rows(cls, part)]

    def copy(self, cls, stage, slot, f, s, part, own):
        step = 3 if slot % 2 else 1
        pf, ps = self.first(cls), self.second(cls)
        to = self.device(cls, pf + step, ps) if stage == 0 else self.device(cls, pf, ps + step)
        dst = self.piece(cls, f, s, part)
        src = self.own.at[self.rows(cls, part)] if own else dst
        return pltpu.make_async_remote_copy(
            src, dst, self.send.at[cls, stage, slot], self.recv.at[cls, stage, slot], device_id=to, device_id_type=MESH
        )

    def full(self, cls, stage, way):
        o = max(stage - 1, 0)
        return self.copy(cls, stage, way, self.first(cls) + o, self.second(cls), None, o == 0)

    def relay(self, cls, stage, way):
        step = 1 if way else 3
        f, s = self.first(cls), self.second(cls)
        if stage == 0:
            f = f + step
        else:
            f, s = f + stage - 1, s + step
        return self.copy(cls, stage, 2 + way, f, s, way, False)

    def cores(self, cls, o):
        s = ((self.z if self.by_row else self.second(cls)) + o) % 4
        if cls or self.by_row:
            ref = self.whole.at[:, s, :, self.core, self.rows(cls, None)]
        else:
            ref = self.whole.at[s // 2, :, s % 2, self.core, self.rows(cls, None)]
        return pltpu.make_async_remote_copy(
            ref,
            ref,
            self.core_send.at[cls, o],
            self.core_recv.at[cls, o],
            device_id=(self.z, self.xlo, 1 - self.core, self.xhi, self.y),
            device_id_type=MESH,
        )

    def each(self, act, *args):
        for cls in range(2):
            for way in range(2):
                act(cls, way, *args)

    def start_full(self, *stages):
        for stage in stages:
            self.each(lambda cls, way: self.full(cls, stage, way).start())

    def take_full(self, *stages):
        for stage in stages:
            self.each(lambda cls, way: self.full(cls, stage, way).wait_recv())
            self.each(lambda cls, way: self.relay(cls, stage, way).start())

    def take_relay(self, *stages):
        for stage in stages:
            self.each(lambda cls, way: self.relay(cls, stage, way).wait_recv())

    def start_cores(self, cls, *offsets):
        for o in offsets:
            self.cores(cls, o).start()

    def row_step(self, n):
        ways = range(2)
        if n == 0:
            self.start_full(0, 1)
        elif n == 1:
            self.take_full(0)
            self.start_full(2, 4)
        elif n == 2:
            self.take_relay(0)
            self.take_full(1)
            self.start_cores(1, 0)
            self.start_full(3)
        elif n == 3:
            for way in ways:
                self.relay(0, 1, way).wait_recv()
            self.start_cores(0, 0)
            self.take_full(2, 4)
        elif n == 4:
            self.take_full(3)
            self.start_cores(1, 1, 3)
            for stage in (2, 4):
                for way in ways:
                    self.relay(0, stage, way).wait_recv()
            self.start_cores(0, 1, 3)
        else:
            for way in ways:
                self.relay(0, 3, way).wait_recv()
                for stage in range(1, 5):
                    self.relay(1, stage, way).wait_recv()
            self.start_cores(0, 2)
            self.start_cores(1, 2)

    def row_ready(self, o):
        for cls in range(2):
            self.cores(cls, o).wait_recv()

    def drain(self):
        for cls in range(2):
            for o in range(4):
                self.cores(cls, o).wait_send()
        for stage in range(5):
            self.each(lambda cls, way: self.full(cls, stage, way).wait_send())
            self.each(lambda cls, way: self.relay(cls, stage, way).wait_send())

    def step(self, n):
        if n == 0:
            self.start_full(0)
        elif n == 1:
            self.start_full(1)
        elif n == 2:
            self.take_full(0)
        elif n == 3:
            self.start_full(2)
        elif n == 4:
            self.start_full(4)
        elif n == 5:
            self.take_relay(0)
            self.start_full(3)
        elif n == 6:
            self.take_full(1)
        elif n == 7:
            self.start_cores(0, 0)
            self.start_cores(1, 0)
            self.take_full(2)
        elif n == 8:
            self.take_full(4)
        elif n == 9:
            self.take_full(3)
            for cls in range(2):
                self.start_cores(cls, 1, 3)
        elif n == 10:
            self.take_relay(1, 2, 3, 4)
            for cls in range(2):
                self.start_cores(cls, 2)
        else:
            for o in range(4):
                self.row_ready(o)

    @staticmethod
    def sems():
        dma = pltpu.SemaphoreType.DMA
        return [dma((2, 5, 4)), dma((2, 5, 4)), dma((2, 4)), dma((2, 4))]


def place(g, y):
    return (g // 8, g // 4 % 2, g // 2 % 2, g % 2, y)


def kernel(lens_ref, ids_ref, gain_ref, trig_ref, table_ref, wq_ref, wk_ref, wv_ref, wo_ref, hidden_ref, cache_ref,
           raw, major, rows, ids, spots, spots_s, staged, xt, w, wo, hidden, cache, own_x, xb, normed, trig, squares, q, k, v, attended,
           stage, mid, passed, final, table_sems, spot_sem, own_sems, out_sems, id_send, id_recv, look_send, look_recv,
           side_send, side_recv, far_send, far_recv, near_send, near_recv, sum_send, sum_recv, *plane_sems):
    feats, vocab = table_ref.shape
    z = lax.axis_index("z")
    xlo = lax.axis_index("xlo")
    core = lax.axis_index("core")
    xhi = lax.axis_index("xhi")
    y = lax.axis_index("y")
    me = ((z * 2 + xlo) * 2 + core) * 2 + xhi
    groups = ids.shape[0]
    quarter, width = hidden.shape
    up = (y + 1) % 4
    down = (y + 3) % 4
    far = (y + 2) % 4
    tiles = vocab // 128

    def at(member):
        return place(me, member)

    def send(src, dst, ssem, rsem, device):
        return pltpu.make_async_remote_copy(src, dst, ssem, rsem, device_id=device, device_id_type=MESH)

    barrier = pltpu.get_barrier_semaphore()
    for n in range(1, 4):
        pl.semaphore_signal(barrier, inc=1, device_id=at((y + n) % 4), device_id_type=MESH)

    def greet(n, _):
        pl.semaphore_signal(barrier, inc=1, device_id=place((me + n) % groups, y), device_id_type=MESH)
        return 0

    lax.fori_loop(1, groups, greet, 0)


    def table_base(n, strip):
        return jnp.minimum(strip * BLOCKS + n * TILES, tiles - TILES)

    def table_copy(n, strip):
        first = pl.multiple_of(table_base(n, strip) * 128, 128)
        return pltpu.make_async_copy(
            table_ref.at[:, pl.ds(first, TILES * 128)], raw.at[n % 2, strip], table_sems.at[n % 2, strip]
        )

    for n in range(2):
        for strip in range(4):
            table_copy(n, strip).start()
    own_w = w.at[xhi, z, xlo, core]
    own_wo = wo.at[xhi, z, xlo, core]
    mine = [
        pltpu.make_async_copy(ref, own_w.at[:, pl.ds(first, ref.shape[1])], own_sems.at[n])
        for n, (ref, first) in enumerate(((wq_ref, 0), (wk_ref, 512), (wv_ref, 640)))
    ] + [pltpu.make_async_copy(wo_ref, own_wo, own_sems.at[3])]
    angles = pltpu.make_async_copy(trig_ref, trig, own_sems.at[4])
    angles.start()
    for copy in mine:
        copy.start()
    plane_w = Plane(w, own_w, plane_sems[:4])
    plane_o = Plane(wo, own_wo, plane_sems[4:], True)

    def turn(n, _):
        for strip in range(4):
            table_copy(n, strip).wait()

        def tile(t, _):
            parts = []
            for strip in range(4):
                first = jnp.minimum(strip * BLOCKS + n * TILES + t, tiles - 1) - table_base(n, strip)
                parts.append(raw[n % 2, strip, :, pl.ds(pl.multiple_of(first * 128, 128), 128)])
            block = jnp.concatenate(parts, axis=0)
            major[pl.ds(pl.multiple_of((n * TILES + t) * 128, 128), 128), :] = block.T.astype(jnp.float32)
            return 0

        lax.fori_loop(0, TILES, tile, 0, unroll=7)

        @pl.when(n + 2 < LOADS)
        def _():
            for strip in range(4):
                table_copy(n + 2, strip).start()

        return 0

    lax.fori_loop(0, 1, turn, 0)
    pl.semaphore_wait(barrier, 3 + groups - 1)
    ids[pl.ds(me, 1), pl.ds(y, 1), :] = ids_ref[...][None]
    line = [
        send(ids_ref, ids.at[me, pl.ds(y, 1)], id_send.at[n - 1], id_recv.at[n - 1], at((y + n) % 4)) for n in range(1, 4)
    ]
    for copy in line:
        copy.start()
    for copy in mine:
        copy.wait()
    plane_w.step(0)
    lax.fori_loop(1, 4, turn, 0)
    for copy in line:
        copy.wait()

    def spread(n, _):
        send(ids.at[me], ids.at[me], id_send.at[3], id_recv.at[3], place((me + n) % groups, y)).start()
        return 0

    lax.fori_loop(1, groups, spread, 0)
    plane_w.step(1)
    lax.fori_loop(4, 9, turn, 0)
    plane_w.step(2)
    plane_w.step(3)
    lax.fori_loop(9, LOADS, turn, 0)
    most = pl.ds(0, groups - 1)
    others = send(ids.at[most], ids.at[most], id_send.at[3], id_recv.at[3], at(up))
    others.wait_recv()
    all_ids = ids[...]
    strip_of = jnp.zeros_like(all_ids)
    for n in range(1, 4):
        strip_of = strip_of + jnp.where(all_ids >= n * STRIP, 1, 0)
    spots_of = all_ids - strip_of * STRIP
    for s in range(4):
        spots[s] = spots_of[:, s]
    to_smem = [pltpu.make_async_copy(spots.at[s], spots_s.at[s], spot_sem.at[s]) for s in range(4)]
    for copy in to_smem:
        copy.start()
    eye = (
        lax.broadcasted_iota(jnp.int32, (128, 128), 0) == lax.broadcasted_iota(jnp.int32, (128, 128), 1)
    ).astype(jnp.bfloat16)


    def look(s):
        to_smem[s].wait()

        def four(j, _):
            def some(i, _):
                g = (me + 4 * j + i) % groups
                for n in range(128):
                    rows[pl.ds(i * 128 + n, 1), :] = major[pl.ds(spots_s[s, g, n], 1), :]
                return 0

            lax.fori_loop(0, 4, some, 0)
            found = lax.dot_general(
                eye, rows[...].astype(jnp.bfloat16), (((1,), (1,)), ((), ())), preferred_element_type=jnp.float32
            )
            for i in range(4):
                g = (me + 4 * j + i) % groups
                word = ids[pl.ds(g, 1), pl.ds(s, 1), :].reshape(1, 128)
                part = found[:, i * 128 : (i + 1) * 128]
                chosen = part[:feats]
                for n in range(1, 4):
                    chosen = jnp.where(word >= n * STRIP, part[n * feats : (n + 1) * feats], chosen)
                chosen = chosen.astype(jnp.bfloat16)
                staged[s, pl.ds(4 * j + i, 1)] = chosen[None]

                def give():
                    send(staged.at[s, 4 * j + i], xt.at[s, me, y], look_send.at[s], look_recv.at[s], place(g, y)).start()

                if i:
                    give()
                else:
                    pl.when(j > 0)(give)

                    @pl.when(j == 0)
                    def _():
                        xt[s, pl.ds(me, 1), pl.ds(y, 1)] = chosen[None, None]

            return 0

        lax.fori_loop(0, 8, four, 0)

    def looked(s):
        return send(staged.at[s, most], xt.at[s, most, y], look_send.at[s], look_recv.at[s], at(up))

    def side(s, slot):
        first, count, of = ((0, groups, y), (0, groups, y), (0, groups // 2, down), (groups // 2, groups // 2, up))[slot]
        part = xt.at[s, pl.ds(first, count), of]
        return send(part, part, side_send.at[s, slot], side_recv.at[s, slot], at(down if slot % 2 else up))

    def gather(s):
        looked(s).wait_recv()
        side(s, 0).start()
        side(s, 1).start()

    def relay(s):
        for way in range(2):
            side(s, way).wait_recv()
            side(s, 2 + way).start()


    length = lens_ref[me]

    def prepare(s):
        for way in range(2):
            side(s, 2 + way).wait_recv()
        squares[...] = jnp.zeros_like(squares)

        def over(c, _):
            cols = pl.ds(pl.multiple_of(c * 128, 128), 128)
            piece = xt[s, pl.ds(c, 1)].reshape(128, 128).T
            xb[:, cols] = piece
            wide = piece.astype(jnp.float32)
            squares[...] += wide * wide
            return 0

        lax.fori_loop(0, width // 128, over, 0, unroll=4)
        scale = lax.rsqrt(jnp.sum(squares[...], axis=1, keepdims=True) / width + norm_eps)
        squares[...] = jnp.broadcast_to(scale, squares.shape)

        @pl.when(y == s)
        def _():
            own_x[...] = xb[...]

        here = slice(s * quarter, (s + 1) * quarter)

        def norm(c, _):
            cols = pl.ds(pl.multiple_of(c * 128, 128), 128)
            wide = xb[:, cols].astype(jnp.float32) * squares[...] * gain_ref[:, cols]
            normed[here, cols] = wide.astype(jnp.bfloat16)
            return 0

        lax.fori_loop(0, width // 128, norm, 0, unroll=4)
    def project(lo, hi):
        here = slice(lo * quarter, hi * quarter)

        def product(b, first):
            return jnp.dot(
                normed[here, :],
                w[b, :, :, :, :, first : first + 256].reshape(width, 256),
                preferred_element_type=jnp.float32,
            )

        def rotated(part):
            return (part * trig[0, here, :] + pltpu.roll(part, HD // 2, 1) * trig[1, here, :]).astype(jnp.bfloat16)

        def heads(b, _):
            for n in range(2):
                both = product(b, n * 256)
                for h in range(2):
                    q[pl.ds(b * 4 + n * 2 + h, 1), here] = rotated(both[:, h * HD : (h + 1) * HD])[None]
            both = product(b, 512)
            k[pl.ds(b, 1), here] = rotated(both[:, :HD])[None]
            v[pl.ds(b, 1), here] = both[:, HD:].astype(jnp.bfloat16)[None]
            return 0

        lax.fori_loop(0, 2, heads, 0)
        for b in range(2):
            cache[0, 0, here, b * HD : (b + 1) * HD] = k[b, here]
            cache[0, 1, here, b * HD : (b + 1) * HD] = v[b, here]

    def attend(s):
        here = slice(s * quarter, (s + 1) * quarter)
        keys = (s + 1) * quarter
        p = lax.broadcasted_iota(jnp.int32, (quarter, keys), 0) + s * quarter
        j = lax.broadcasted_iota(jnp.int32, (quarter, keys), 1)
        allowed = ((j <= p) & (j < length))[None]
        for b in range(2):
            scores = lax.dot_general(
                q[b * 4 : b * 4 + 4, here].reshape(4 * quarter, HD),
                k[b, :keys],
                (((1,), (1,)), ((), ())),
                preferred_element_type=jnp.float32,
            ).reshape(4, quarter, keys)
            scores = jnp.where(allowed, scores * np.float32(1 / np.sqrt(HD)), -1e30)
            expd = jnp.exp(scores - jnp.max(scores, axis=2, keepdims=True))
            weights = (expd / jnp.sum(expd, axis=2, keepdims=True)).astype(jnp.bfloat16)
            got = jnp.dot(weights.reshape(4 * quarter, keys), v[b, :keys], preferred_element_type=jnp.float32)
            got = got.astype(jnp.bfloat16)
            for h in range(4):
                attended[here, (b * 4 + h) * HD : (b * 4 + h + 1) * HD] = got[h * quarter : (h + 1) * quarter]

    look(0)
    plane_w.step(4)
    look(1)
    gather(0)
    plane_w.step(5)
    plane_w.step(6)
    look(2)
    gather(1)
    relay(0)
    plane_w.step(7)
    plane_w.step(8)
    look(3)
    gather(2)
    plane_w.step(9)
    relay(1)
    prepare(0)
    gather(3)
    plane_o.row_step(0)
    plane_w.step(10)
    relay(2)
    plane_w.step(11)
    angles.wait()
    project(0, 1)
    plane_o.row_step(1)
    attend(0)
    prepare(1)
    project(1, 2)
    attend(1)
    relay(3)
    prepare(2)
    plane_o.row_step(2)
    project(2, 3)
    attend(2)
    prepare(3)
    plane_o.row_step(3)
    project(3, 4)
    attend(3)


    def far_copy(c, way):
        return send(stage.at[c, far, way], mid.at[c, way], far_send.at[c, way], far_recv.at[c, way], at(down if way else up))

    def near_copy(c, way):
        part = stage.at[c, down if way else up, 1 - way]
        return send(part, final.at[c, way, 1 - way], near_send.at[c, way], near_recv.at[c, way], at(down if way else up))

    def sum_copy(c, way):
        return send(passed.at[c, way], final.at[c, way, way], sum_send.at[c, way], sum_recv.at[c, way], at(down if way else up))

    def wide(ref):
        return ref.reshape(quarter, 256).astype(jnp.float32)

    def pass_on(c):
        for way in range(2):
            far_copy(c, way).wait_recv()
            total = wide(stage[pl.ds(c, 1), pl.ds(down if way else up, 1), way]) + wide(mid[pl.ds(c, 1), way])
            passed[pl.ds(c, 1), way] = total.astype(jnp.bfloat16)[None]
            sum_copy(c, way).start()

    def row_of(c):
        g = c // 2
        return (z + g + g // 2 * (1 - 2 * (g % 2))) % 4

    def leave(c):
        cols = pl.ds(pl.multiple_of(row_of(c) * 1024 + c % 2 * 512, 512), 512)
        return pltpu.make_async_copy(hidden.at[:, cols], hidden_ref.at[:, cols], out_sems.at[c])

    def finish(c, _):
        for way in range(2):
            near_copy(c, way).wait_recv()
            sum_copy(c, way).wait_recv()
        for half in range(2):
            cols = pl.ds(pl.multiple_of(row_of(c) * 1024 + c % 2 * 512 + half * 256, 256), 256)
            total = wide(stage[pl.ds(c, 1), pl.ds(y, 1), half])
            for way in range(2):
                total = total + wide(final[pl.ds(c, 1), way, half])
            hidden[:, cols] = (own_x[:, cols].astype(jnp.float32) + total).astype(jnp.bfloat16)
        leave(c).start()
        return 0

    chunks = stage.shape[0]

    def output(c, _):
        for half in range(2):
            part = jnp.dot(attended[:, :512], wo[0, row_of(c), c % 2, half], preferred_element_type=jnp.float32)
            part = part + jnp.dot(attended[:, 512:], wo[1, row_of(c), c % 2, half], preferred_element_type=jnp.float32)
            part = part.astype(jnp.bfloat16)
            for member in range(4):
                stage[pl.ds(c, 1), member, half] = part[member * quarter : (member + 1) * quarter][None]
        for way in range(2):
            far_copy(c, way).start()
        for way in range(2):
            near_copy(c, way).start()

        @pl.when(c > 0)
        def _():
            pass_on(c - 1)

        @pl.when(c > 1)
        def _():
            finish(c - 2, 0)

        return 0

    plane_o.row_ready(0)
    cache_out = pltpu.make_async_copy(cache, cache_ref, own_sems.at[5])
    lax.fori_loop(0, 1, output, 0)
    plane_o.row_step(4)
    cache_out.start()
    lax.fori_loop(1, 2, output, 0)
    plane_o.row_ready(1)
    lax.fori_loop(2, 4, output, 0)
    plane_o.row_step(5)
    plane_o.row_ready(3)
    lax.fori_loop(4, 6, output, 0)
    others.wait_send()
    for s in range(4):
        looked(s).wait_send()
        for slot in range(4):
            side(s, slot).wait_send()
    plane_w.drain()
    plane_o.drain()
    plane_o.row_ready(2)
    lax.fori_loop(6, chunks, output, 0)
    pass_on(chunks - 1)
    lax.fori_loop(chunks - 2, chunks, finish, 0)
    def drain(c, _):
        for way in range(2):
            far_copy(c, way).wait_send()
            near_copy(c, way).wait_send()
            sum_copy(c, way).wait_send()
        leave(c).wait()
        return 0

    lax.fori_loop(0, chunks, drain, 0)
    cache_out.wait()


def shards(prompt_ids, prompt_lengths, embed_table, norm_gain, w_query, w_key, w_value, w_out):
    quarter = prompt_ids.shape[0]
    prompt = quarter * 4
    feats, vocab = embed_table.shape
    width = feats * lax.axis_size(AXES)
    depth, across = w_query.shape[0], w_query.shape[1] + w_key.shape[1] + w_value.shape[1]
    groups = prompt_lengths.shape[0]
    angle = np.arange(prompt)[:, None] * rope_theta ** (-2.0 * np.arange(HD // 2) / HD)[None, :]
    cosine = np.concatenate([np.cos(angle), np.cos(angle)], axis=1).astype(np.float32)
    sine = np.concatenate([-np.sin(angle), np.sin(angle)], axis=1).astype(np.float32)
    chunks = width // 512
    bf, f32 = jnp.bfloat16, jnp.float32
    vmem = pl.BlockSpec(memory_space=pltpu.VMEM)
    anyw = pl.BlockSpec(memory_space=pl.ANY)
    dma = pltpu.SemaphoreType.DMA
    return pl.pallas_call(
        kernel,
        out_shape=(
            jax.ShapeDtypeStruct((quarter, width), bf),
            jax.ShapeDtypeStruct((1, 2, prompt, 2 * HD), bf),
        ),
        in_specs=[pl.BlockSpec(memory_space=pltpu.SMEM)] + [vmem] * 2 + [anyw] * 6,
        out_specs=(anyw, anyw),
        scratch_shapes=[
            pltpu.VMEM((2, 4, feats, TILES * 128), bf),
            pltpu.VMEM((STRIP, 128), f32),
            pltpu.VMEM((512, 128), f32),
            pltpu.VMEM((groups, 4, 128), jnp.int32),
            pltpu.VMEM((4, groups, 128), jnp.int32),
            pltpu.SMEM((4, groups, 128), jnp.int32),
            pltpu.VMEM((4, groups, feats, 128), bf),
            pltpu.VMEM((4, groups, 4, feats, 128), bf),
            pltpu.VMEM((2, 4, 2, 2, depth, across), bf),
            pltpu.VMEM((2, 4, 2, 2, *w_out.shape), bf),
            pltpu.VMEM((quarter, width), bf),
            pltpu.VMEM((1, 2, prompt, 2 * HD), bf),
            pltpu.VMEM((quarter, width), bf),
            pltpu.VMEM((quarter, width), bf),
            pltpu.VMEM((prompt, width), bf),
            pltpu.VMEM((2, prompt, HD), f32),
            pltpu.VMEM((quarter, 128), f32),
            pltpu.VMEM((8, prompt, HD), bf),
            pltpu.VMEM((2, prompt, HD), bf),
            pltpu.VMEM((2, prompt, HD), bf),
            pltpu.VMEM((prompt, 1024), bf),
            pltpu.VMEM((chunks, 4, 2, quarter, 256), bf),
            pltpu.VMEM((chunks, 2, quarter, 256), bf),
            pltpu.VMEM((chunks, 2, quarter, 256), bf),
            pltpu.VMEM((chunks, 2, 2, quarter, 256), bf),
            dma((2, 4)),
            dma((4,)),
            dma((6,)),
            dma((chunks,)),
            dma((4,)),
            dma((4,)),
            dma((4,)),
            dma((4,)),
            dma((4, 4)),
            dma((4, 4)),
        ]
        + [dma((chunks, 2))] * 6
        + Plane.sems()
        + Plane.sems(),
        compiler_params=pltpu.CompilerParams(vmem_limit_bytes=67043328, collective_id=0, has_side_effects=True),
    )(
        prompt_lengths,
        prompt_ids.reshape(1, quarter),
        norm_gain.reshape(1, width),
        np.stack([cosine, sine]),
        embed_table,
        w_query,
        w_key,
        w_value,
        w_out,
    )


def solution(mesh):
    split = Mesh(mesh.devices.reshape(4, 2, 2, 2, 4), AXES)
    placed = (
        P(AXES),
        P(),
        P(AXES, None),
        P(),
        P(DP, TENSOR),
        P(DP, TENSOR),
        P(DP, TENSOR),
        P(TENSOR, DP),
    )
    return jax.shard_map(
        shards,
        mesh=split,
        in_specs=placed,
        out_specs=(P(AXES, None), P(AXES, None, None, None)),
        check_vma=False,
    )
```

```python
import jax
import jax.numpy as jnp
import numpy as np
from jax import lax
from jax.experimental import pallas as pl
from jax.experimental.pallas import tpu as pltpu
from jax.sharding import Mesh
from jax.sharding import PartitionSpec as P

HD = 128
AXES = ("z", "xlo", "core", "xhi", "y")
DP = ("z", "xlo", "core")
TENSOR = ("xhi", "y")
MESH = pl.DeviceIdType.MESH

norm_eps = 1e-05
rope_theta = 500000.0

BLOCKS = 252
STRIP = BLOCKS * 128
TILES = 21
LOADS = BLOCKS // TILES


class Plane:
    def __init__(self, whole, own, sems, by_row=False):
        self.whole, self.own, self.by_row = whole, own, by_row
        self.send, self.recv, self.core_send, self.core_recv = sems
        self.z = lax.axis_index("z")
        self.xlo = lax.axis_index("xlo")
        self.core = lax.axis_index("core")
        self.xhi = lax.axis_index("xhi")
        self.y = lax.axis_index("y")
        self.x = self.xhi * 2 + self.xlo
        self.half = whole.shape[4] // 2

    def neighbours(self):
        found = []
        for cls in range(2):
            for way in range(2):
                found.append(self.device(cls, self.first(cls) + (3 if way else 1), self.second(cls)))
        found.append((self.z, self.xlo, 1 - self.core, self.xhi, self.y))
        return found

    def first(self, cls):
        return self.x if cls else self.z

    def second(self, cls):
        return self.z if cls else self.x

    def device(self, cls, f, s):
        f, s = f % 4, s % 4
        x, z = (f, s) if cls else (s, f)
        return (z, x % 2, self.core, x // 2, self.y)

    def rows(self, cls, part):
        if part is None:
            return pl.ds(cls * self.half, self.half)
        return pl.ds(cls * self.half + part * (self.half // 2), self.half // 2)

    def piece(self, cls, f, s, part=None):
        f, s = f % 4, s % 4
        x, z = (f, s) if cls else (s, f)
        return self.whole.at[x // 2, z, x % 2, self.core, self.rows(cls, part)]

    def copy(self, cls, stage, slot, f, s, part, own):
        step = 3 if slot % 2 else 1
        pf, ps = self.first(cls), self.second(cls)
        to = self.device(cls, pf + step, ps) if stage == 0 else self.device(cls, pf, ps + step)
        dst = self.piece(cls, f, s, part)
        src = self.own.at[self.rows(cls, part)] if own else dst
        return pltpu.make_async_remote_copy(
            src, dst, self.send.at[cls, stage, slot], self.recv.at[cls, stage, slot], device_id=to, device_id_type=MESH
        )

    def full(self, cls, stage, way):
        o = max(stage - 1, 0)
        return self.copy(cls, stage, way, self.first(cls) + o, self.second(cls), None, o == 0)

    def relay(self, cls, stage, way):
        step = 1 if way else 3
        f, s = self.first(cls), self.second(cls)
        if stage == 0:
            f = f + step
        else:
            f, s = f + stage - 1, s + step
        return self.copy(cls, stage, 2 + way, f, s, way, False)

    def cores(self, cls, o):
        s = ((self.z if self.by_row else self.second(cls)) + o) % 4
        if cls or self.by_row:
            ref = self.whole.at[:, s, :, self.core, self.rows(cls, None)]
        else:
            ref = self.whole.at[s // 2, :, s % 2, self.core, self.rows(cls, None)]
        return pltpu.make_async_remote_copy(
            ref,
            ref,
            self.core_send.at[cls, o],
            self.core_recv.at[cls, o],
            device_id=(self.z, self.xlo, 1 - self.core, self.xhi, self.y),
            device_id_type=MESH,
        )

    def each(self, act, *args):
        for cls in range(2):
            for way in range(2):
                act(cls, way, *args)

    def start_full(self, *stages):
        for stage in stages:
            self.each(lambda cls, way: self.full(cls, stage, way).start())

    def take_full(self, *stages):
        for stage in stages:
            self.each(lambda cls, way: self.full(cls, stage, way).wait_recv())
            self.each(lambda cls, way: self.relay(cls, stage, way).start())

    def take_relay(self, *stages):
        for stage in stages:
            self.each(lambda cls, way: self.relay(cls, stage, way).wait_recv())

    def start_cores(self, cls, *offsets):
        for o in offsets:
            self.cores(cls, o).start()

    def row_step(self, n):
        ways = range(2)
        if n == 0:
            self.start_full(0, 1)
        elif n == 1:
            self.take_full(0)
            self.start_full(2, 4)
        elif n == 2:
            self.take_relay(0)
            self.take_full(1)
            self.start_cores(1, 0)
            self.start_full(3)
        elif n == 3:
            for way in ways:
                self.relay(0, 1, way).wait_recv()
            self.start_cores(0, 0)
            self.take_full(2, 4)
        elif n == 4:
            self.take_full(3)
            self.start_cores(1, 1, 3)
            for stage in (2, 4):
                for way in ways:
                    self.relay(0, stage, way).wait_recv()
            self.start_cores(0, 1, 3)
        else:
            for way in ways:
                self.relay(0, 3, way).wait_recv()
                for stage in range(1, 5):
                    self.relay(1, stage, way).wait_recv()
            self.start_cores(0, 2)
            self.start_cores(1, 2)

    def row_ready(self, o):
        for cls in range(2):
            self.cores(cls, o).wait_recv()

    def drain(self):
        for cls in range(2):
            for o in range(4):
                self.cores(cls, o).wait_send()
        for stage in range(5):
            self.each(lambda cls, way: self.full(cls, stage, way).wait_send())
            self.each(lambda cls, way: self.relay(cls, stage, way).wait_send())

    def step(self, n):
        if n == 0:
            self.start_full(0)
        elif n == 1:
            self.start_full(1)
        elif n == 2:
            self.take_full(0)
        elif n == 3:
            self.start_full(2)
        elif n == 4:
            self.start_full(4)
        elif n == 5:
            self.take_relay(0)
            self.start_full(3)
        elif n == 6:
            self.take_full(1)
        elif n == 7:
            self.start_cores(0, 0)
            self.start_cores(1, 0)
            self.take_full(2)
        elif n == 8:
            self.take_full(4)
        elif n == 9:
            self.take_full(3)
            for cls in range(2):
                self.start_cores(cls, 1, 3)
        elif n == 10:
            self.take_relay(1, 2, 3, 4)
            for cls in range(2):
                self.start_cores(cls, 2)
        else:
            for o in range(4):
                self.row_ready(o)

    @staticmethod
    def sems():
        dma = pltpu.SemaphoreType.DMA
        return [dma((2, 5, 4)), dma((2, 5, 4)), dma((2, 4)), dma((2, 4))]


def place(g, y):
    return (g // 8, g // 4 % 2, g // 2 % 2, g % 2, y)


def kernel(lens_ref, ids_ref, gain_ref, trig_ref, table_ref, wq_ref, wk_ref, wv_ref, wo_ref, hidden_ref, cache_ref,
           raw, major, rows, ids, spots, spots_s, staged, xt, w, wo, hidden, cache, own_x, xb, normed, trig, squares, q, k, v, attended,
           stage, mid, passed, final, table_sems, spot_sem, own_sems, out_sems, id_send, id_recv, look_send, look_recv,
           side_send, side_recv, far_send, far_recv, near_send, near_recv, sum_send, sum_recv, *plane_sems):
    feats, vocab = table_ref.shape
    z = lax.axis_index("z")
    xlo = lax.axis_index("xlo")
    core = lax.axis_index("core")
    xhi = lax.axis_index("xhi")
    y = lax.axis_index("y")
    me = ((z * 2 + xlo) * 2 + core) * 2 + xhi
    groups = ids.shape[0]
    quarter, width = hidden.shape
    up = (y + 1) % 4
    down = (y + 3) % 4
    far = (y + 2) % 4
    tiles = vocab // 128

    def at(member):
        return place(me, member)

    def send(src, dst, ssem, rsem, device):
        return pltpu.make_async_remote_copy(src, dst, ssem, rsem, device_id=device, device_id_type=MESH)

    barrier = pltpu.get_barrier_semaphore()
    for n in range(1, 4):
        pl.semaphore_signal(barrier, inc=1, device_id=at((y + n) % 4), device_id_type=MESH)

    def greet(n, _):
        pl.semaphore_signal(barrier, inc=1, device_id=place((me + n) % groups, y), device_id_type=MESH)
        return 0

    lax.fori_loop(1, groups, greet, 0)


    def table_base(n, strip):
        return jnp.minimum(strip * BLOCKS + n * TILES, tiles - TILES)

    def table_copy(n, strip):
        first = pl.multiple_of(table_base(n, strip) * 128, 128)
        return pltpu.make_async_copy(
            table_ref.at[:, pl.ds(first, TILES * 128)], raw.at[n % 2, strip], table_sems.at[n % 2, strip]
        )

    for n in range(2):
        for strip in range(4):
            table_copy(n, strip).start()
    own_w = w.at[xhi, z, xlo, core]
    own_wo = wo.at[xhi, z, xlo, core]
    mine = [
        pltpu.make_async_copy(ref, own_w.at[:, pl.ds(first, ref.shape[1])], own_sems.at[n])
        for n, (ref, first) in enumerate(((wq_ref, 0), (wk_ref, 512), (wv_ref, 640)))
    ] + [pltpu.make_async_copy(wo_ref, own_wo, own_sems.at[3])]
    angles = pltpu.make_async_copy(trig_ref, trig, own_sems.at[4])
    angles.start()
    for copy in mine:
        copy.start()
    plane_w = Plane(w, own_w, plane_sems[:4])
    plane_o = Plane(wo, own_wo, plane_sems[4:], True)

    def turn(n, _):
        for strip in range(4):
            table_copy(n, strip).wait()

        def tile(t, _):
            parts = []
            for strip in range(4):
                first = jnp.minimum(strip * BLOCKS + n * TILES + t, tiles - 1) - table_base(n, strip)
                parts.append(raw[n % 2, strip, :, pl.ds(pl.multiple_of(first * 128, 128), 128)])
            block = jnp.concatenate(parts, axis=0)
            major[pl.ds(pl.multiple_of((n * TILES + t) * 128, 128), 128), :] = block.T.astype(jnp.float32)
            return 0

        lax.fori_loop(0, TILES, tile, 0, unroll=7)

        @pl.when(n + 2 < LOADS)
        def _():
            for strip in range(4):
                table_copy(n + 2, strip).start()

        return 0

    lax.fori_loop(0, 1, turn, 0)
    pl.semaphore_wait(barrier, 3 + groups - 1)
    ids[pl.ds(me, 1), pl.ds(y, 1), :] = ids_ref[...][None]
    line = [
        send(ids_ref, ids.at[me, pl.ds(y, 1)], id_send.at[n - 1], id_recv.at[n - 1], at((y + n) % 4)) for n in range(1, 4)
    ]
    for copy in line:
        copy.start()
    for copy in mine:
        copy.wait()
    plane_w.step(0)
    lax.fori_loop(1, 4, turn, 0)
    for copy in line:
        copy.wait()

    def spread(n, _):
        send(ids.at[me], ids.at[me], id_send.at[3], id_recv.at[3], place((me + n) % groups, y)).start()
        return 0

    lax.fori_loop(1, groups, spread, 0)
    plane_w.step(1)
    lax.fori_loop(4, 9, turn, 0)
    plane_w.step(2)
    plane_w.step(3)
    lax.fori_loop(9, LOADS, turn, 0)
    most = pl.ds(0, groups - 1)
    others = send(ids.at[most], ids.at[most], id_send.at[3], id_recv.at[3], at(up))
    others.wait_recv()
    all_ids = ids[...]
    strip_of = jnp.zeros_like(all_ids)
    for n in range(1, 4):
        strip_of = strip_of + jnp.where(all_ids >= n * STRIP, 1, 0)
    spots_of = all_ids - strip_of * STRIP
    for s in range(4):
        spots[s] = spots_of[:, s]
    to_smem = [pltpu.make_async_copy(spots.at[s], spots_s.at[s], spot_sem.at[s]) for s in range(4)]
    for copy in to_smem:
        copy.start()
    eye = (
        lax.broadcasted_iota(jnp.int32, (128, 128), 0) == lax.broadcasted_iota(jnp.int32, (128, 128), 1)
    ).astype(jnp.bfloat16)


    def look(s):
        to_smem[s].wait()

        def four(j, _):
            def some(i, _):
                g = (me + 4 * j + i) % groups
                for n in range(128):
                    rows[pl.ds(i * 128 + n, 1), :] = major[pl.ds(spots_s[s, g, n], 1), :]
                return 0

            lax.fori_loop(0, 4, some, 0)
            found = lax.dot_general(
                eye, rows[...].astype(jnp.bfloat16), (((1,), (1,)), ((), ())), preferred_element_type=jnp.float32
            )
            for i in range(4):
                g = (me + 4 * j + i) % groups
                word = ids[pl.ds(g, 1), pl.ds(s, 1), :].reshape(1, 128)
                part = found[:, i * 128 : (i + 1) * 128]
                chosen = part[:feats]
                for n in range(1, 4):
                    chosen = jnp.where(word >= n * STRIP, part[n * feats : (n + 1) * feats], chosen)
                chosen = chosen.astype(jnp.bfloat16)
                staged[s, pl.ds(4 * j + i, 1)] = chosen[None]

                def give():
                    send(staged.at[s, 4 * j + i], xt.at[s, me, y], look_send.at[s], look_recv.at[s], place(g, y)).start()

                if i:
                    give()
                else:
                    pl.when(j > 0)(give)

                    @pl.when(j == 0)
                    def _():
                        xt[s, pl.ds(me, 1), pl.ds(y, 1)] = chosen[None, None]

            return 0

        lax.fori_loop(0, 8, four, 0)

    def looked(s):
        return send(staged.at[s, most], xt.at[s, most, y], look_send.at[s], look_recv.at[s], at(up))

    def side(s, slot):
        first, count, of = ((0, groups, y), (0, groups, y), (0, groups // 2, down), (groups // 2, groups // 2, up))[slot]
        part = xt.at[s, pl.ds(first, count), of]
        return send(part, part, side_send.at[s, slot], side_recv.at[s, slot], at(down if slot % 2 else up))

    def gather(s):
        looked(s).wait_recv()
        side(s, 0).start()
        side(s, 1).start()

    def relay(s):
        for way in range(2):
            side(s, way).wait_recv()
            side(s, 2 + way).start()


    length = lens_ref[me]

    def prepare(s):
        for way in range(2):
            side(s, 2 + way).wait_recv()
        squares[...] = jnp.zeros_like(squares)

        def over(c, _):
            cols = pl.ds(pl.multiple_of(c * 128, 128), 128)
            piece = xt[s, pl.ds(c, 1)].reshape(128, 128).T
            xb[:, cols] = piece
            wide = piece.astype(jnp.float32)
            squares[...] += wide * wide
            return 0

        lax.fori_loop(0, width // 128, over, 0, unroll=4)
        scale = lax.rsqrt(jnp.sum(squares[...], axis=1, keepdims=True) / width + norm_eps)
        squares[...] = jnp.broadcast_to(scale, squares.shape)

        @pl.when(y == s)
        def _():
            own_x[...] = xb[...]

        here = slice(s * quarter, (s + 1) * quarter)

        def norm(c, _):
            cols = pl.ds(pl.multiple_of(c * 128, 128), 128)
            wide = xb[:, cols].astype(jnp.float32) * squares[...] * gain_ref[:, cols]
            normed[here, cols] = wide.astype(jnp.bfloat16)
            return 0

        lax.fori_loop(0, width // 128, norm, 0, unroll=4)
    def project(lo, hi):
        here = slice(lo * quarter, hi * quarter)

        def product(b, first):
            return jnp.dot(
                normed[here, :],
                w[b, :, :, :, :, first : first + 256].reshape(width, 256),
                preferred_element_type=jnp.float32,
            )

        def rotated(part):
            return (part * trig[0, here, :] + pltpu.roll(part, HD // 2, 1) * trig[1, here, :]).astype(jnp.bfloat16)

        def heads(b, _):
            for n in range(2):
                both = product(b, n * 256)
                for h in range(2):
                    q[pl.ds(b * 4 + n * 2 + h, 1), here] = rotated(both[:, h * HD : (h + 1) * HD])[None]
            both = product(b, 512)
            k[pl.ds(b, 1), here] = rotated(both[:, :HD])[None]
            v[pl.ds(b, 1), here] = both[:, HD:].astype(jnp.bfloat16)[None]
            return 0

        lax.fori_loop(0, 2, heads, 0)
        for b in range(2):
            cache[0, 0, here, b * HD : (b + 1) * HD] = k[b, here]
            cache[0, 1, here, b * HD : (b + 1) * HD] = v[b, here]

    def attend(s):
        here = slice(s * quarter, (s + 1) * quarter)
        keys = (s + 1) * quarter
        p = lax.broadcasted_iota(jnp.int32, (quarter, keys), 0) + s * quarter
        j = lax.broadcasted_iota(jnp.int32, (quarter, keys), 1)
        allowed = ((j <= p) & (j < length))[None]
        for b in range(2):
            scores = lax.dot_general(
                q[b * 4 : b * 4 + 4, here].reshape(4 * quarter, HD),
                k[b, :keys],
                (((1,), (1,)), ((), ())),
                preferred_element_type=jnp.float32,
            ).reshape(4, quarter, keys)
            scores = jnp.where(allowed, scores * np.float32(1 / np.sqrt(HD)), -1e30)
            expd = jnp.exp(scores - jnp.max(scores, axis=2, keepdims=True))
            weights = (expd / jnp.sum(expd, axis=2, keepdims=True)).astype(jnp.bfloat16)
            got = jnp.dot(weights.reshape(4 * quarter, keys), v[b, :keys], preferred_element_type=jnp.float32)
            got = got.astype(jnp.bfloat16)
            for h in range(4):
                attended[here, (b * 4 + h) * HD : (b * 4 + h + 1) * HD] = got[h * quarter : (h + 1) * quarter]

    look(0)
    plane_w.step(4)
    look(1)
    gather(0)
    plane_w.step(5)
    plane_w.step(6)
    look(2)
    gather(1)
    relay(0)
    plane_w.step(7)
    plane_w.step(8)
    look(3)
    gather(2)
    plane_w.step(9)
    relay(1)
    prepare(0)
    gather(3)
    plane_o.row_step(0)
    plane_w.step(10)
    relay(2)
    plane_w.step(11)
    angles.wait()
    project(0, 1)
    plane_o.row_step(1)
    attend(0)
    prepare(1)
    project(1, 2)
    attend(1)
    relay(3)
    prepare(2)
    plane_o.row_step(2)
    project(2, 3)
    attend(2)
    prepare(3)
    plane_o.row_step(3)
    project(3, 4)
    attend(3)


    def far_copy(c, way):
        return send(stage.at[c, far, way], mid.at[c, way], far_send.at[c, way], far_recv.at[c, way], at(down if way else up))

    def near_copy(c, way):
        part = stage.at[c, down if way else up, 1 - way]
        return send(part, final.at[c, way, 1 - way], near_send.at[c, way], near_recv.at[c, way], at(down if way else up))

    def sum_copy(c, way):
        return send(passed.at[c, way], final.at[c, way, way], sum_send.at[c, way], sum_recv.at[c, way], at(down if way else up))

    def wide(ref):
        return ref.reshape(quarter, 256).astype(jnp.float32)

    def pass_on(c):
        for way in range(2):
            far_copy(c, way).wait_recv()
            total = wide(stage[pl.ds(c, 1), pl.ds(down if way else up, 1), way]) + wide(mid[pl.ds(c, 1), way])
            passed[pl.ds(c, 1), way] = total.astype(jnp.bfloat16)[None]
            sum_copy(c, way).start()

    def row_of(c):
        g = c // 2
        return (z + g + g // 2 * (1 - 2 * (g % 2))) % 4

    def leave(c):
        cols = pl.ds(pl.multiple_of(row_of(c) * 1024 + c % 2 * 512, 512), 512)
        return pltpu.make_async_copy(hidden.at[:, cols], hidden_ref.at[:, cols], out_sems.at[c])

    def finish(c, _):
        for way in range(2):
            near_copy(c, way).wait_recv()
            sum_copy(c, way).wait_recv()
        for half in range(2):
            cols = pl.ds(pl.multiple_of(row_of(c) * 1024 + c % 2 * 512 + half * 256, 256), 256)
            total = wide(stage[pl.ds(c, 1), pl.ds(y, 1), half])
            for way in range(2):
                total = total + wide(final[pl.ds(c, 1), way, half])
            hidden[:, cols] = (own_x[:, cols].astype(jnp.float32) + total).astype(jnp.bfloat16)
        leave(c).start()
        return 0

    chunks = stage.shape[0]

    def output(c, _):
        for half in range(2):
            part = jnp.dot(attended[:, :512], wo[0, row_of(c), c % 2, half], preferred_element_type=jnp.float32)
            part = part + jnp.dot(attended[:, 512:], wo[1, row_of(c), c % 2, half], preferred_element_type=jnp.float32)
            part = part.astype(jnp.bfloat16)
            for member in range(4):
                stage[pl.ds(c, 1), member, half] = part[member * quarter : (member + 1) * quarter][None]
        for way in range(2):
            far_copy(c, way).start()
        for way in range(2):
            near_copy(c, way).start()

        @pl.when(c > 0)
        def _():
            pass_on(c - 1)

        @pl.when(c > 1)
        def _():
            finish(c - 2, 0)

        return 0

    plane_o.row_ready(0)
    cache_out = pltpu.make_async_copy(cache, cache_ref, own_sems.at[5])
    lax.fori_loop(0, 1, output, 0)
    plane_o.row_step(4)
    cache_out.start()
    lax.fori_loop(1, 2, output, 0)
    plane_o.row_ready(1)
    lax.fori_loop(2, 4, output, 0)
    plane_o.row_step(5)
    plane_o.row_ready(3)
    lax.fori_loop(4, 6, output, 0)
    others.wait_send()
    for s in range(4):
        looked(s).wait_send()
        for slot in range(4):
            side(s, slot).wait_send()
    plane_w.drain()
    plane_o.drain()
    plane_o.row_ready(2)
    lax.fori_loop(6, chunks, output, 0)
    pass_on(chunks - 1)
    lax.fori_loop(chunks - 2, chunks, finish, 0)
    def drain(c, _):
        for way in range(2):
            far_copy(c, way).wait_send()
            near_copy(c, way).wait_send()
            sum_copy(c, way).wait_send()
        leave(c).wait()
        return 0

    lax.fori_loop(0, chunks, drain, 0)
    cache_out.wait()


def settle_kernel(first_ref, second_ref, first_out, second_out, first, second, sems):
    pieces = []
    for n in range(4):
        part = pl.ds(n * (first.shape[0] // 4), first.shape[0] // 4)
        pieces.append((first_ref.at[part], first.at[part], first_out.at[part]))
    for n in range(2):
        pieces.append((second_ref.at[0, n], second.at[0, n], second_out.at[0, n]))
    ways = [
        (pltpu.make_async_copy(a, b, sems.at[0, n]), pltpu.make_async_copy(b, c, sems.at[1, n]))
        for n, (a, b, c) in enumerate(pieces)
    ]
    for into, _ in ways:
        into.start()
    for into, out in ways:
        into.wait()
        out.start()
    for _, out in ways:
        out.wait()


def settle(first, second):
    anyw = pl.BlockSpec(memory_space=pl.ANY)
    return pl.pallas_call(
        settle_kernel,
        out_shape=(jax.ShapeDtypeStruct(first.shape, first.dtype), jax.ShapeDtypeStruct(second.shape, second.dtype)),
        in_specs=[anyw, anyw],
        out_specs=(anyw, anyw),
        scratch_shapes=[
            pltpu.VMEM(first.shape, first.dtype),
            pltpu.VMEM(second.shape, second.dtype),
            pltpu.SemaphoreType.DMA((2, 6)),
        ],
        compiler_params=pltpu.CompilerParams(vmem_limit_bytes=67043328),
    )(first, second)


def shards(prompt_ids, prompt_lengths, embed_table, norm_gain, w_query, w_key, w_value, w_out):
    quarter = prompt_ids.shape[0]
    prompt = quarter * 4
    feats, vocab = embed_table.shape
    width = feats * lax.axis_size(AXES)
    depth, across = w_query.shape[0], w_query.shape[1] + w_key.shape[1] + w_value.shape[1]
    groups = prompt_lengths.shape[0]
    angle = np.arange(prompt)[:, None] * rope_theta ** (-2.0 * np.arange(HD // 2) / HD)[None, :]
    cosine = np.concatenate([np.cos(angle), np.cos(angle)], axis=1).astype(np.float32)
    sine = np.concatenate([-np.sin(angle), np.sin(angle)], axis=1).astype(np.float32)
    chunks = width // 512
    bf, f32 = jnp.bfloat16, jnp.float32
    vmem = pl.BlockSpec(memory_space=pltpu.VMEM)
    anyw = pl.BlockSpec(memory_space=pl.ANY)
    dma = pltpu.SemaphoreType.DMA
    hidden, cache = pl.pallas_call(
        kernel,
        out_shape=(
            jax.ShapeDtypeStruct((quarter, width), bf),
            jax.ShapeDtypeStruct((1, 2, prompt, 2 * HD), bf),
        ),
        in_specs=[pl.BlockSpec(memory_space=pltpu.SMEM)] + [vmem] * 2 + [anyw] * 6,
        out_specs=(anyw, anyw),
        scratch_shapes=[
            pltpu.VMEM((2, 4, feats, TILES * 128), bf),
            pltpu.VMEM((STRIP, 128), f32),
            pltpu.VMEM((512, 128), f32),
            pltpu.VMEM((groups, 4, 128), jnp.int32),
            pltpu.VMEM((4, groups, 128), jnp.int32),
            pltpu.SMEM((4, groups, 128), jnp.int32),
            pltpu.VMEM((4, groups, feats, 128), bf),
            pltpu.VMEM((4, groups, 4, feats, 128), bf),
            pltpu.VMEM((2, 4, 2, 2, depth, across), bf),
            pltpu.VMEM((2, 4, 2, 2, *w_out.shape), bf),
            pltpu.VMEM((quarter, width), bf),
            pltpu.VMEM((1, 2, prompt, 2 * HD), bf),
            pltpu.VMEM((quarter, width), bf),
            pltpu.VMEM((quarter, width), bf),
            pltpu.VMEM((prompt, width), bf),
            pltpu.VMEM((2, prompt, HD), f32),
            pltpu.VMEM((quarter, 128), f32),
            pltpu.VMEM((8, prompt, HD), bf),
            pltpu.VMEM((2, prompt, HD), bf),
            pltpu.VMEM((2, prompt, HD), bf),
            pltpu.VMEM((prompt, 1024), bf),
            pltpu.VMEM((chunks, 4, 2, quarter, 256), bf),
            pltpu.VMEM((chunks, 2, quarter, 256), bf),
            pltpu.VMEM((chunks, 2, quarter, 256), bf),
            pltpu.VMEM((chunks, 2, 2, quarter, 256), bf),
            dma((2, 4)),
            dma((4,)),
            dma((6,)),
            dma((chunks,)),
            dma((4,)),
            dma((4,)),
            dma((4,)),
            dma((4,)),
            dma((4, 4)),
            dma((4, 4)),
        ]
        + [dma((chunks, 2))] * 6
        + Plane.sems()
        + Plane.sems(),
        compiler_params=pltpu.CompilerParams(vmem_limit_bytes=67043328, collective_id=0, has_side_effects=True),
    )(
        prompt_lengths,
        prompt_ids.reshape(1, quarter),
        norm_gain.reshape(1, width),
        np.stack([cosine, sine]),
        embed_table,
        w_query,
        w_key,
        w_value,
        w_out,
    )
    return settle(hidden, cache)


def solution(mesh):
    split = Mesh(mesh.devices.reshape(4, 2, 2, 2, 4), AXES)
    placed = (
        P(AXES),
        P(),
        P(AXES, None),
        P(),
        P(DP, TENSOR),
        P(DP, TENSOR),
        P(DP, TENSOR),
        P(TENSOR, DP),
    )
    return jax.shard_map(
        shards,
        mesh=split,
        in_specs=placed,
        out_specs=(P(AXES, None), P(AXES, None, None, None)),
        check_vma=False,
    )
```

```python
import jax
import jax.numpy as jnp
import numpy as np
from jax import lax
from jax.experimental import pallas as pl
from jax.experimental.pallas import tpu as pltpu
from jax.sharding import Mesh
from jax.sharding import PartitionSpec as P

HD = 128
AXES = ("z", "xlo", "core", "xhi", "y")
DP = ("z", "xlo", "core")
TENSOR = ("xhi", "y")
MESH = pl.DeviceIdType.MESH

norm_eps = 1e-05
rope_theta = 500000.0

BLOCKS = 252
STRIP = BLOCKS * 128
TILES = 21
LOADS = BLOCKS // TILES


class Plane:
    def __init__(self, whole, own, sems, by_row=False):
        self.whole, self.own, self.by_row = whole, own, by_row
        self.send, self.recv, self.core_send, self.core_recv = sems
        self.z = lax.axis_index("z")
        self.xlo = lax.axis_index("xlo")
        self.core = lax.axis_index("core")
        self.xhi = lax.axis_index("xhi")
        self.y = lax.axis_index("y")
        self.x = self.xhi * 2 + self.xlo
        self.half = whole.shape[4] // 2

    def neighbours(self):
        found = []
        for cls in range(2):
            for way in range(2):
                found.append(self.device(cls, self.first(cls) + (3 if way else 1), self.second(cls)))
        found.append((self.z, self.xlo, 1 - self.core, self.xhi, self.y))
        return found

    def first(self, cls):
        return self.x if cls else self.z

    def second(self, cls):
        return self.z if cls else self.x

    def device(self, cls, f, s):
        f, s = f % 4, s % 4
        x, z = (f, s) if cls else (s, f)
        return (z, x % 2, self.core, x // 2, self.y)

    def rows(self, cls, part):
        if part is None:
            return pl.ds(cls * self.half, self.half)
        return pl.ds(cls * self.half + part * (self.half // 2), self.half // 2)

    def piece(self, cls, f, s, part=None):
        f, s = f % 4, s % 4
        x, z = (f, s) if cls else (s, f)
        return self.whole.at[x // 2, z, x % 2, self.core, self.rows(cls, part)]

    def copy(self, cls, stage, slot, f, s, part, own):
        step = 3 if slot % 2 else 1
        pf, ps = self.first(cls), self.second(cls)
        to = self.device(cls, pf + step, ps) if stage == 0 else self.device(cls, pf, ps + step)
        dst = self.piece(cls, f, s, part)
        src = self.own.at[self.rows(cls, part)] if own else dst
        return pltpu.make_async_remote_copy(
            src, dst, self.send.at[cls, stage, slot], self.recv.at[cls, stage, slot], device_id=to, device_id_type=MESH
        )

    def full(self, cls, stage, way):
        o = max(stage - 1, 0)
        return self.copy(cls, stage, way, self.first(cls) + o, self.second(cls), None, o == 0)

    def relay(self, cls, stage, way):
        step = 1 if way else 3
        f, s = self.first(cls), self.second(cls)
        if stage == 0:
            f = f + step
        else:
            f, s = f + stage - 1, s + step
        return self.copy(cls, stage, 2 + way, f, s, way, False)

    def cores(self, cls, o):
        s = ((self.z if self.by_row else self.second(cls)) + o) % 4
        if cls or self.by_row:
            ref = self.whole.at[:, s, :, self.core, self.rows(cls, None)]
        else:
            ref = self.whole.at[s // 2, :, s % 2, self.core, self.rows(cls, None)]
        return pltpu.make_async_remote_copy(
            ref,
            ref,
            self.core_send.at[cls, o],
            self.core_recv.at[cls, o],
            device_id=(self.z, self.xlo, 1 - self.core, self.xhi, self.y),
            device_id_type=MESH,
        )

    def each(self, act, *args):
        for cls in range(2):
            for way in range(2):
                act(cls, way, *args)

    def start_full(self, *stages):
        for stage in stages:
            self.each(lambda cls, way: self.full(cls, stage, way).start())

    def take_full(self, *stages):
        for stage in stages:
            self.each(lambda cls, way: self.full(cls, stage, way).wait_recv())
            self.each(lambda cls, way: self.relay(cls, stage, way).start())

    def take_relay(self, *stages):
        for stage in stages:
            self.each(lambda cls, way: self.relay(cls, stage, way).wait_recv())

    def start_cores(self, cls, *offsets):
        for o in offsets:
            self.cores(cls, o).start()

    def row_step(self, n):
        ways = range(2)
        if n == 0:
            self.start_full(0, 1)
        elif n == 1:
            self.take_full(0)
            self.start_full(2, 4)
        elif n == 2:
            self.take_relay(0)
            self.take_full(1)
            self.start_cores(1, 0)
            self.start_full(3)
        elif n == 3:
            for way in ways:
                self.relay(0, 1, way).wait_recv()
            self.start_cores(0, 0)
            self.take_full(2, 4)
        elif n == 4:
            self.take_full(3)
            self.start_cores(1, 1, 3)
            for stage in (2, 4):
                for way in ways:
                    self.relay(0, stage, way).wait_recv()
            self.start_cores(0, 1, 3)
        else:
            for way in ways:
                self.relay(0, 3, way).wait_recv()
                for stage in range(1, 5):
                    self.relay(1, stage, way).wait_recv()
            self.start_cores(0, 2)
            self.start_cores(1, 2)

    def row_ready(self, o):
        for cls in range(2):
            self.cores(cls, o).wait_recv()

    def drain(self):
        for cls in range(2):
            for o in range(4):
                self.cores(cls, o).wait_send()
        for stage in range(5):
            self.each(lambda cls, way: self.full(cls, stage, way).wait_send())
            self.each(lambda cls, way: self.relay(cls, stage, way).wait_send())

    def step(self, n):
        if n == 0:
            self.start_full(0)
        elif n == 1:
            self.start_full(1)
        elif n == 2:
            self.take_full(0)
        elif n == 3:
            self.start_full(2)
        elif n == 4:
            self.start_full(4)
        elif n == 5:
            self.take_relay(0)
            self.start_full(3)
        elif n == 6:
            self.take_full(1)
        elif n == 7:
            self.start_cores(0, 0)
            self.start_cores(1, 0)
            self.take_full(2)
        elif n == 8:
            self.take_full(4)
        elif n == 9:
            self.take_full(3)
            for cls in range(2):
                self.start_cores(cls, 1, 3)
        elif n == 10:
            self.take_relay(1, 2, 3, 4)
            for cls in range(2):
                self.start_cores(cls, 2)
        else:
            for o in range(4):
                self.row_ready(o)

    @staticmethod
    def sems():
        dma = pltpu.SemaphoreType.DMA
        return [dma((2, 5, 4)), dma((2, 5, 4)), dma((2, 4)), dma((2, 4))]


def place(g, y):
    return (g // 8, g // 4 % 2, g // 2 % 2, g % 2, y)


def kernel(lens_ref, ids_ref, gain_ref, trig_ref, table_ref, wq_ref, wk_ref, wv_ref, wo_ref, hidden_ref, cache_ref,
           raw, major, rows, ids, spots, spots_s, staged, xt, w, wo, hidden, cache, own_x, xb, normed, trig, squares, q, k, v, attended,
           stage, mid, passed, final, table_sems, spot_sem, own_sems, out_sems, id_send, id_recv, look_send, look_recv,
           side_send, side_recv, far_send, far_recv, near_send, near_recv, sum_send, sum_recv, *plane_sems):
    feats, vocab = table_ref.shape
    z = lax.axis_index("z")
    xlo = lax.axis_index("xlo")
    core = lax.axis_index("core")
    xhi = lax.axis_index("xhi")
    y = lax.axis_index("y")
    me = ((z * 2 + xlo) * 2 + core) * 2 + xhi
    groups = ids.shape[0]
    quarter, width = hidden.shape
    up = (y + 1) % 4
    down = (y + 3) % 4
    far = (y + 2) % 4
    tiles = vocab // 128

    def at(member):
        return place(me, member)

    def send(src, dst, ssem, rsem, device):
        return pltpu.make_async_remote_copy(src, dst, ssem, rsem, device_id=device, device_id_type=MESH)

    barrier = pltpu.get_barrier_semaphore()
    for n in range(1, 4):
        pl.semaphore_signal(barrier, inc=1, device_id=at((y + n) % 4), device_id_type=MESH)

    def greet(n, _):
        pl.semaphore_signal(barrier, inc=1, device_id=place((me + n) % groups, y), device_id_type=MESH)
        return 0

    lax.fori_loop(1, groups, greet, 0)


    def table_base(n, strip):
        return jnp.minimum(strip * BLOCKS + n * TILES, tiles - TILES)

    def table_copy(n, strip):
        first = pl.multiple_of(table_base(n, strip) * 128, 128)
        return pltpu.make_async_copy(
            table_ref.at[:, pl.ds(first, TILES * 128)], raw.at[n % 2, strip], table_sems.at[n % 2, strip]
        )

    for n in range(2):
        for strip in range(4):
            table_copy(n, strip).start()
    own_w = w.at[xhi, z, xlo, core]
    own_wo = wo.at[xhi, z, xlo, core]
    mine = [
        pltpu.make_async_copy(ref, own_w.at[:, pl.ds(first, ref.shape[1])], own_sems.at[n])
        for n, (ref, first) in enumerate(((wq_ref, 0), (wk_ref, 512), (wv_ref, 640)))
    ] + [pltpu.make_async_copy(wo_ref, own_wo, own_sems.at[3])]
    angles = pltpu.make_async_copy(trig_ref, trig, own_sems.at[4])
    angles.start()
    for copy in mine:
        copy.start()
    plane_w = Plane(w, own_w, plane_sems[:4])
    plane_o = Plane(wo, own_wo, plane_sems[4:], True)

    def turn(n, _):
        for strip in range(4):
            table_copy(n, strip).wait()

        def tile(t, _):
            parts = []
            for strip in range(4):
                first = jnp.minimum(strip * BLOCKS + n * TILES + t, tiles - 1) - table_base(n, strip)
                parts.append(raw[n % 2, strip, :, pl.ds(pl.multiple_of(first * 128, 128), 128)])
            block = jnp.concatenate(parts, axis=0)
            major[pl.ds(pl.multiple_of((n * TILES + t) * 128, 128), 128), :] = block.T.astype(jnp.float32)
            return 0

        lax.fori_loop(0, TILES, tile, 0, unroll=7)

        @pl.when(n + 2 < LOADS)
        def _():
            for strip in range(4):
                table_copy(n + 2, strip).start()

        return 0

    lax.fori_loop(0, 1, turn, 0)
    pl.semaphore_wait(barrier, 3 + groups - 1)
    ids[pl.ds(me, 1), pl.ds(y, 1), :] = ids_ref[...][None]
    line = [
        send(ids_ref, ids.at[me, pl.ds(y, 1)], id_send.at[n - 1], id_recv.at[n - 1], at((y + n) % 4)) for n in range(1, 4)
    ]
    for copy in line:
        copy.start()
    for copy in mine:
        copy.wait()
    plane_w.step(0)
    lax.fori_loop(1, 4, turn, 0)
    for copy in line:
        copy.wait()

    def spread(n, _):
        send(ids.at[me], ids.at[me], id_send.at[3], id_recv.at[3], place((me + n) % groups, y)).start()
        return 0

    lax.fori_loop(1, groups, spread, 0)
    plane_w.step(1)
    lax.fori_loop(4, 9, turn, 0)
    plane_w.step(2)
    plane_w.step(3)
    lax.fori_loop(9, LOADS, turn, 0)
    most = pl.ds(0, groups - 1)
    others = send(ids.at[most], ids.at[most], id_send.at[3], id_recv.at[3], at(up))
    others.wait_recv()
    all_ids = ids[...]
    strip_of = jnp.zeros_like(all_ids)
    for n in range(1, 4):
        strip_of = strip_of + jnp.where(all_ids >= n * STRIP, 1, 0)
    spots_of = all_ids - strip_of * STRIP
    for s in range(4):
        spots[s] = spots_of[:, s]
    to_smem = [pltpu.make_async_copy(spots.at[s], spots_s.at[s], spot_sem.at[s]) for s in range(4)]
    for copy in to_smem:
        copy.start()
    eye = (
        lax.broadcasted_iota(jnp.int32, (128, 128), 0) == lax.broadcasted_iota(jnp.int32, (128, 128), 1)
    ).astype(jnp.bfloat16)


    def look(s):
        to_smem[s].wait()

        def four(j, _):
            def some(i, _):
                g = (me + 4 * j + i) % groups
                for n in range(128):
                    rows[pl.ds(i * 128 + n, 1), :] = major[pl.ds(spots_s[s, g, n], 1), :]
                return 0

            lax.fori_loop(0, 4, some, 0)
            found = lax.dot_general(
                eye, rows[...].astype(jnp.bfloat16), (((1,), (1,)), ((), ())), preferred_element_type=jnp.float32
            )
            for i in range(4):
                g = (me + 4 * j + i) % groups
                word = ids[pl.ds(g, 1), pl.ds(s, 1), :].reshape(1, 128)
                part = found[:, i * 128 : (i + 1) * 128]
                chosen = part[:feats]
                for n in range(1, 4):
                    chosen = jnp.where(word >= n * STRIP, part[n * feats : (n + 1) * feats], chosen)
                chosen = chosen.astype(jnp.bfloat16)
                staged[s, pl.ds(4 * j + i, 1)] = chosen[None]

                def give():
                    send(staged.at[s, 4 * j + i], xt.at[s, me, y], look_send.at[s], look_recv.at[s], place(g, y)).start()

                if i:
                    give()
                else:
                    pl.when(j > 0)(give)

                    @pl.when(j == 0)
                    def _():
                        xt[s, pl.ds(me, 1), pl.ds(y, 1)] = chosen[None, None]

            return 0

        lax.fori_loop(0, 8, four, 0)

    def looked(s):
        return send(staged.at[s, most], xt.at[s, most, y], look_send.at[s], look_recv.at[s], at(up))

    def side(s, slot):
        first, count, of = ((0, groups, y), (0, groups, y), (0, groups // 2, down), (groups // 2, groups // 2, up))[slot]
        part = xt.at[s, pl.ds(first, count), of]
        return send(part, part, side_send.at[s, slot], side_recv.at[s, slot], at(down if slot % 2 else up))

    def gather(s):
        looked(s).wait_recv()
        side(s, 0).start()
        side(s, 1).start()

    def relay(s):
        for way in range(2):
            side(s, way).wait_recv()
            side(s, 2 + way).start()


    length = lens_ref[me]

    def prepare(s):
        for way in range(2):
            side(s, 2 + way).wait_recv()
        squares[...] = jnp.zeros_like(squares)

        def over(c, _):
            cols = pl.ds(pl.multiple_of(c * 128, 128), 128)
            piece = xt[s, pl.ds(c, 1)].reshape(128, 128).T
            xb[:, cols] = piece
            wide = piece.astype(jnp.float32)
            squares[...] += wide * wide
            return 0

        lax.fori_loop(0, width // 128, over, 0, unroll=4)
        scale = lax.rsqrt(jnp.sum(squares[...], axis=1, keepdims=True) / width + norm_eps)
        squares[...] = jnp.broadcast_to(scale, squares.shape)

        @pl.when(y == s)
        def _():
            own_x[...] = xb[...]

        here = slice(s * quarter, (s + 1) * quarter)

        def norm(c, _):
            cols = pl.ds(pl.multiple_of(c * 128, 128), 128)
            wide = xb[:, cols].astype(jnp.float32) * squares[...] * gain_ref[:, cols]
            normed[here, cols] = wide.astype(jnp.bfloat16)
            return 0

        lax.fori_loop(0, width // 128, norm, 0, unroll=4)
    def project(lo, hi):
        here = slice(lo * quarter, hi * quarter)

        def product(b, first):
            return jnp.dot(
                normed[here, :],
                w[b, :, :, :, :, first : first + 256].reshape(width, 256),
                preferred_element_type=jnp.float32,
            )

        def rotated(part):
            return (part * trig[0, here, :] + pltpu.roll(part, HD // 2, 1) * trig[1, here, :]).astype(jnp.bfloat16)

        def heads(b, _):
            for n in range(2):
                both = product(b, n * 256)
                for h in range(2):
                    q[pl.ds(b * 4 + n * 2 + h, 1), here] = rotated(both[:, h * HD : (h + 1) * HD])[None]
            both = product(b, 512)
            k[pl.ds(b, 1), here] = rotated(both[:, :HD])[None]
            v[pl.ds(b, 1), here] = both[:, HD:].astype(jnp.bfloat16)[None]
            return 0

        lax.fori_loop(0, 2, heads, 0)
        for b in range(2):
            cache[0, 0, here, b * HD : (b + 1) * HD] = k[b, here]
            cache[0, 1, here, b * HD : (b + 1) * HD] = v[b, here]

    def attend(s):
        here = slice(s * quarter, (s + 1) * quarter)
        keys = (s + 1) * quarter
        p = lax.broadcasted_iota(jnp.int32, (quarter, keys), 0) + s * quarter
        j = lax.broadcasted_iota(jnp.int32, (quarter, keys), 1)
        allowed = ((j <= p) & (j < length))[None]
        for b in range(2):
            scores = lax.dot_general(
                q[b * 4 : b * 4 + 4, here].reshape(4 * quarter, HD),
                k[b, :keys],
                (((1,), (1,)), ((), ())),
                preferred_element_type=jnp.float32,
            ).reshape(4, quarter, keys)
            scores = jnp.where(allowed, scores * np.float32(1 / np.sqrt(HD)), -1e30)
            expd = jnp.exp(scores - jnp.max(scores, axis=2, keepdims=True))
            weights = (expd / jnp.sum(expd, axis=2, keepdims=True)).astype(jnp.bfloat16)
            got = jnp.dot(weights.reshape(4 * quarter, keys), v[b, :keys], preferred_element_type=jnp.float32)
            got = got.astype(jnp.bfloat16)
            for h in range(4):
                attended[here, (b * 4 + h) * HD : (b * 4 + h + 1) * HD] = got[h * quarter : (h + 1) * quarter]

    look(0)
    plane_w.step(4)
    look(1)
    gather(0)
    plane_w.step(5)
    plane_w.step(6)
    look(2)
    gather(1)
    relay(0)
    plane_w.step(7)
    plane_w.step(8)
    look(3)
    gather(2)
    plane_w.step(9)
    relay(1)
    prepare(0)
    gather(3)
    plane_o.row_step(0)
    plane_w.step(10)
    relay(2)
    prepare(1)
    plane_w.step(11)
    plane_o.row_step(1)
    angles.wait()
    project(0, 2)
    attend(0)
    relay(3)
    attend(1)
    prepare(2)
    plane_o.row_step(2)
    project(2, 3)
    attend(2)
    prepare(3)
    plane_o.row_step(3)
    project(3, 4)
    attend(3)


    def far_copy(c, way):
        return send(stage.at[c, far, way], mid.at[c, way], far_send.at[c, way], far_recv.at[c, way], at(down if way else up))

    def near_copy(c, way):
        part = stage.at[c, down if way else up, 1 - way]
        return send(part, final.at[c, way, 1 - way], near_send.at[c, way], near_recv.at[c, way], at(down if way else up))

    def sum_copy(c, way):
        return send(passed.at[c, way], final.at[c, way, way], sum_send.at[c, way], sum_recv.at[c, way], at(down if way else up))

    def wide(ref):
        return ref.reshape(quarter, 256).astype(jnp.float32)

    def pass_on(c):
        for way in range(2):
            far_copy(c, way).wait_recv()
            total = wide(stage[pl.ds(c, 1), pl.ds(down if way else up, 1), way]) + wide(mid[pl.ds(c, 1), way])
            passed[pl.ds(c, 1), way] = total.astype(jnp.bfloat16)[None]
            sum_copy(c, way).start()

    def row_of(c):
        g = c // 2
        return (z + g + g // 2 * (1 - 2 * (g % 2))) % 4

    def leave(c):
        cols = pl.ds(pl.multiple_of(row_of(c) * 1024 + c % 2 * 512, 512), 512)
        return pltpu.make_async_copy(hidden.at[:, cols], hidden_ref.at[:, cols], out_sems.at[c])

    def finish(c, _):
        for way in range(2):
            near_copy(c, way).wait_recv()
            sum_copy(c, way).wait_recv()
        for half in range(2):
            cols = pl.ds(pl.multiple_of(row_of(c) * 1024 + c % 2 * 512 + half * 256, 256), 256)
            total = wide(stage[pl.ds(c, 1), pl.ds(y, 1), half])
            for way in range(2):
                total = total + wide(final[pl.ds(c, 1), way, half])
            hidden[:, cols] = (own_x[:, cols].astype(jnp.float32) + total).astype(jnp.bfloat16)
        leave(c).start()
        return 0

    chunks = stage.shape[0]

    def output(c, _):
        for half in range(2):
            part = jnp.dot(attended[:, :512], wo[0, row_of(c), c % 2, half], preferred_element_type=jnp.float32)
            part = part + jnp.dot(attended[:, 512:], wo[1, row_of(c), c % 2, half], preferred_element_type=jnp.float32)
            part = part.astype(jnp.bfloat16)
            for member in range(4):
                stage[pl.ds(c, 1), member, half] = part[member * quarter : (member + 1) * quarter][None]
        for way in range(2):
            far_copy(c, way).start()
        for way in range(2):
            near_copy(c, way).start()

        @pl.when(c > 0)
        def _():
            pass_on(c - 1)

        @pl.when(c > 1)
        def _():
            finish(c - 2, 0)

        return 0

    plane_o.row_ready(0)
    cache_out = pltpu.make_async_copy(cache, cache_ref, own_sems.at[5])
    lax.fori_loop(0, 1, output, 0)
    plane_o.row_step(4)
    cache_out.start()
    lax.fori_loop(1, 2, output, 0)
    plane_o.row_ready(1)
    lax.fori_loop(2, 4, output, 0)
    plane_o.row_step(5)
    plane_o.row_ready(3)
    lax.fori_loop(4, 6, output, 0)
    others.wait_send()
    for s in range(4):
        looked(s).wait_send()
        for slot in range(4):
            side(s, slot).wait_send()
    plane_w.drain()
    plane_o.drain()
    plane_o.row_ready(2)
    lax.fori_loop(6, chunks, output, 0)
    pass_on(chunks - 1)
    lax.fori_loop(chunks - 2, chunks, finish, 0)
    def drain(c, _):
        for way in range(2):
            far_copy(c, way).wait_send()
            near_copy(c, way).wait_send()
            sum_copy(c, way).wait_send()
        leave(c).wait()
        return 0

    lax.fori_loop(0, chunks, drain, 0)
    cache_out.wait()


def settle_kernel(first_ref, second_ref, first_out, second_out, first, second, sems):
    pieces = []
    for n in range(4):
        part = pl.ds(n * (first.shape[0] // 4), first.shape[0] // 4)
        pieces.append((first_ref.at[part], first.at[part], first_out.at[part]))
    for n in range(2):
        pieces.append((second_ref.at[0, n], second.at[0, n], second_out.at[0, n]))
    ways = [
        (pltpu.make_async_copy(a, b, sems.at[0, n]), pltpu.make_async_copy(b, c, sems.at[1, n]))
        for n, (a, b, c) in enumerate(pieces)
    ]
    for into, _ in ways:
        into.start()
    for into, out in ways:
        into.wait()
        out.start()
    for _, out in ways:
        out.wait()


def settle(first, second):
    anyw = pl.BlockSpec(memory_space=pl.ANY)
    return pl.pallas_call(
        settle_kernel,
        out_shape=(jax.ShapeDtypeStruct(first.shape, first.dtype), jax.ShapeDtypeStruct(second.shape, second.dtype)),
        in_specs=[anyw, anyw],
        out_specs=(anyw, anyw),
        scratch_shapes=[
            pltpu.VMEM(first.shape, first.dtype),
            pltpu.VMEM(second.shape, second.dtype),
            pltpu.SemaphoreType.DMA((2, 6)),
        ],
        compiler_params=pltpu.CompilerParams(vmem_limit_bytes=67043328),
    )(first, second)


def shards(prompt_ids, prompt_lengths, embed_table, norm_gain, w_query, w_key, w_value, w_out):
    quarter = prompt_ids.shape[0]
    prompt = quarter * 4
    feats, vocab = embed_table.shape
    width = feats * lax.axis_size(AXES)
    depth, across = w_query.shape[0], w_query.shape[1] + w_key.shape[1] + w_value.shape[1]
    groups = prompt_lengths.shape[0]
    angle = np.arange(prompt)[:, None] * rope_theta ** (-2.0 * np.arange(HD // 2) / HD)[None, :]
    cosine = np.concatenate([np.cos(angle), np.cos(angle)], axis=1).astype(np.float32)
    sine = np.concatenate([-np.sin(angle), np.sin(angle)], axis=1).astype(np.float32)
    chunks = width // 512
    bf, f32 = jnp.bfloat16, jnp.float32
    vmem = pl.BlockSpec(memory_space=pltpu.VMEM)
    anyw = pl.BlockSpec(memory_space=pl.ANY)
    dma = pltpu.SemaphoreType.DMA
    hidden, cache = pl.pallas_call(
        kernel,
        out_shape=(
            jax.ShapeDtypeStruct((quarter, width), bf),
            jax.ShapeDtypeStruct((1, 2, prompt, 2 * HD), bf),
        ),
        in_specs=[pl.BlockSpec(memory_space=pltpu.SMEM)] + [vmem] * 2 + [anyw] * 6,
        out_specs=(anyw, anyw),
        scratch_shapes=[
            pltpu.VMEM((2, 4, feats, TILES * 128), bf),
            pltpu.VMEM((STRIP, 128), f32),
            pltpu.VMEM((512, 128), f32),
            pltpu.VMEM((groups, 4, 128), jnp.int32),
            pltpu.VMEM((4, groups, 128), jnp.int32),
            pltpu.SMEM((4, groups, 128), jnp.int32),
            pltpu.VMEM((4, groups, feats, 128), bf),
            pltpu.VMEM((4, groups, 4, feats, 128), bf),
            pltpu.VMEM((2, 4, 2, 2, depth, across), bf),
            pltpu.VMEM((2, 4, 2, 2, *w_out.shape), bf),
            pltpu.VMEM((quarter, width), bf),
            pltpu.VMEM((1, 2, prompt, 2 * HD), bf),
            pltpu.VMEM((quarter, width), bf),
            pltpu.VMEM((quarter, width), bf),
            pltpu.VMEM((prompt, width), bf),
            pltpu.VMEM((2, prompt, HD), f32),
            pltpu.VMEM((quarter, 128), f32),
            pltpu.VMEM((8, prompt, HD), bf),
            pltpu.VMEM((2, prompt, HD), bf),
            pltpu.VMEM((2, prompt, HD), bf),
            pltpu.VMEM((prompt, 1024), bf),
            pltpu.VMEM((chunks, 4, 2, quarter, 256), bf),
            pltpu.VMEM((chunks, 2, quarter, 256), bf),
            pltpu.VMEM((chunks, 2, quarter, 256), bf),
            pltpu.VMEM((chunks, 2, 2, quarter, 256), bf),
            dma((2, 4)),
            dma((4,)),
            dma((6,)),
            dma((chunks,)),
            dma((4,)),
            dma((4,)),
            dma((4,)),
            dma((4,)),
            dma((4, 4)),
            dma((4, 4)),
        ]
        + [dma((chunks, 2))] * 6
        + Plane.sems()
        + Plane.sems(),
        compiler_params=pltpu.CompilerParams(vmem_limit_bytes=67043328, collective_id=0, has_side_effects=True),
    )(
        prompt_lengths,
        prompt_ids.reshape(1, quarter),
        norm_gain.reshape(1, width),
        np.stack([cosine, sine]),
        embed_table,
        w_query,
        w_key,
        w_value,
        w_out,
    )
    return settle(hidden, cache)


def solution(mesh):
    split = Mesh(mesh.devices.reshape(4, 2, 2, 2, 4), AXES)
    placed = (
        P(AXES),
        P(),
        P(AXES, None),
        P(),
        P(DP, TENSOR),
        P(DP, TENSOR),
        P(DP, TENSOR),
        P(TENSOR, DP),
    )
    return jax.shard_map(
        shards,
        mesh=split,
        in_specs=placed,
        out_specs=(P(AXES, None), P(AXES, None, None, None)),
        check_vma=False,
    )
```

```python
import jax
import jax.numpy as jnp
import numpy as np
from jax import lax
from jax.experimental import pallas as pl
from jax.experimental.pallas import tpu as pltpu
from jax.sharding import Mesh
from jax.sharding import PartitionSpec as P

HD = 128
AXES = ("z", "xlo", "core", "xhi", "y")
DP = ("z", "xlo", "core")
TENSOR = ("xhi", "y")
MESH = pl.DeviceIdType.MESH

norm_eps = 1e-05
rope_theta = 500000.0

BLOCKS = 252
STRIP = BLOCKS * 128
TILES = 21
LOADS = BLOCKS // TILES


class Plane:
    def __init__(self, whole, own, sems, by_row=False):
        self.whole, self.own, self.by_row = whole, own, by_row
        self.send, self.recv, self.core_send, self.core_recv = sems
        self.z = lax.axis_index("z")
        self.xlo = lax.axis_index("xlo")
        self.core = lax.axis_index("core")
        self.xhi = lax.axis_index("xhi")
        self.y = lax.axis_index("y")
        self.x = self.xhi * 2 + self.xlo
        self.half = whole.shape[4] // 2

    def neighbours(self):
        found = []
        for cls in range(2):
            for way in range(2):
                found.append(self.device(cls, self.first(cls) + (3 if way else 1), self.second(cls)))
        found.append((self.z, self.xlo, 1 - self.core, self.xhi, self.y))
        return found

    def first(self, cls):
        return self.x if cls else self.z

    def second(self, cls):
        return self.z if cls else self.x

    def device(self, cls, f, s):
        f, s = f % 4, s % 4
        x, z = (f, s) if cls else (s, f)
        return (z, x % 2, self.core, x // 2, self.y)

    def rows(self, cls, part):
        if part is None:
            return pl.ds(cls * self.half, self.half)
        return pl.ds(cls * self.half + part * (self.half // 2), self.half // 2)

    def piece(self, cls, f, s, part=None):
        f, s = f % 4, s % 4
        x, z = (f, s) if cls else (s, f)
        return self.whole.at[x // 2, z, x % 2, self.core, self.rows(cls, part)]

    def copy(self, cls, stage, slot, f, s, part, own):
        step = 3 if slot % 2 else 1
        pf, ps = self.first(cls), self.second(cls)
        to = self.device(cls, pf + step, ps) if stage == 0 else self.device(cls, pf, ps + step)
        dst = self.piece(cls, f, s, part)
        src = self.own.at[self.rows(cls, part)] if own else dst
        return pltpu.make_async_remote_copy(
            src, dst, self.send.at[cls, stage, slot], self.recv.at[cls, stage, slot], device_id=to, device_id_type=MESH
        )

    def full(self, cls, stage, way):
        o = max(stage - 1, 0)
        return self.copy(cls, stage, way, self.first(cls) + o, self.second(cls), None, o == 0)

    def relay(self, cls, stage, way):
        step = 1 if way else 3
        f, s = self.first(cls), self.second(cls)
        if stage == 0:
            f = f + step
        else:
            f, s = f + stage - 1, s + step
        return self.copy(cls, stage, 2 + way, f, s, way, False)

    def cores(self, cls, o):
        s = ((self.z if self.by_row else self.second(cls)) + o) % 4
        if cls or self.by_row:
            ref = self.whole.at[:, s, :, self.core, self.rows(cls, None)]
        else:
            ref = self.whole.at[s // 2, :, s % 2, self.core, self.rows(cls, None)]
        return pltpu.make_async_remote_copy(
            ref,
            ref,
            self.core_send.at[cls, o],
            self.core_recv.at[cls, o],
            device_id=(self.z, self.xlo, 1 - self.core, self.xhi, self.y),
            device_id_type=MESH,
        )

    def each(self, act, *args):
        for cls in range(2):
            for way in range(2):
                act(cls, way, *args)

    def start_full(self, *stages):
        for stage in stages:
            self.each(lambda cls, way: self.full(cls, stage, way).start())

    def take_full(self, *stages):
        for stage in stages:
            self.each(lambda cls, way: self.full(cls, stage, way).wait_recv())
            self.each(lambda cls, way: self.relay(cls, stage, way).start())

    def take_relay(self, *stages):
        for stage in stages:
            self.each(lambda cls, way: self.relay(cls, stage, way).wait_recv())

    def start_cores(self, cls, *offsets):
        for o in offsets:
            self.cores(cls, o).start()

    def row_step(self, n):
        ways = range(2)
        if n == 0:
            self.start_full(0, 1)
        elif n == 1:
            self.take_full(0)
            self.start_full(2, 4)
        elif n == 2:
            self.take_relay(0)
            self.take_full(1)
            self.start_cores(1, 0)
            self.start_full(3)
        elif n == 3:
            for way in ways:
                self.relay(0, 1, way).wait_recv()
            self.start_cores(0, 0)
            self.take_full(2, 4)
        elif n == 4:
            self.take_full(3)
            self.start_cores(1, 1, 3)
            for stage in (2, 4):
                for way in ways:
                    self.relay(0, stage, way).wait_recv()
            self.start_cores(0, 1, 3)
        else:
            for way in ways:
                self.relay(0, 3, way).wait_recv()
                for stage in range(1, 5):
                    self.relay(1, stage, way).wait_recv()
            self.start_cores(0, 2)
            self.start_cores(1, 2)

    def row_ready(self, o):
        for cls in range(2):
            self.cores(cls, o).wait_recv()

    def drain(self):
        for cls in range(2):
            for o in range(4):
                self.cores(cls, o).wait_send()
        for stage in range(5):
            self.each(lambda cls, way: self.full(cls, stage, way).wait_send())
            self.each(lambda cls, way: self.relay(cls, stage, way).wait_send())

    def step(self, n):
        if n == 0:
            self.start_full(0)
        elif n == 1:
            self.start_full(1)
        elif n == 2:
            self.take_full(0)
        elif n == 3:
            self.start_full(2)
        elif n == 4:
            self.start_full(4)
        elif n == 5:
            self.take_relay(0)
            self.start_full(3)
        elif n == 6:
            self.take_full(1)
        elif n == 7:
            self.start_cores(0, 0)
            self.start_cores(1, 0)
            self.take_full(2)
        elif n == 8:
            self.take_full(4)
        elif n == 9:
            self.take_full(3)
            for cls in range(2):
                self.start_cores(cls, 1, 3)
        elif n == 10:
            self.take_relay(1, 2, 3, 4)
            for cls in range(2):
                self.start_cores(cls, 2)
        else:
            for o in range(4):
                self.row_ready(o)

    @staticmethod
    def sems():
        dma = pltpu.SemaphoreType.DMA
        return [dma((2, 5, 4)), dma((2, 5, 4)), dma((2, 4)), dma((2, 4))]


def place(g, y):
    return (g // 8, g // 4 % 2, g // 2 % 2, g % 2, y)


def kernel(lens_ref, ids_ref, gain_ref, trig_ref, table_ref, wq_ref, wk_ref, wv_ref, wo_ref, hidden_ref, cache_ref,
           raw, major, rows, ids, spots, spots_s, staged, xt, w, wo, hidden, cache, own_x, xb, normed, trig, squares, q, k, v, attended,
           stage, mid, passed, final, table_sems, spot_sem, own_sems, out_sems, id_send, id_recv, look_send, look_recv,
           side_send, side_recv, far_send, far_recv, near_send, near_recv, sum_send, sum_recv, *plane_sems):
    feats, vocab = table_ref.shape
    z = lax.axis_index("z")
    xlo = lax.axis_index("xlo")
    core = lax.axis_index("core")
    xhi = lax.axis_index("xhi")
    y = lax.axis_index("y")
    me = ((z * 2 + xlo) * 2 + core) * 2 + xhi
    groups = ids.shape[0]
    quarter, width = hidden.shape
    up = (y + 1) % 4
    down = (y + 3) % 4
    far = (y + 2) % 4
    tiles = vocab // 128

    def at(member):
        return place(me, member)

    def send(src, dst, ssem, rsem, device):
        return pltpu.make_async_remote_copy(src, dst, ssem, rsem, device_id=device, device_id_type=MESH)

    barrier = pltpu.get_barrier_semaphore()
    for n in range(1, 4):
        pl.semaphore_signal(barrier, inc=1, device_id=at((y + n) % 4), device_id_type=MESH)

    def greet(n, _):
        pl.semaphore_signal(barrier, inc=1, device_id=place((me + n) % groups, y), device_id_type=MESH)
        return 0

    lax.fori_loop(1, groups, greet, 0)


    def table_base(n, strip):
        return jnp.minimum(strip * BLOCKS + n * TILES, tiles - TILES)

    def table_copy(n, strip):
        first = pl.multiple_of(table_base(n, strip) * 128, 128)
        return pltpu.make_async_copy(
            table_ref.at[:, pl.ds(first, TILES * 128)], raw.at[n % 2, strip], table_sems.at[n % 2, strip]
        )

    for n in range(2):
        for strip in range(4):
            table_copy(n, strip).start()
    own_w = w.at[xhi, z, xlo, core]
    own_wo = wo.at[xhi, z, xlo, core]
    mine = [
        pltpu.make_async_copy(ref, own_w.at[:, pl.ds(first, ref.shape[1])], own_sems.at[n])
        for n, (ref, first) in enumerate(((wq_ref, 0), (wk_ref, 512), (wv_ref, 640)))
    ] + [pltpu.make_async_copy(wo_ref, own_wo, own_sems.at[3])]
    angles = pltpu.make_async_copy(trig_ref, trig, own_sems.at[4])
    angles.start()
    for copy in mine:
        copy.start()
    plane_w = Plane(w, own_w, plane_sems[:4])
    plane_o = Plane(wo, own_wo, plane_sems[4:], True)

    def turn(n, _):
        for strip in range(4):
            table_copy(n, strip).wait()

        def tile(t, _):
            parts = []
            for strip in range(4):
                first = jnp.minimum(strip * BLOCKS + n * TILES + t, tiles - 1) - table_base(n, strip)
                parts.append(raw[n % 2, strip, :, pl.ds(pl.multiple_of(first * 128, 128), 128)])
            block = jnp.concatenate(parts, axis=0)
            major[pl.ds(pl.multiple_of((n * TILES + t) * 128, 128), 128), :] = block.T.astype(jnp.float32)
            return 0

        lax.fori_loop(0, TILES, tile, 0, unroll=7)

        @pl.when(n + 2 < LOADS)
        def _():
            for strip in range(4):
                table_copy(n + 2, strip).start()

        return 0

    lax.fori_loop(0, 1, turn, 0)
    pl.semaphore_wait(barrier, 3 + groups - 1)
    ids[pl.ds(me, 1), pl.ds(y, 1), :] = ids_ref[...][None]
    line = [
        send(ids_ref, ids.at[me, pl.ds(y, 1)], id_send.at[n - 1], id_recv.at[n - 1], at((y + n) % 4)) for n in range(1, 4)
    ]
    for copy in line:
        copy.start()
    for copy in mine:
        copy.wait()
    plane_w.step(0)
    lax.fori_loop(1, 4, turn, 0)
    for copy in line:
        copy.wait()

    def spread(n, _):
        send(ids.at[me], ids.at[me], id_send.at[3], id_recv.at[3], place((me + n) % groups, y)).start()
        return 0

    lax.fori_loop(1, groups, spread, 0)
    plane_w.step(1)
    lax.fori_loop(4, 9, turn, 0)
    plane_w.step(2)
    plane_w.step(3)
    lax.fori_loop(9, LOADS, turn, 0)
    most = pl.ds(0, groups - 1)
    others = send(ids.at[most], ids.at[most], id_send.at[3], id_recv.at[3], at(up))
    others.wait_recv()
    all_ids = ids[...]
    strip_of = jnp.zeros_like(all_ids)
    for n in range(1, 4):
        strip_of = strip_of + jnp.where(all_ids >= n * STRIP, 1, 0)
    spots_of = all_ids - strip_of * STRIP
    for s in range(4):
        spots[s] = spots_of[:, s]
    to_smem = [pltpu.make_async_copy(spots.at[s], spots_s.at[s], spot_sem.at[s]) for s in range(4)]
    for copy in to_smem:
        copy.start()
    eye = (
        lax.broadcasted_iota(jnp.int32, (128, 128), 0) == lax.broadcasted_iota(jnp.int32, (128, 128), 1)
    ).astype(jnp.bfloat16)


    def look(s):
        to_smem[s].wait()

        def four(j, _):
            def some(i, _):
                g = (me + 4 * j + i) % groups
                for n in range(128):
                    rows[pl.ds(i * 128 + n, 1), :] = major[pl.ds(spots_s[s, g, n], 1), :]
                return 0

            lax.fori_loop(0, 4, some, 0)
            found = lax.dot_general(
                eye, rows[...].astype(jnp.bfloat16), (((1,), (1,)), ((), ())), preferred_element_type=jnp.float32
            )
            for i in range(4):
                g = (me + 4 * j + i) % groups
                word = ids[pl.ds(g, 1), pl.ds(s, 1), :].reshape(1, 128)
                part = found[:, i * 128 : (i + 1) * 128]
                chosen = part[:feats]
                for n in range(1, 4):
                    chosen = jnp.where(word >= n * STRIP, part[n * feats : (n + 1) * feats], chosen)
                chosen = chosen.astype(jnp.bfloat16)
                staged[s, pl.ds(4 * j + i, 1)] = chosen[None]

                def give():
                    send(staged.at[s, 4 * j + i], xt.at[s, me, y], look_send.at[s], look_recv.at[s], place(g, y)).start()

                if i:
                    give()
                else:
                    pl.when(j > 0)(give)

                    @pl.when(j == 0)
                    def _():
                        xt[s, pl.ds(me, 1), pl.ds(y, 1)] = chosen[None, None]

            return 0

        lax.fori_loop(0, 8, four, 0)

    def looked(s):
        return send(staged.at[s, most], xt.at[s, most, y], look_send.at[s], look_recv.at[s], at(up))

    def side(s, slot):
        first, count, of = ((0, groups, y), (0, groups, y), (0, groups // 2, down), (groups // 2, groups // 2, up))[slot]
        part = xt.at[s, pl.ds(first, count), of]
        return send(part, part, side_send.at[s, slot], side_recv.at[s, slot], at(down if slot % 2 else up))

    def gather(s):
        looked(s).wait_recv()
        side(s, 0).start()
        side(s, 1).start()

    def relay(s):
        for way in range(2):
            side(s, way).wait_recv()
            side(s, 2 + way).start()


    length = lens_ref[me]

    def prepare(s):
        for way in range(2):
            side(s, 2 + way).wait_recv()
        squares[...] = jnp.zeros_like(squares)

        def over(c, _):
            cols = pl.ds(pl.multiple_of(c * 128, 128), 128)
            piece = xt[s, pl.ds(c, 1)].reshape(128, 128).T
            xb[:, cols] = piece
            wide = piece.astype(jnp.float32)
            squares[...] += wide * wide
            return 0

        lax.fori_loop(0, width // 128, over, 0, unroll=4)
        scale = lax.rsqrt(jnp.sum(squares[...], axis=1, keepdims=True) / width + norm_eps)
        squares[...] = jnp.broadcast_to(scale, squares.shape)

        @pl.when(y == s)
        def _():
            own_x[...] = xb[...]

        here = slice(s * quarter, (s + 1) * quarter)

        def norm(c, _):
            cols = pl.ds(pl.multiple_of(c * 128, 128), 128)
            wide = xb[:, cols].astype(jnp.float32) * squares[...] * gain_ref[:, cols]
            normed[here, cols] = wide.astype(jnp.bfloat16)
            return 0

        lax.fori_loop(0, width // 128, norm, 0, unroll=4)
    def project(lo, hi):
        here = slice(lo * quarter, hi * quarter)

        def product(b, first):
            return jnp.dot(
                normed[here, :],
                w[b, :, :, :, :, first : first + 256].reshape(width, 256),
                preferred_element_type=jnp.float32,
            )

        def rotated(part):
            return (part * trig[0, here, :] + pltpu.roll(part, HD // 2, 1) * trig[1, here, :]).astype(jnp.bfloat16)

        def heads(b, _):
            for n in range(2):
                both = product(b, n * 256)
                for h in range(2):
                    q[pl.ds(b * 4 + n * 2 + h, 1), here] = rotated(both[:, h * HD : (h + 1) * HD])[None]
            both = product(b, 512)
            k[pl.ds(b, 1), here] = rotated(both[:, :HD])[None]
            v[pl.ds(b, 1), here] = both[:, HD:].astype(jnp.bfloat16)[None]
            return 0

        lax.fori_loop(0, 2, heads, 0)
        for b in range(2):
            cache[0, 0, here, b * HD : (b + 1) * HD] = k[b, here]
            cache[0, 1, here, b * HD : (b + 1) * HD] = v[b, here]

    def attend(s):
        here = slice(s * quarter, (s + 1) * quarter)
        keys = (s + 1) * quarter
        p = lax.broadcasted_iota(jnp.int32, (quarter, keys), 0) + s * quarter
        j = lax.broadcasted_iota(jnp.int32, (quarter, keys), 1)
        allowed = ((j <= p) & (j < length))[None]
        for b in range(2):
            scores = lax.dot_general(
                q[b * 4 : b * 4 + 4, here].reshape(4 * quarter, HD),
                k[b, :keys],
                (((1,), (1,)), ((), ())),
                preferred_element_type=jnp.float32,
            ).reshape(4, quarter, keys)
            scores = jnp.where(allowed, scores * np.float32(1 / np.sqrt(HD)), -1e30)
            expd = jnp.exp(scores - jnp.max(scores, axis=2, keepdims=True))
            weights = (expd / jnp.sum(expd, axis=2, keepdims=True)).astype(jnp.bfloat16)
            got = jnp.dot(weights.reshape(4 * quarter, keys), v[b, :keys], preferred_element_type=jnp.float32)
            got = got.astype(jnp.bfloat16)
            for h in range(4):
                attended[here, (b * 4 + h) * HD : (b * 4 + h + 1) * HD] = got[h * quarter : (h + 1) * quarter]

    look(0)
    plane_w.step(4)
    look(1)
    gather(0)
    plane_w.step(5)
    plane_w.step(6)
    look(2)
    gather(1)
    relay(0)
    plane_w.step(7)
    plane_w.step(8)
    look(3)
    gather(2)
    plane_w.step(9)
    relay(1)
    prepare(0)
    gather(3)
    plane_o.row_step(0)
    plane_w.step(10)
    relay(2)
    prepare(1)
    plane_o.row_step(1)
    plane_w.step(11)
    angles.wait()
    project(0, 2)
    attend(0)
    relay(3)
    attend(1)
    prepare(2)
    plane_o.row_step(2)
    project(2, 3)
    attend(2)
    prepare(3)
    plane_o.row_step(3)
    project(3, 4)
    attend(3)


    def far_copy(c, way):
        return send(stage.at[c, far, way], mid.at[c, way], far_send.at[c, way], far_recv.at[c, way], at(down if way else up))

    def near_copy(c, way):
        part = stage.at[c, down if way else up, 1 - way]
        return send(part, final.at[c, way, 1 - way], near_send.at[c, way], near_recv.at[c, way], at(down if way else up))

    def sum_copy(c, way):
        return send(passed.at[c, way], final.at[c, way, way], sum_send.at[c, way], sum_recv.at[c, way], at(down if way else up))

    def wide(ref):
        return ref.reshape(quarter, 256).astype(jnp.float32)

    def pass_on(c):
        for way in range(2):
            far_copy(c, way).wait_recv()
            total = wide(stage[pl.ds(c, 1), pl.ds(down if way else up, 1), way]) + wide(mid[pl.ds(c, 1), way])
            passed[pl.ds(c, 1), way] = total.astype(jnp.bfloat16)[None]
            sum_copy(c, way).start()

    def row_of(c):
        g = c // 2
        return (z + g + g // 2 * (1 - 2 * (g % 2))) % 4

    def leave(c):
        cols = pl.ds(pl.multiple_of(row_of(c) * 1024 + c % 2 * 512, 512), 512)
        return pltpu.make_async_copy(hidden.at[:, cols], hidden_ref.at[:, cols], out_sems.at[c])

    def finish(c, _):
        for way in range(2):
            near_copy(c, way).wait_recv()
            sum_copy(c, way).wait_recv()
        for half in range(2):
            cols = pl.ds(pl.multiple_of(row_of(c) * 1024 + c % 2 * 512 + half * 256, 256), 256)
            total = wide(stage[pl.ds(c, 1), pl.ds(y, 1), half])
            for way in range(2):
                total = total + wide(final[pl.ds(c, 1), way, half])
            hidden[:, cols] = (own_x[:, cols].astype(jnp.float32) + total).astype(jnp.bfloat16)
        leave(c).start()
        return 0

    chunks = stage.shape[0]

    def output(c, _):
        for half in range(2):
            part = jnp.dot(attended[:, :512], wo[0, row_of(c), c % 2, half], preferred_element_type=jnp.float32)
            part = part + jnp.dot(attended[:, 512:], wo[1, row_of(c), c % 2, half], preferred_element_type=jnp.float32)
            part = part.astype(jnp.bfloat16)
            for member in range(4):
                stage[pl.ds(c, 1), member, half] = part[member * quarter : (member + 1) * quarter][None]
        for way in range(2):
            far_copy(c, way).start()
        for way in range(2):
            near_copy(c, way).start()

        @pl.when(c > 0)
        def _():
            pass_on(c - 1)

        @pl.when(c > 1)
        def _():
            finish(c - 2, 0)

        return 0

    plane_o.row_ready(0)
    cache_out = pltpu.make_async_copy(cache, cache_ref, own_sems.at[5])
    lax.fori_loop(0, 1, output, 0)
    plane_o.row_step(4)
    cache_out.start()
    lax.fori_loop(1, 2, output, 0)
    plane_o.row_ready(1)
    lax.fori_loop(2, 4, output, 0)
    plane_o.row_step(5)
    plane_o.row_ready(3)
    lax.fori_loop(4, 6, output, 0)
    others.wait_send()
    for s in range(4):
        looked(s).wait_send()
        for slot in range(4):
            side(s, slot).wait_send()
    plane_w.drain()
    plane_o.drain()
    plane_o.row_ready(2)
    lax.fori_loop(6, chunks, output, 0)
    pass_on(chunks - 1)
    lax.fori_loop(chunks - 2, chunks, finish, 0)
    def drain(c, _):
        for way in range(2):
            far_copy(c, way).wait_send()
            near_copy(c, way).wait_send()
            sum_copy(c, way).wait_send()
        leave(c).wait()
        return 0

    lax.fori_loop(0, chunks, drain, 0)
    cache_out.wait()


def settle_kernel(first_ref, second_ref, first_out, second_out, first, second, sems):
    pieces = []
    for n in range(4):
        part = pl.ds(n * (first.shape[0] // 4), first.shape[0] // 4)
        pieces.append((first_ref.at[part], first.at[part], first_out.at[part]))
    for n in range(2):
        pieces.append((second_ref.at[0, n], second.at[0, n], second_out.at[0, n]))
    ways = [
        (pltpu.make_async_copy(a, b, sems.at[0, n]), pltpu.make_async_copy(b, c, sems.at[1, n]))
        for n, (a, b, c) in enumerate(pieces)
    ]
    for into, _ in ways:
        into.start()
    for into, out in ways:
        into.wait()
        out.start()
    for _, out in ways:
        out.wait()


def settle(first, second):
    anyw = pl.BlockSpec(memory_space=pl.ANY)
    return pl.pallas_call(
        settle_kernel,
        out_shape=(jax.ShapeDtypeStruct(first.shape, first.dtype), jax.ShapeDtypeStruct(second.shape, second.dtype)),
        in_specs=[anyw, anyw],
        out_specs=(anyw, anyw),
        scratch_shapes=[
            pltpu.VMEM(first.shape, first.dtype),
            pltpu.VMEM(second.shape, second.dtype),
            pltpu.SemaphoreType.DMA((2, 6)),
        ],
        compiler_params=pltpu.CompilerParams(vmem_limit_bytes=67043328),
    )(first, second)


def shards(prompt_ids, prompt_lengths, embed_table, norm_gain, w_query, w_key, w_value, w_out):
    quarter = prompt_ids.shape[0]
    prompt = quarter * 4
    feats, vocab = embed_table.shape
    width = feats * lax.axis_size(AXES)
    depth, across = w_query.shape[0], w_query.shape[1] + w_key.shape[1] + w_value.shape[1]
    groups = prompt_lengths.shape[0]
    angle = np.arange(prompt)[:, None] * rope_theta ** (-2.0 * np.arange(HD // 2) / HD)[None, :]
    cosine = np.concatenate([np.cos(angle), np.cos(angle)], axis=1).astype(np.float32)
    sine = np.concatenate([-np.sin(angle), np.sin(angle)], axis=1).astype(np.float32)
    chunks = width // 512
    bf, f32 = jnp.bfloat16, jnp.float32
    vmem = pl.BlockSpec(memory_space=pltpu.VMEM)
    anyw = pl.BlockSpec(memory_space=pl.ANY)
    dma = pltpu.SemaphoreType.DMA
    hidden, cache = pl.pallas_call(
        kernel,
        out_shape=(
            jax.ShapeDtypeStruct((quarter, width), bf),
            jax.ShapeDtypeStruct((1, 2, prompt, 2 * HD), bf),
        ),
        in_specs=[pl.BlockSpec(memory_space=pltpu.SMEM)] + [vmem] * 2 + [anyw] * 6,
        out_specs=(anyw, anyw),
        scratch_shapes=[
            pltpu.VMEM((2, 4, feats, TILES * 128), bf),
            pltpu.VMEM((STRIP, 128), f32),
            pltpu.VMEM((512, 128), f32),
            pltpu.VMEM((groups, 4, 128), jnp.int32),
            pltpu.VMEM((4, groups, 128), jnp.int32),
            pltpu.SMEM((4, groups, 128), jnp.int32),
            pltpu.VMEM((4, groups, feats, 128), bf),
            pltpu.VMEM((4, groups, 4, feats, 128), bf),
            pltpu.VMEM((2, 4, 2, 2, depth, across), bf),
            pltpu.VMEM((2, 4, 2, 2, *w_out.shape), bf),
            pltpu.VMEM((quarter, width), bf),
            pltpu.VMEM((1, 2, prompt, 2 * HD), bf),
            pltpu.VMEM((quarter, width), bf),
            pltpu.VMEM((quarter, width), bf),
            pltpu.VMEM((prompt, width), bf),
            pltpu.VMEM((2, prompt, HD), f32),
            pltpu.VMEM((quarter, 128), f32),
            pltpu.VMEM((8, prompt, HD), bf),
            pltpu.VMEM((2, prompt, HD), bf),
            pltpu.VMEM((2, prompt, HD), bf),
            pltpu.VMEM((prompt, 1024), bf),
            pltpu.VMEM((chunks, 4, 2, quarter, 256), bf),
            pltpu.VMEM((chunks, 2, quarter, 256), bf),
            pltpu.VMEM((chunks, 2, quarter, 256), bf),
            pltpu.VMEM((chunks, 2, 2, quarter, 256), bf),
            dma((2, 4)),
            dma((4,)),
            dma((6,)),
            dma((chunks,)),
            dma((4,)),
            dma((4,)),
            dma((4,)),
            dma((4,)),
            dma((4, 4)),
            dma((4, 4)),
        ]
        + [dma((chunks, 2))] * 6
        + Plane.sems()
        + Plane.sems(),
        compiler_params=pltpu.CompilerParams(vmem_limit_bytes=67043328, collective_id=0, has_side_effects=True),
    )(
        prompt_lengths,
        prompt_ids.reshape(1, quarter),
        norm_gain.reshape(1, width),
        np.stack([cosine, sine]),
        embed_table,
        w_query,
        w_key,
        w_value,
        w_out,
    )
    return settle(hidden, cache)


def solution(mesh):
    split = Mesh(mesh.devices.reshape(4, 2, 2, 2, 4), AXES)
    placed = (
        P(AXES),
        P(),
        P(AXES, None),
        P(),
        P(DP, TENSOR),
        P(DP, TENSOR),
        P(DP, TENSOR),
        P(TENSOR, DP),
    )
    return jax.shard_map(
        shards,
        mesh=split,
        in_specs=placed,
        out_specs=(P(AXES, None), P(AXES, None, None, None)),
        check_vma=False,
    )
```
